128 devices in a mesh: dp: 1, tx: 16 (over z, y), ty: 8 (over x, core).
Axes of the slice: x: 4, y: 4, z: 4, core: 2. Of those that a mesh axis runs over, the one named last changes fastest.
Arguments:
- residual: float32 [1024, 2048], P('dp', 'tx')
- norm_w: float32 [2, 2048], P(None, 'tx')
- w_in: bfloat16 [2, 2048, 2, 4096], P(None, 'tx', None, 'ty')
- conv_w: float32 [2, 4096, 4], P(None, 'ty')
- conv_b: float32 [2, 4096], P(None, 'ty')
- w_x: bfloat16 [2, 4096, 160], P(None, 'ty')
- w_dt: bfloat16 [2, 128, 4096], P(None, None, 'ty')
- dt_bias: float32 [2, 4096], P(None, 'ty')
- a_log: float32 [2, 4096, 16], P(None, 'ty')
- d_skip: float32 [2, 4096], P(None, 'ty')
- w_out: bfloat16 [2, 4096, 2048], P(None, 'ty', 'tx')
- conv_state: bfloat16 [2, 1024, 4096, 3], P(None, ('dp', 'tx'), 'ty')
- ssm_state: float32 [2, 1024, 4096, 16], P(None, ('dp', 'tx'), 'ty')
Outputs:
- output 1: float32 [1024, 2048], P('dp', 'tx')
- output 2: bfloat16 [2, 1024, 4096, 3], P(None, ('dp', 'tx'), 'ty')
- output 3: float32 [2, 1024, 4096, 16], P(None, ('dp', 'tx'), 'ty')
All inputs are finite; a program needn't handle non-finite values.
Results may differ from the reference program's by a relative error of at most 0.0181924.
Values are sent between devices in bfloat16 or wider.
A program may use at most 1 GiB of HBM per device.

```python
import math
import jax
import jax.numpy as jnp
from jax import lax

BATCH_ROWS = 1024
D_MODEL = 2048
D_INNER = 4096
D_STATE = 16
DT_RANK = 128
CONV_WIDTH = 4
LAYERS = 2
NORM_EPS = 1e-5
INNER_EPS = 1e-6


def setup_inputs(seed: int = 0, part: int = 0) -> dict:
    keys = jax.random.split(jax.random.key(seed), 10)
    row_keys = jax.random.split(jax.random.fold_in(jax.random.key(seed + 1), part), 3)
    col_pos = jnp.arange(D_MODEL, dtype=jnp.float32) / D_MODEL
    col_scale = jnp.exp(3.0 * col_pos - 1.5)
    residual = jax.random.normal(row_keys[0], (BATCH_ROWS, D_MODEL), jnp.float32) * col_scale
    norm_w = jax.random.uniform(keys[0], (LAYERS, D_MODEL), jnp.float32, 0.5, 1.5)
    w_in = (jax.random.normal(keys[1], (LAYERS, D_MODEL, 2, D_INNER), jnp.float32) * D_MODEL ** -0.5).astype(jnp.bfloat16)
    conv_w = jax.random.normal(keys[2], (LAYERS, D_INNER, CONV_WIDTH), jnp.float32) * CONV_WIDTH ** -0.5
    conv_b = jax.random.normal(keys[3], (LAYERS, D_INNER), jnp.float32) * 0.2
    w_x = (jax.random.normal(keys[4], (LAYERS, D_INNER, DT_RANK + 2 * D_STATE), jnp.float32) * D_INNER ** -0.5).astype(jnp.bfloat16)
    w_dt = (jax.random.normal(keys[5], (LAYERS, DT_RANK, D_INNER), jnp.float32) * DT_RANK ** -0.5).astype(jnp.bfloat16)
    dt_init = jnp.exp(jax.random.uniform(keys[6], (LAYERS, D_INNER), jnp.float32, math.log(0.005), math.log(0.1)))
    dt_bias = dt_init + jnp.log(-jnp.expm1(-dt_init))
    a_log = jnp.log(jax.random.uniform(keys[7], (LAYERS, D_INNER, D_STATE), jnp.float32, 1.0, 16.0))
    d_skip = jax.random.uniform(keys[8], (LAYERS, D_INNER), jnp.float32, 0.5, 2.0)
    w_out = (jax.random.normal(keys[9], (LAYERS, D_INNER, D_MODEL), jnp.float32) * D_INNER ** -0.5).astype(jnp.bfloat16)
    conv_state = jax.random.normal(row_keys[1], (LAYERS, BATCH_ROWS, D_INNER, CONV_WIDTH - 1), jnp.float32).astype(jnp.bfloat16)
    ssm_state = jax.random.normal(row_keys[2], (LAYERS, BATCH_ROWS, D_INNER, D_STATE), jnp.float32) * 0.5
    return {"residual": residual, "norm_w": norm_w, "w_in": w_in, "conv_w": conv_w, "conv_b": conv_b, "w_x": w_x, "w_dt": w_dt, "dt_bias": dt_bias, "a_log": a_log, "d_skip": d_skip, "w_out": w_out, "conv_state": conv_state, "ssm_state": ssm_state}


def unit_rms(vec):
    return vec * lax.rsqrt(jnp.mean(vec * vec, axis=-1, keepdims=True) + INNER_EPS)


def mixer_layer(residual, params):
    norm_w, w_in, conv_w, conv_b, w_x, w_dt, dt_bias, a_log, d_skip, w_out, conv_prev, ssm_prev = params
    variance = jnp.mean(residual * residual, axis=-1, keepdims=True)
    normed = (residual * lax.rsqrt(variance + NORM_EPS) * norm_w).astype(jnp.bfloat16)
    proj_in = jnp.dot(normed, w_in.reshape(D_MODEL, 2 * D_INNER), preferred_element_type=jnp.float32).astype(jnp.bfloat16)
    x_branch = proj_in[:, :D_INNER]
    z_branch = proj_in[:, D_INNER:]
    window = jnp.concatenate([conv_prev, x_branch[:, :, None]], axis=-1)
    conv_val = jnp.sum(window.astype(jnp.float32) * conv_w, axis=-1) + conv_b
    x_conv = jax.nn.silu(conv_val).astype(jnp.bfloat16)
    x_dbl = jnp.dot(x_conv, w_x, preferred_element_type=jnp.float32)
    dt_low = unit_rms(x_dbl[:, :DT_RANK])
    b_mat = unit_rms(x_dbl[:, DT_RANK:DT_RANK + D_STATE])
    c_mat = unit_rms(x_dbl[:, DT_RANK + D_STATE:])
    delta = jax.nn.softplus(jnp.dot(dt_low.astype(jnp.bfloat16), w_dt, preferred_element_type=jnp.float32) + dt_bias)
    x_float = x_conv.astype(jnp.float32)
    decay = jnp.exp(delta[:, :, None] * -jnp.exp(a_log))
    ssm_new = decay * ssm_prev + (delta * x_float)[:, :, None] * b_mat[:, None, :]
    state_val = jnp.sum(ssm_new * c_mat[:, None, :], axis=-1)
    gated = ((state_val + d_skip * x_float) * jax.nn.silu(z_branch.astype(jnp.float32))).astype(jnp.bfloat16)
    out_proj = jnp.dot(gated, w_out, preferred_element_type=jnp.float32)
    return residual + out_proj, (window[:, :, 1:], ssm_new)


def reference(residual, norm_w, w_in, conv_w, conv_b, w_x, w_dt, dt_bias, a_log, d_skip, w_out, conv_state, ssm_state):
    layer_params = (norm_w, w_in, conv_w, conv_b, w_x, w_dt, dt_bias, a_log, d_skip, w_out, conv_state, ssm_state)
    residual_out, caches = lax.scan(mixer_layer, residual, layer_params)
    return residual_out, caches[0], caches[1]
```

```python
import functools

import jax
import jax.numpy as jnp
from jax import lax
from jax.experimental import pallas as pl
from jax.experimental.pallas import tpu as pltpu
from jax.sharding import PartitionSpec as P

NORM_EPS = 1e-5
INNER_EPS = 1e-6
MESH = pl.DeviceIdType.MESH
F32 = jnp.float32
BF16 = jnp.bfloat16
LANES = 128


def nt_dot(lhs, rhs, precision=None):
    return lax.dot_general(lhs, rhs, (((1,), (1,)), ((), ())), precision=precision, preferred_element_type=F32)


def nn_dot(lhs, rhs):
    return jnp.dot(lhs, rhs, preferred_element_type=F32)


def unit_rms(vec, count):
    return vec * lax.rsqrt(jnp.sum(vec * vec, axis=-1, keepdims=True) / count + INNER_EPS)


def step_kernel(dims, res_ref, norm_ref, win_ref, cw_ref, cb_ref, wx_ref, wdt_ref, dtb_ref, al_ref, dsk_ref, wo_ref, cs_ref, ssm_in,
                res_out, conv_out, ssm_out,
                send_a, recv_a, send_b, recv_b, send_a2, recv_a2, send_b2, recv_b2, st_send, st_recv, st2_send, st2_recv, stat_t,
                p_send, p_recv, y_a, y_b, o_send, o_recv, sum_buf, ssm_buf, res_buf, dt_buf, dx_buf, bc_buf, yv_buf, xc_buf,
                a_ss, a_rs, b_ss, b_rs, a2_ss, a2_rs, b2_ss, b2_rs, st_ss, st_rs, st2_ss, st2_rs, p_ss, p_rs,
                ya_ss, ya_rs, yb_ss, yb_rs, ya2_ss, ya2_rs, yb2_ss, yb2_rs, o_ss, o_rs, s_ss, s_rs, ssm_is, ssm_os):
    n_z, n_y, n_ty, rows, layers, d_model, n_state, rank = dims
    tx, ty = lax.axis_index("tx"), lax.axis_index("ty")
    zi, yi = tx // n_y, tx % n_y
    chans = win_ref.shape[-1]
    half = chans // 2
    own_rows = o_recv.shape[2]
    pk = p_send.shape[1] - rows

    def y_peer(off):
        return lax.rem(yi + off, n_y)

    def z_peer(off):
        return lax.rem(zi + off, n_z)

    def at_y(off):
        return {"tx": zi * n_y + y_peer(off), "ty": ty}

    def at_z(off):
        return {"tx": z_peer(off) * n_y + yi, "ty": ty}

    def at_ty(idx):
        return {"tx": tx, "ty": idx}

    pending = []

    def copy(src, dst, ssem, rsem, device):
        return pltpu.make_async_remote_copy(src_ref=src, dst_ref=dst, send_sem=ssem, recv_sem=rsem, device_id=device, device_id_type=MESH)

    def send(src, dst, ssem, rsem, device):
        desc = copy(src, dst, ssem, rsem, device)
        desc.start()
        pending.append(desc)
        return desc

    for lyr in range(layers):
        pltpu.make_async_copy(ssm_in.at[lyr], ssm_buf.at[lyr], ssm_is.at[lyr]).start()

    barrier = pltpu.get_barrier_semaphore()
    for off in range(1, n_y):
        pl.semaphore_signal(barrier, inc=1, device_id=at_y(off), device_id_type=MESH)
    for off in range(1, n_z):
        pl.semaphore_signal(barrier, inc=1, device_id=at_z(off), device_id_type=MESH)
    for off in range(1, n_ty):
        pl.semaphore_signal(barrier, inc=1, device_id=at_ty(lax.rem(ty + off, n_ty)), device_id_type=MESH)
    pl.semaphore_wait(barrier, n_y + n_z + n_ty - 3)

    group = n_y * rows

    def input_matmul(lyr, source):
        ones = jnp.ones((8, LANES), F32)
        norm = norm_ref[lyr:lyr + 1, :]
        hidden = []
        for zz in range(n_z):
            res = source[zz * group:(zz + 1) * group, :]
            st_send[lyr, zz] = nt_dot(ones, res * res, lax.Precision.HIGHEST)
            hidden.append((res * norm).astype(BF16))
        for part in range(2):
            weight = win_ref[lyr, part]
            for zz in range(n_z):
                prod = nn_dot(hidden[zz], weight).astype(BF16)
                send_b[lyr, part, zz] = prod[:, half:]
                for yy in range(n_y):
                    send_a[lyr, part, yy, zz * rows:(zz + 1) * rows, :] = prod[yy * rows:(yy + 1) * rows, :half]
            if part == 0:
                phase_one(lyr, 0)

    def phase_one(lyr, part):
        for off in range(1, n_y):
            send(send_a.at[lyr, part, y_peer(off)], recv_a.at[lyr, part, off - 1], a_ss.at[lyr, part, off - 1], a_rs.at[lyr, part, off - 1], at_y(off))
        for off in range(1, n_z):
            if part == 0:
                send(st_send.at[lyr, z_peer(off)], st_recv.at[lyr, off - 1], st_ss.at[lyr, off - 1], st_rs.at[lyr, off - 1], at_z(off))
            send(send_b.at[lyr, part, z_peer(off)], recv_b.at[lyr, part, off - 1], b_ss.at[lyr, part, off - 1], b_rs.at[lyr, part, off - 1], at_z(off))

    def await_recv(src, dst, ssem, rsem, device):
        copy(src, dst, ssem, rsem, device).wait_recv()

    def phase_two(lyr, part):
        for off in range(1, n_z):
            if part == 0:
                await_recv(st_send.at[lyr, 0], st_recv.at[lyr, off - 1], st_ss.at[lyr, off - 1], st_rs.at[lyr, off - 1], at_z(off))
        if part == 0:
            st2_send[lyr] = functools.reduce(jnp.add, [st_recv[lyr, off - 1] for off in range(1, n_z)], st_send[lyr, zi])
            for off in range(1, n_y):
                send(st2_send.at[lyr], st2_recv.at[lyr, off - 1], st2_ss.at[lyr, off - 1], st2_rs.at[lyr, off - 1], at_y(off))
        for off in range(1, n_y):
            await_recv(send_a.at[lyr, part, 0], recv_a.at[lyr, part, off - 1], a_ss.at[lyr, part, off - 1], a_rs.at[lyr, part, off - 1], at_y(off))
        for zz in range(n_z):
            span = slice(zz * rows, (zz + 1) * rows)
            total = functools.reduce(jnp.add, [recv_a[lyr, part, off - 1, span, :].astype(F32) for off in range(1, n_y)], send_a[lyr, part, yi, span, :].astype(F32))
            send_a2[lyr, part, zz] = total.astype(BF16)
        for off in range(1, n_z):
            send(send_a2.at[lyr, part, z_peer(off)], recv_a2.at[lyr, part, off - 1], a2_ss.at[lyr, part, off - 1], a2_rs.at[lyr, part, off - 1], at_z(off))
        for off in range(1, n_z):
            await_recv(send_b.at[lyr, part, 0], recv_b.at[lyr, part, off - 1], b_ss.at[lyr, part, off - 1], b_rs.at[lyr, part, off - 1], at_z(off))
        for yy in range(n_y):
            span = slice(yy * rows, (yy + 1) * rows)
            total = functools.reduce(jnp.add, [recv_b[lyr, part, off - 1, span, :].astype(F32) for off in range(1, n_z)], send_b[lyr, part, zi, span, :].astype(F32))
            send_b2[lyr, part, yy] = total.astype(BF16)
        for off in range(1, n_y):
            send(send_b2.at[lyr, part, y_peer(off)], recv_b2.at[lyr, part, off - 1], b2_ss.at[lyr, part, off - 1], b2_rs.at[lyr, part, off - 1], at_y(off))

    def finish_sum(lyr, part):
        for off in range(1, n_z):
            await_recv(send_a2.at[lyr, part, 0], recv_a2.at[lyr, part, off - 1], a2_ss.at[lyr, part, off - 1], a2_rs.at[lyr, part, off - 1], at_z(off))
        for off in range(1, n_y):
            await_recv(send_b2.at[lyr, part, 0], recv_b2.at[lyr, part, off - 1], b2_ss.at[lyr, part, off - 1], b2_rs.at[lyr, part, off - 1], at_y(off))
        tot_a = functools.reduce(jnp.add, [recv_a2[lyr, part, off - 1].astype(F32) for off in range(1, n_z)], send_a2[lyr, part, zi].astype(F32))
        tot_b = functools.reduce(jnp.add, [recv_b2[lyr, part, off - 1].astype(F32) for off in range(1, n_y)], send_b2[lyr, part, yi].astype(F32))
        return jnp.concatenate([tot_a, tot_b], axis=-1)

    def row_scale(lyr):
        for off in range(1, n_y):
            await_recv(st2_send.at[lyr], st2_recv.at[lyr, off - 1], st2_ss.at[lyr, off - 1], st2_rs.at[lyr, off - 1], at_y(off))
        total = functools.reduce(jnp.add, [st2_recv[lyr, off - 1] for off in range(1, n_y)], st2_send[lyr])
        stat_t[...] = total.T
        mine = stat_t[pl.ds(pl.multiple_of(yi * rows, 8), rows), :][:, :1]
        return lax.rsqrt(mine / d_model + NORM_EPS)

    source = res_ref
    for lyr in range(layers):
        input_matmul(lyr, source)
        phase_two(lyr, 0)
        phase_one(lyr, 1)
        scale = row_scale(lyr)
        x_in = (finish_sum(lyr, 0) * scale).astype(BF16)

        taps = [cs_ref[lyr, k] for k in range(3)]
        conv_out[lyr, 0] = taps[1]
        conv_out[lyr, 1] = taps[2]
        conv_out[lyr, 2] = x_in
        conv = x_in.astype(F32) * cw_ref[lyr, 3:4, :] + cb_ref[lyr:lyr + 1, :]
        for k in range(3):
            conv = conv + taps[k].astype(F32) * cw_ref[lyr, k:k + 1, :]
        x_conv = (conv * jax.nn.sigmoid(conv)).astype(BF16)

        wx = wx_ref[lyr]
        dt_part = nt_dot(x_conv, wx[:rank])
        bc_w = jnp.concatenate([wx[rank:], jnp.zeros((LANES - 2 * n_state, chans), BF16)], axis=0)
        bc_part = nt_dot(x_conv, bc_w)
        packs = rows // pk
        shift = LANES // packs
        packed = bc_part[:pk]
        for q in range(1, packs):
            packed = packed + pltpu.roll(bc_part[q * pk:(q + 1) * pk], q * shift, 1)
        p_send[lyr, :rows] = dt_part.astype(BF16)
        p_send[lyr, rows:] = packed.astype(BF16)
        for off in range(1, n_ty):
            send(p_send.at[lyr], p_recv.at[lyr, off - 1], p_ss.at[lyr, off - 1], p_rs.at[lyr, off - 1], at_ty(lax.rem(ty + off, n_ty)))

        phase_two(lyr, 1)

        for off in range(1, n_ty):
            await_recv(p_send.at[lyr], p_recv.at[lyr, off - 1], p_ss.at[lyr, off - 1], p_rs.at[lyr, off - 1], at_ty(ty))
        proj = functools.reduce(jnp.add, [p_recv[lyr, off - 1].astype(F32) for off in range(1, n_ty)], p_send[lyr].astype(F32))
        dt_low = unit_rms(proj[:rows], rank).astype(BF16)
        lane = lax.broadcasted_iota(jnp.int32, (pk, LANES), 1)
        for q in range(packs):
            piece = proj[rows:]
            if q:
                piece = pltpu.roll(piece, LANES - q * shift, 1)
            sq = piece * piece
            b_inv = lax.rsqrt(jnp.sum(jnp.where(lane < n_state, sq, 0.0), axis=-1, keepdims=True) / n_state + INNER_EPS)
            c_inv = lax.rsqrt(jnp.sum(jnp.where((lane >= n_state) & (lane < 2 * n_state), sq, 0.0), axis=-1, keepdims=True) / n_state + INNER_EPS)
            bc_buf[q * pk:(q + 1) * pk] = piece * jnp.where(lane < n_state, b_inv, c_inv)
        raw = nn_dot(dt_low, wdt_ref[lyr]) + dtb_ref[lyr:lyr + 1, :]
        delta = jnp.maximum(raw, 0.0) + jnp.log1p(jnp.exp(-jnp.abs(raw)))
        dt_buf[...] = delta
        dx_buf[...] = delta * x_conv.astype(F32)
        xc_buf[...] = x_conv

        pltpu.make_async_copy(ssm_in.at[lyr], ssm_buf.at[lyr], ssm_is.at[lyr]).wait()
        neg_a = -jnp.exp(al_ref[lyr])

        def update(grp, carry):
            base = pl.multiple_of(grp * 8, 8)
            d_rows = dt_buf[pl.ds(base, 8), :]
            x_rows = dx_buf[pl.ds(base, 8), :]
            bc_t = bc_buf[pl.ds(base, 8), :].T
            outs = []
            for j in range(8):
                decay = jnp.exp(d_rows[j:j + 1, :] * neg_a)
                state = decay * ssm_buf[lyr, base + j] + x_rows[j:j + 1, :] * bc_t[:n_state, j:j + 1]
                ssm_buf[lyr, base + j] = state
                outs.append(jnp.sum(state * bc_t[n_state:2 * n_state, j:j + 1], axis=0, keepdims=True))
            yv_buf[pl.ds(base, 8), :] = jnp.concatenate(outs, axis=0)
            return carry

        lax.fori_loop(0, rows // 8, update, 0)
        pltpu.make_async_copy(ssm_buf.at[lyr], ssm_out.at[lyr], ssm_os.at[lyr]).start()

        z_in = (finish_sum(lyr, 1) * scale).astype(BF16).astype(F32)
        gated = ((yv_buf[...] + dsk_ref[lyr:lyr + 1, :] * xc_buf[...].astype(F32)) * (z_in * jax.nn.sigmoid(z_in))).astype(BF16)
        y_a[lyr, zi, yi] = gated[:, :half]
        y_b[lyr, zi, yi] = gated[:, half:]

        def push(buf, zz, yy, ssem, rsem, device):
            send(buf.at[lyr, zz, yy], buf.at[lyr, zz, yy], ssem, rsem, device)

        def landed(buf, ssem, rsem):
            await_recv(buf.at[lyr, 0, 0], buf.at[lyr, 0, 0], ssem, rsem, at_ty(ty))

        for off in range(1, n_y):
            push(y_a, zi, yi, ya_ss.at[lyr, off - 1], ya_rs.at[lyr, off - 1], at_y(off))
        for off in range(1, n_z):
            push(y_b, zi, yi, yb_ss.at[lyr, off - 1], yb_rs.at[lyr, off - 1], at_z(off))
        for out in range(1, n_z):
            push(y_a, zi, yi, ya2_ss.at[lyr, out - 1, 0], ya2_rs.at[lyr, out - 1, 0], at_z(out))
        for out in range(1, n_y):
            push(y_b, zi, yi, yb2_ss.at[lyr, out - 1, 0], yb2_rs.at[lyr, out - 1, 0], at_y(out))
        for off in range(1, n_y):
            landed(y_a, ya_ss.at[lyr, off - 1], ya_rs.at[lyr, off - 1])
            for out in range(1, n_z):
                push(y_a, zi, lax.rem(yi + n_y - off, n_y), ya2_ss.at[lyr, out - 1, off], ya2_rs.at[lyr, out - 1, off], at_z(out))
        for off in range(1, n_z):
            landed(y_b, yb_ss.at[lyr, off - 1], yb_rs.at[lyr, off - 1])
            for out in range(1, n_y):
                push(y_b, lax.rem(zi + n_z - off, n_z), yi, yb2_ss.at[lyr, out - 1, off], yb2_rs.at[lyr, out - 1, off], at_y(out))

        per_group = n_ty // n_z
        for off in range(n_z):
            zz = lax.rem(zi + n_z - off, n_z)
            if off:
                for oy in range(n_y):
                    landed(y_a, ya2_ss.at[lyr, off - 1, oy], ya2_rs.at[lyr, off - 1, oy])
            for oy in range(1, n_y):
                landed(y_b, yb2_ss.at[lyr, oy - 1, off], yb2_rs.at[lyr, oy - 1, off])
            part = nn_dot(y_a[lyr, zz].reshape(group, half), wo_ref[lyr, :half]) + nn_dot(y_b[lyr, zz].reshape(group, half), wo_ref[lyr, half:])
            for i in range(per_group):
                o_send[lyr, zz * per_group + i] = part[i * own_rows:(i + 1) * own_rows].astype(BF16)
            for i in range(per_group):
                owner = zz * per_group + i
                slot = lax.rem(owner - ty + n_ty - 1, n_ty)

                @pl.when(owner != ty)
                def _():
                    copy(o_send.at[lyr, owner], o_recv.at[lyr, slot], o_ss.at[lyr, slot], o_rs.at[lyr, slot], at_ty(owner)).start()

        for off in range(1, n_ty):
            await_recv(o_send.at[lyr, 0], o_recv.at[lyr, off - 1], o_ss.at[lyr, off - 1], o_rs.at[lyr, off - 1], at_ty(ty))
        total = functools.reduce(jnp.add, [o_recv[lyr, off - 1].astype(F32) for off in range(1, n_ty)], o_send[lyr, ty].astype(F32))
        sum_buf[lyr, ty] = total.astype(BF16)
        for off in range(1, n_ty):
            send(sum_buf.at[lyr, ty], sum_buf.at[lyr, ty], s_ss.at[lyr, off - 1], s_rs.at[lyr, off - 1], at_ty(lax.rem(ty + off, n_ty)))
        for off in range(1, n_ty):
            await_recv(sum_buf.at[lyr, 0], sum_buf.at[lyr, 0], s_ss.at[lyr, off - 1], s_rs.at[lyr, off - 1], at_ty(ty))
        target = res_out if lyr == layers - 1 else res_buf
        for blk in range(n_ty):
            span = slice(blk * own_rows, (blk + 1) * own_rows)
            target[span, :] = source[span, :] + sum_buf[lyr, blk].astype(F32)
        source = target

    for desc in pending:
        desc.wait_send()
    for lyr in range(layers):
        for off in range(1, n_ty):
            copy(o_send.at[lyr, 0], o_recv.at[lyr, off - 1], o_ss.at[lyr, off - 1], o_rs.at[lyr, off - 1], at_ty(ty)).wait_send()
        pltpu.make_async_copy(ssm_buf.at[lyr], ssm_out.at[lyr], ssm_os.at[lyr]).wait()


def build(mesh, n_y):
    n_tx, n_ty = mesh.shape["tx"], mesh.shape["ty"]
    n_z = n_tx // n_y

    def local_step(residual, norm_w, w_in, conv_w, conv_b, w_x, w_dt, dt_bias, a_log, d_skip, w_out, conv_state, ssm_state):
        layers, batch, chans, n_state = ssm_state.shape
        rows = batch
        all_rows, d_local = residual.shape
        rank = w_dt.shape[1]
        half = chans // 2
        own = all_rows // n_ty
        pk = rows * 2 * n_state // LANES
        dims = (n_z, n_y, n_ty, rows, layers, d_local * n_tx, n_state, rank)
        vmem = pl.BlockSpec(memory_space=pltpu.VMEM)
        anyspace = pl.BlockSpec(memory_space=pl.ANY)
        dma = pltpu.SemaphoreType.DMA
        scratch = [
            pltpu.VMEM((layers, 2, n_y, n_z * rows, half), BF16),
            pltpu.VMEM((layers, 2, n_y - 1, n_z * rows, half), BF16),
            pltpu.VMEM((layers, 2, n_z, n_y * rows, half), BF16),
            pltpu.VMEM((layers, 2, n_z - 1, n_y * rows, half), BF16),
            pltpu.VMEM((layers, 2, n_z, rows, half), BF16),
            pltpu.VMEM((layers, 2, n_z - 1, rows, half), BF16),
            pltpu.VMEM((layers, 2, n_y, rows, half), BF16),
            pltpu.VMEM((layers, 2, n_y - 1, rows, half), BF16),
            pltpu.VMEM((layers, n_z, 8, n_y * rows), F32),
            pltpu.VMEM((layers, n_z - 1, 8, n_y * rows), F32),
            pltpu.VMEM((layers, 8, n_y * rows), F32),
            pltpu.VMEM((layers, n_y - 1, 8, n_y * rows), F32),
            pltpu.VMEM((n_y * rows, 8), F32),
            pltpu.VMEM((layers, rows + pk, LANES), BF16),
            pltpu.VMEM((layers, n_ty - 1, rows + pk, LANES), BF16),
            pltpu.VMEM((layers, n_z, n_y, rows, half), BF16),
            pltpu.VMEM((layers, n_z, n_y, rows, half), BF16),
            pltpu.VMEM((layers, n_ty, own, d_local), BF16),
            pltpu.VMEM((layers, n_ty - 1, own, d_local), BF16),
            pltpu.VMEM((layers, n_ty, own, d_local), BF16),
            pltpu.VMEM((layers, rows, n_state, chans), F32),
            pltpu.VMEM((all_rows, d_local), F32),
            pltpu.VMEM((rows, chans), F32),
            pltpu.VMEM((rows, chans), F32),
            pltpu.VMEM((rows, LANES), F32),
            pltpu.VMEM((rows, chans), F32),
            pltpu.VMEM((rows, chans), BF16),
        ]
        y1, z1, t1 = n_y - 1, n_z - 1, n_ty - 1
        for shape in [(layers, 2, y1), (layers, 2, z1), (layers, 2, z1), (layers, 2, y1), (layers, z1), (layers, y1), (layers, t1),
                      (layers, y1), (layers, z1), (layers, z1, n_y), (layers, y1, n_z), (layers, t1), (layers, t1)]:
            scratch += [dma(shape), dma(shape)]
        scratch += [dma((layers,)), dma((layers,))]
        res, conv, ssm = pl.pallas_call(
            functools.partial(step_kernel, dims),
            out_shape=(
                jax.ShapeDtypeStruct(residual.shape, F32),
                jax.ShapeDtypeStruct((layers, 3, rows, chans), BF16),
                jax.ShapeDtypeStruct((layers, rows, n_state, chans), F32),
            ),
            in_specs=[vmem] * 12 + [anyspace],
            out_specs=(vmem, vmem, anyspace),
            scratch_shapes=scratch,
            compiler_params=pltpu.CompilerParams(collective_id=0, has_side_effects=True, vmem_limit_bytes=60 * 1024 * 1024),
        )(
            residual, norm_w, w_in.transpose(0, 2, 1, 3), conv_w.transpose(0, 2, 1), conv_b, w_x.transpose(0, 2, 1), w_dt, dt_bias,
            a_log.transpose(0, 2, 1), d_skip, w_out, conv_state.transpose(0, 3, 1, 2), ssm_state.transpose(0, 1, 3, 2),
        )
        return res, conv.transpose(0, 2, 3, 1), ssm.transpose(0, 1, 3, 2)

    cache_spec = P(None, ("dp", "tx"), "ty", None)
    in_specs = (P("dp", "tx"), P(None, "tx"), P(None, "tx", None, "ty"), P(None, "ty", None), P(None, "ty"), P(None, "ty", None), P(None, None, "ty"), P(None, "ty"), P(None, "ty", None), P(None, "ty"), P(None, "ty", "tx"), cache_spec, cache_spec)
    out_specs = (P("dp", "tx"), cache_spec, cache_spec)
    return jax.shard_map(local_step, mesh=mesh, in_specs=in_specs, out_specs=out_specs, check_vma=False)


def solution(mesh):
    return build(mesh, 4)
```

```python
import functools

import jax
import jax.numpy as jnp
from jax import lax
from jax.experimental import pallas as pl
from jax.experimental.pallas import tpu as pltpu
from jax.sharding import PartitionSpec as P

NORM_EPS = 1e-5
INNER_EPS = 1e-6
MESH = pl.DeviceIdType.MESH
F32 = jnp.float32
BF16 = jnp.bfloat16
LANES = 128
VMEM_LIMIT = 52 * 1024 * 1024


def nt_dot(lhs, rhs, precision=None):
    return lax.dot_general(lhs, rhs, (((1,), (1,)), ((), ())), precision=precision, preferred_element_type=F32)


def nn_dot(lhs, rhs):
    return jnp.dot(lhs, rhs, preferred_element_type=F32)


def unit_rms(vec, count):
    return vec * lax.rsqrt(jnp.sum(vec * vec, axis=-1, keepdims=True) / count + INNER_EPS)


def step_kernel(dims, res_in, norm_in, win_in, cw_in, cb_in, wx_in, wdt_in, dtb_in, al_in, dsk_in, wo_in, cs_in, ssm_in,
                res_out, conv_out, ssm_buf,
                res_ref, norm_ref, win_ref, cw_ref, cb_ref, wx_ref, wdt_ref, dtb_ref, al_ref, dsk_ref, wo_ref, cs_ref,
                w_buf, send_a, recv_a, send_b, recv_b, send_a2, recv_a2, send_b2, recv_b2, st_send, st_recv, st2_send, st2_recv, stat_t,
                p_send, p_recv, y_a, y_b, o_send, o_recv, sum_buf, res_buf, dt_buf, dx_buf, bc_buf, yv_buf, xc_buf,
                a_ss, a_rs, b_ss, b_rs, a2_ss, a2_rs, b2_ss, b2_rs, st_ss, st_rs, st2_ss, st2_rs, p_ss, p_rs,
                ya_ss, ya_rs, yb_ss, yb_rs, ya2_ss, ya2_rs, yb2_ss, yb2_rs, o_ss, o_rs, s_ss, s_rs, in_sems):
    n_z, n_y, n_ty, n_str, rows, layers, d_model, n_state, rank, lag = dims
    tx, ty = lax.axis_index("tx"), lax.axis_index("ty")
    zi, yi = tx // n_y, tx % n_y
    chans = win_ref.shape[-1]
    half = chans // 2
    own_blocks = n_z * n_y // n_ty
    own_rows = own_blocks * rows
    group = n_y * rows
    pk = p_send.shape[1] - rows
    scope = jax.named_scope

    def y_peer(off):
        return lax.rem(yi + off, n_y)

    def z_peer(off):
        return lax.rem(zi + off, n_z)

    def at_y(off):
        return {"tx": zi * n_y + y_peer(off), "ty": ty}

    def at_z(off):
        return {"tx": z_peer(off) * n_y + yi, "ty": ty}

    def at_ty(idx):
        return {"tx": tx, "ty": idx}

    def ty_peer(off):
        return at_ty(lax.rem(ty + off, n_ty))

    pending = []

    def copy(src, dst, ssem, rsem, device):
        return pltpu.make_async_remote_copy(src_ref=src, dst_ref=dst, send_sem=ssem, recv_sem=rsem, device_id=device, device_id_type=MESH)

    def send(src, dst, ssem, rsem, device):
        desc = copy(src, dst, ssem, rsem, device)
        desc.start()
        pending.append(desc)

    def await_recv(src, dst, ssem, rsem, device):
        copy(src, dst, ssem, rsem, device).wait_recv()

    def add_up(first, others):
        return functools.reduce(jnp.add, [o.astype(F32) for o in others], first.astype(F32))

    def input_matmul(k, lyr, strm, source, part):
        norm = norm_ref[lyr:lyr + 1, :]
        for zz in range(n_z):
            res = source[zz * n_y:(zz + 1) * n_y, strm].reshape(group, LANES)
            if part == 0:
                st_send[k, zz] = nt_dot(jnp.ones((8, LANES), F32), res * res, lax.Precision.HIGHEST)
            prod = nn_dot((res * norm).astype(BF16), w_buf[lyr, part]).astype(BF16)
            send_b[k, part, zz] = prod[:, half:]
            for yy in range(n_y):
                send_a[k, part, yy, zz * rows:(zz + 1) * rows, :] = prod[yy * rows:(yy + 1) * rows, :half]

    def phase_one(k, part):
        for off in range(1, n_z):
            if part == 0:
                send(st_send.at[k, z_peer(off)], st_recv.at[k, off - 1], st_ss.at[k, off - 1], st_rs.at[k, off - 1], at_z(off))
        for off in range(1, max(n_y, n_z)):
            if off < n_y:
                send(send_a.at[k, part, y_peer(off)], recv_a.at[k, part, off - 1], a_ss.at[k, part, off - 1], a_rs.at[k, part, off - 1], at_y(off))
            if off < n_z:
                send(send_b.at[k, part, z_peer(off)], recv_b.at[k, part, off - 1], b_ss.at[k, part, off - 1], b_rs.at[k, part, off - 1], at_z(off))

    def phase_two(k, part):
        if part == 0:
            for off in range(1, n_z):
                await_recv(st_send.at[k, 0], st_recv.at[k, off - 1], st_ss.at[k, off - 1], st_rs.at[k, off - 1], at_z(off))
            st2_send[k] = add_up(st_send[k, zi], [st_recv[k, off - 1] for off in range(1, n_z)])
            for off in range(1, n_y):
                send(st2_send.at[k], st2_recv.at[k, off - 1], st2_ss.at[k, off - 1], st2_rs.at[k, off - 1], at_y(off))
        with scope(f"wait_a1_{part}"):
            for off in range(1, n_y):
                await_recv(send_a.at[k, part, 0], recv_a.at[k, part, off - 1], a_ss.at[k, part, off - 1], a_rs.at[k, part, off - 1], at_y(off))
        for zz in range(n_z):
            span = slice(zz * rows, (zz + 1) * rows)
            send_a2[k, part, zz] = add_up(send_a[k, part, yi, span, :], [recv_a[k, part, off - 1, span, :] for off in range(1, n_y)]).astype(BF16)
        for off in range(1, n_z):
            send(send_a2.at[k, part, z_peer(off)], recv_a2.at[k, part, off - 1], a2_ss.at[k, part, off - 1], a2_rs.at[k, part, off - 1], at_z(off))
        with scope(f"wait_b1_{part}"):
            for off in range(1, n_z):
                await_recv(send_b.at[k, part, 0], recv_b.at[k, part, off - 1], b_ss.at[k, part, off - 1], b_rs.at[k, part, off - 1], at_z(off))
        for yy in range(n_y):
            span = slice(yy * rows, (yy + 1) * rows)
            send_b2[k, part, yy] = add_up(send_b[k, part, zi, span, :], [recv_b[k, part, off - 1, span, :] for off in range(1, n_z)]).astype(BF16)
        for off in range(1, n_y):
            send(send_b2.at[k, part, y_peer(off)], recv_b2.at[k, part, off - 1], b2_ss.at[k, part, off - 1], b2_rs.at[k, part, off - 1], at_y(off))

    def finish_sum(k, part):
        with scope(f"wait_2_{part}"):
            for off in range(1, n_z):
                await_recv(send_a2.at[k, part, 0], recv_a2.at[k, part, off - 1], a2_ss.at[k, part, off - 1], a2_rs.at[k, part, off - 1], at_z(off))
            for off in range(1, n_y):
                await_recv(send_b2.at[k, part, 0], recv_b2.at[k, part, off - 1], b2_ss.at[k, part, off - 1], b2_rs.at[k, part, off - 1], at_y(off))
        tot_a = add_up(send_a2[k, part, zi], [recv_a2[k, part, off - 1] for off in range(1, n_z)])
        tot_b = add_up(send_b2[k, part, yi], [recv_b2[k, part, off - 1] for off in range(1, n_y)])
        return jnp.concatenate([tot_a, tot_b], axis=-1)

    def row_scale(k):
        for off in range(1, n_y):
            await_recv(st2_send.at[k], st2_recv.at[k, off - 1], st2_ss.at[k, off - 1], st2_rs.at[k, off - 1], at_y(off))
        stat_t[k] = add_up(st2_send[k], [st2_recv[k, off - 1] for off in range(1, n_y)]).T
        mine = stat_t[k, pl.ds(pl.multiple_of(yi * rows, 8), rows), :][:, :1]
        return lax.rsqrt(mine / d_model + NORM_EPS)

    def conv_and_proj(k, lyr, mine, x_in):
        taps = [cs_ref[lyr, j, mine, :] for j in range(3)]
        conv_out[lyr, 0, mine, :] = taps[1]
        conv_out[lyr, 1, mine, :] = taps[2]
        conv_out[lyr, 2, mine, :] = x_in
        conv = x_in.astype(F32) * cw_ref[lyr, 3:4, :] + cb_ref[lyr:lyr + 1, :]
        for j in range(3):
            conv = conv + taps[j].astype(F32) * cw_ref[lyr, j:j + 1, :]
        x_conv = (conv * jax.nn.sigmoid(conv)).astype(BF16)
        xc_buf[k] = x_conv
        wx = wx_ref[lyr]
        bc_w = jnp.concatenate([wx[rank:], jnp.zeros((LANES - 2 * n_state, chans), BF16)], axis=0)
        bc_part = nt_dot(x_conv, bc_w)
        packed = bc_part[:pk]
        for q in range(1, rows // pk):
            packed = packed + pltpu.roll(bc_part[q * pk:(q + 1) * pk], q * 2 * n_state, 1)
        p_send[k, :rows] = nt_dot(x_conv, wx[:rank]).astype(BF16)
        p_send[k, rows:] = packed.astype(BF16)

    def step_sizes(k, lyr):
        proj = add_up(p_send[k], [p_recv[k, off - 1] for off in range(1, n_ty)])
        dt_low = unit_rms(proj[:rows], rank).astype(BF16)
        lane = lax.broadcasted_iota(jnp.int32, (pk, LANES), 1)
        for q in range(rows // pk):
            piece = proj[rows:]
            if q:
                piece = pltpu.roll(piece, LANES - q * 2 * n_state, 1)
            sq = piece * piece
            b_inv = lax.rsqrt(jnp.sum(jnp.where(lane < n_state, sq, 0.0), axis=-1, keepdims=True) / n_state + INNER_EPS)
            c_inv = lax.rsqrt(jnp.sum(jnp.where((lane >= n_state) & (lane < 2 * n_state), sq, 0.0), axis=-1, keepdims=True) / n_state + INNER_EPS)
            bc_buf[k, q * pk:(q + 1) * pk] = piece * jnp.where(lane < n_state, b_inv, c_inv)
        raw = nn_dot(dt_low, wdt_ref[lyr]) + dtb_ref[lyr:lyr + 1, :]
        delta = jnp.maximum(raw, 0.0) + jnp.log1p(jnp.exp(-jnp.abs(raw)))
        dt_buf[k] = delta
        dx_buf[k] = delta * xc_buf[k].astype(F32)

    def state_update(k, lyr, strm):
        neg_a = -jnp.exp(al_ref[lyr])

        def update(grp, carry):
            base = pl.multiple_of(grp * 8, 8)
            d_rows = dt_buf[k, pl.ds(base, 8), :]
            x_rows = dx_buf[k, pl.ds(base, 8), :]
            bc_t = bc_buf[k, pl.ds(base, 8), :].T
            outs = []
            for j in range(8):
                row = strm * rows + base + j
                decay = jnp.exp(d_rows[j:j + 1, :] * neg_a)
                state = decay * ssm_buf[lyr, row] + x_rows[j:j + 1, :] * bc_t[:n_state, j:j + 1]
                ssm_buf[lyr, row] = state
                outs.append(jnp.sum(state * bc_t[n_state:2 * n_state, j:j + 1], axis=0, keepdims=True))
            yv_buf[k, pl.ds(base, 8), :] = jnp.concatenate(outs, axis=0)
            return carry

        lax.fori_loop(0, rows // 8, update, 0)

    def push(buf, k, zz, yy, ssem, rsem, device):
        send(buf.at[k, zz, yy], buf.at[k, zz, yy], ssem, rsem, device)

    def landed(buf, k, ssem, rsem):
        await_recv(buf.at[k, 0, 0], buf.at[k, 0, 0], ssem, rsem, at_ty(ty))

    def stream(strm):
        mine = slice(strm * rows, (strm + 1) * rows)
        source = res_ref
        for lyr in range(layers):
            k = lyr * n_str + strm
            with scope(f"matmul_{strm}"):
                input_matmul(k, lyr, strm, source, 0)
            if lyr == 0:
                input_matmul(k, lyr, strm, source, 1)
                yield
            phase_one(k, 0)
            if lyr:
                input_matmul(k, lyr, strm, source, 1)
            yield
            with scope(f"phase2_{strm}"):
                phase_two(k, 0)
            phase_one(k, 1)
            yield
            with scope(f"xconv_{strm}"):
                scale = row_scale(k)
                need(7)
                conv_and_proj(k, lyr, mine, (finish_sum(k, 0) * scale).astype(BF16))
            for off in range(1, n_ty):
                send(p_send.at[k], p_recv.at[k, off - 1], p_ss.at[k, off - 1], p_rs.at[k, off - 1], ty_peer(off))
            yield
            with scope(f"phase2z_{strm}"):
                phase_two(k, 1)
            yield
            with scope(f"wait_p_{strm}"):
                for off in range(1, n_ty):
                    await_recv(p_send.at[k], p_recv.at[k, off - 1], p_ss.at[k, off - 1], p_rs.at[k, off - 1], ty_peer(off))
            with scope(f"ssm_{strm}"):
                need(13 + lyr)
                step_sizes(k, lyr)
                state_update(k, lyr, strm)
            yield
            with scope(f"gate_{strm}"):
                z_in = (finish_sum(k, 1) * scale).astype(BF16).astype(F32)
                gated = ((yv_buf[k] + dsk_ref[lyr:lyr + 1, :] * xc_buf[k].astype(F32)) * (z_in * jax.nn.sigmoid(z_in))).astype(BF16)
                y_a[k, zi, yi] = gated[:, :half]
                y_b[k, zi, yi] = gated[:, half:]
            for off in range(1, n_y):
                push(y_a, k, zi, yi, ya_ss.at[k, off - 1], ya_rs.at[k, off - 1], at_y(off))
            for off in range(1, n_z):
                push(y_b, k, zi, yi, yb_ss.at[k, off - 1], yb_rs.at[k, off - 1], at_z(off))
            for out in range(1, n_z):
                push(y_a, k, zi, yi, ya2_ss.at[k, out - 1, 0], ya2_rs.at[k, out - 1, 0], at_z(out))
            for out in range(1, n_y):
                push(y_b, k, zi, yi, yb2_ss.at[k, out - 1, 0], yb2_rs.at[k, out - 1, 0], at_y(out))
            yield
            with scope(f"fwd_{strm}"):
                for off in range(1, max(n_y, n_z)):
                    if off < n_y:
                        landed(y_a, k, ya_ss.at[k, off - 1], ya_rs.at[k, off - 1])
                        for out in range(1, n_z):
                            push(y_a, k, zi, lax.rem(yi + n_y - off, n_y), ya2_ss.at[k, out - 1, off], ya2_rs.at[k, out - 1, off], at_z(out))
                    if off < n_z:
                        landed(y_b, k, yb_ss.at[k, off - 1], yb_rs.at[k, off - 1])
                        for out in range(1, n_y):
                            push(y_b, k, lax.rem(zi + n_z - off, n_z), yi, yb2_ss.at[k, out - 1, off], yb2_rs.at[k, out - 1, off], at_y(out))
            per_group = n_ty // n_z
            for off in range(n_z):
                if off < 2:
                    yield
                with scope(f"outmm_{strm}_{off}"):
                    zz = lax.rem(zi + n_z - off, n_z)
                    if off:
                        for oy in range(n_y):
                            landed(y_a, k, ya2_ss.at[k, off - 1, oy], ya2_rs.at[k, off - 1, oy])
                    for oy in range(1, n_y):
                        landed(y_b, k, yb2_ss.at[k, oy - 1, off], yb2_rs.at[k, oy - 1, off])
                    part = nn_dot(y_a[k, zz].reshape(group, half), wo_ref[lyr, :half]) + nn_dot(y_b[k, zz].reshape(group, half), wo_ref[lyr, half:])
                    for i in range(per_group):
                        o_send[k, zz * per_group + i] = part[i * own_rows:(i + 1) * own_rows].astype(BF16)
                    for i in range(per_group):
                        owner = zz * per_group + i
                        slot = lax.rem(owner - ty + n_ty - 1, n_ty)

                        @pl.when(owner != ty)
                        def _():
                            copy(o_send.at[k, owner], o_recv.at[k, slot], o_ss.at[k, slot], o_rs.at[k, slot], at_ty(owner)).start()

            yield
            with scope(f"wait_o_{strm}"):
                for off in range(1, n_ty):
                    await_recv(o_send.at[k, 0], o_recv.at[k, off - 1], o_ss.at[k, off - 1], o_rs.at[k, off - 1], at_ty(ty))
            sum_buf[k, ty] = add_up(o_send[k, ty], [o_recv[k, off - 1] for off in range(1, n_ty)]).astype(BF16)
            for off in range(1, n_ty):
                send(sum_buf.at[k, ty], sum_buf.at[k, ty], s_ss.at[k, off - 1], s_rs.at[k, off - 1], ty_peer(off))
            yield
            with scope(f"wait_s_{strm}"):
                for off in range(1, n_ty):
                    await_recv(sum_buf.at[k, 0], sum_buf.at[k, 0], s_ss.at[k, off - 1], s_rs.at[k, off - 1], at_ty(ty))
            target = res_out if lyr == layers - 1 else res_buf
            for blk in range(n_ty):
                span = slice(blk * own_blocks, (blk + 1) * own_blocks)
                total = source[span, strm] + sum_buf[k, blk].astype(F32).reshape(own_blocks, rows, LANES)
                target[span, strm] = total
            source = target

    moves = [(res_in, res_ref), (norm_in, norm_ref), (win_in, win_ref), (cw_in, cw_ref), (cb_in, cb_ref), (cs_in, cs_ref), (wx_in, wx_ref),
             (wdt_in, wdt_ref), (dtb_in, dtb_ref), (al_in, al_ref), (dsk_in, dsk_ref), (wo_in, wo_ref)]
    moves += [(ssm_in.at[lyr], ssm_buf.at[lyr]) for lyr in range(layers)]
    loads = [pltpu.make_async_copy(src, dst, in_sems.at[i]) for i, (src, dst) in enumerate(moves)]
    for load in loads:
        load.start()

    barrier = pltpu.get_barrier_semaphore()
    for off in range(1, n_y):
        pl.semaphore_signal(barrier, inc=1, device_id=at_y(off), device_id_type=MESH)
    for off in range(1, n_z):
        pl.semaphore_signal(barrier, inc=1, device_id=at_z(off), device_id_type=MESH)
    for off in range(1, n_ty):
        pl.semaphore_signal(barrier, inc=1, device_id=ty_peer(off), device_id_type=MESH)

    def need(count):
        while len(moves) - len(loads) < count:
            loads.pop(0).wait()

    need(3)
    for lyr in range(layers):
        for part in range(2):
            w_buf[lyr, part] = win_ref[lyr, :, part, :]
    streams = [stream(strm) for strm in range(n_str)]
    for strm in streams:
        next(strm)
    with scope("barrier"):
        pl.semaphore_wait(barrier, n_y + n_z + n_ty - 3)

    live = list(streams)
    turn = 0
    while live:
        for idx, strm in enumerate(streams):
            if strm in live and turn >= idx * lag:
                try:
                    next(strm)
                except StopIteration:
                    live.remove(strm)
        turn += 1

    with scope("drain"):
        for desc in pending:
            desc.wait_send()
        for k in range(layers * n_str):
            for off in range(1, n_ty):
                copy(o_send.at[k, 0], o_recv.at[k, off - 1], o_ss.at[k, off - 1], o_rs.at[k, off - 1], at_ty(ty)).wait_send()


def store_kernel(res_ref, conv_ref, ssm_ref, res_out, conv_out, ssm_out, sems):
    copies = [pltpu.make_async_copy(src, dst, sems.at[i]) for i, (src, dst) in enumerate([(ssm_ref, ssm_out), (res_ref, res_out), (conv_ref, conv_out)])]
    for desc in copies:
        desc.start()
    for desc in copies:
        desc.wait()


def on_chip(shape, dtype):
    return pltpu.VMEM(shape, dtype)


def from_chip(array):
    return pltpu.with_memory_space_constraint(array, pltpu.VMEM)


def build(mesh, n_y, n_str, lag):
    n_tx, n_ty = mesh.shape["tx"], mesh.shape["ty"]
    n_z = n_tx // n_y

    def local_step(residual, norm_w, w_in, conv_w, conv_b, w_x, w_dt, dt_bias, a_log, d_skip, w_out, conv_state, ssm_state):
        layers, batch, chans, n_state = ssm_state.shape
        rows = batch // n_str
        all_rows, d_local = residual.shape
        rank = w_dt.shape[1]
        half = chans // 2
        own = all_rows // n_ty // n_str
        pk = rows * 2 * n_state // LANES
        ks = layers * n_str
        dims = (n_z, n_y, n_ty, n_str, rows, layers, d_local * n_tx, n_state, rank, lag)
        vmem = pl.BlockSpec(memory_space=pltpu.VMEM)
        anyspace = pl.BlockSpec(memory_space=pl.ANY)
        dma = pltpu.SemaphoreType.DMA
        res_shape = (n_tx, n_str, rows, d_local)
        conv_shape = (layers, 3, batch, chans)
        ssm_shape = (layers, batch, n_state, chans)
        operands = [
            residual.reshape(res_shape), norm_w, w_in, conv_w.transpose(0, 2, 1), conv_b, w_x.transpose(0, 2, 1), w_dt, dt_bias,
            a_log.transpose(0, 2, 1), d_skip, w_out, conv_state.transpose(0, 3, 1, 2), ssm_state.transpose(0, 1, 3, 2),
        ]
        scratch = [pltpu.VMEM(op.shape, op.dtype) for op in operands[:-1]]
        scratch += [
            pltpu.VMEM((layers, 2, d_local, chans), BF16),
            pltpu.VMEM((ks, 2, n_y, n_z * rows, half), BF16),
            pltpu.VMEM((ks, 2, n_y - 1, n_z * rows, half), BF16),
            pltpu.VMEM((ks, 2, n_z, n_y * rows, half), BF16),
            pltpu.VMEM((ks, 2, n_z - 1, n_y * rows, half), BF16),
            pltpu.VMEM((ks, 2, n_z, rows, half), BF16),
            pltpu.VMEM((ks, 2, n_z - 1, rows, half), BF16),
            pltpu.VMEM((ks, 2, n_y, rows, half), BF16),
            pltpu.VMEM((ks, 2, n_y - 1, rows, half), BF16),
            pltpu.VMEM((ks, n_z, 8, n_y * rows), F32),
            pltpu.VMEM((ks, n_z - 1, 8, n_y * rows), F32),
            pltpu.VMEM((ks, 8, n_y * rows), F32),
            pltpu.VMEM((ks, n_y - 1, 8, n_y * rows), F32),
            pltpu.VMEM((ks, n_y * rows, 8), F32),
            pltpu.VMEM((ks, rows + pk, LANES), BF16),
            pltpu.VMEM((ks, n_ty - 1, rows + pk, LANES), BF16),
            pltpu.VMEM((ks, n_z, n_y, rows, half), BF16),
            pltpu.VMEM((ks, n_z, n_y, rows, half), BF16),
            pltpu.VMEM((ks, n_ty, own, d_local), BF16),
            pltpu.VMEM((ks, n_ty - 1, own, d_local), BF16),
            pltpu.VMEM((ks, n_ty, own, d_local), BF16),
            pltpu.VMEM(res_shape, F32),
            pltpu.VMEM((ks, rows, chans), F32),
            pltpu.VMEM((ks, rows, chans), F32),
            pltpu.VMEM((ks, rows, LANES), F32),
            pltpu.VMEM((ks, rows, chans), F32),
            pltpu.VMEM((ks, rows, chans), BF16),
        ]
        y1, z1, t1 = n_y - 1, n_z - 1, n_ty - 1
        for shape in [(ks, 2, y1), (ks, 2, z1), (ks, 2, z1), (ks, 2, y1), (ks, z1), (ks, y1), (ks, t1),
                      (ks, y1), (ks, z1), (ks, z1, n_y), (ks, y1, n_z), (ks, t1), (ks, t1)]:
            scratch += [dma(shape), dma(shape)]
        scratch += [dma((len(operands) - 1 + layers,))]
        res, conv, ssm = pl.pallas_call(
            functools.partial(step_kernel, dims),
            out_shape=(on_chip(res_shape, F32), on_chip(conv_shape, BF16), on_chip(ssm_shape, F32)),
            in_specs=[pl.BlockSpec(memory_space=pltpu.HBM)] * len(operands),
            out_specs=(vmem, vmem, vmem),
            scratch_shapes=scratch,
            compiler_params=pltpu.CompilerParams(collective_id=0, has_side_effects=True, vmem_limit_bytes=VMEM_LIMIT),
        )(*operands)
        res, conv, ssm = pl.pallas_call(
            store_kernel,
            out_shape=(jax.ShapeDtypeStruct(res_shape, F32), jax.ShapeDtypeStruct(conv_shape, BF16), jax.ShapeDtypeStruct(ssm_shape, F32)),
            in_specs=[vmem] * 3,
            out_specs=(anyspace,) * 3,
            scratch_shapes=[dma((3,))],
            compiler_params=pltpu.CompilerParams(vmem_limit_bytes=16 * 1024 * 1024),
        )(*(from_chip(out) for out in (res, conv, ssm)))
        return res.reshape(all_rows, d_local), conv.transpose(0, 2, 3, 1), ssm.transpose(0, 1, 3, 2)

    cache_spec = P(None, ("dp", "tx"), "ty", None)
    in_specs = (P("dp", "tx"), P(None, "tx"), P(None, "tx", None, "ty"), P(None, "ty", None), P(None, "ty"), P(None, "ty", None), P(None, None, "ty"), P(None, "ty"), P(None, "ty", None), P(None, "ty"), P(None, "ty", "tx"), cache_spec, cache_spec)
    out_specs = (P("dp", "tx"), cache_spec, cache_spec)
    return jax.shard_map(local_step, mesh=mesh, in_specs=in_specs, out_specs=out_specs, check_vma=False)


def solution(mesh):
    return build(mesh, 4, 2, 1)
```

```python
import functools

import jax
import jax.numpy as jnp
from jax import lax
from jax.experimental import pallas as pl
from jax.experimental.pallas import tpu as pltpu
from jax.sharding import PartitionSpec as P

NORM_EPS = 1e-5
INNER_EPS = 1e-6
MESH = pl.DeviceIdType.MESH
F32 = jnp.float32
BF16 = jnp.bfloat16
LANES = 128
GATE = 10
STREAMS = 4
ORDER = (
    1, 0, 11, 1, 10, 0, 2, 11, 1, 12, 3, 0, 10, 2, 1, 1, 0, 13, 3, 0, 2, 12, 1, 13,
    3, 0, 2, 2, 1, 3, 3, 2, 0, 1, 3, 0, 2, 1, 11, 3, 0, 2, 10, 1, 3, 2, 11, 0,
    3, 12, 1, 2, 13, 1, 3, 1, 10, 0, 12, 2, 13, 3, 1, 0, 0, 2, 2, 3, 3, 0, 2, 3,
    1, 0, 2, 3, 1, 0, 2, 3, 0, 1, 2, 3,
)
VMEM_LIMIT = 52 * 1024 * 1024


def nt_dot(lhs, rhs, precision=None):
    return lax.dot_general(lhs, rhs, (((1,), (1,)), ((), ())), precision=precision, preferred_element_type=F32)


def nn_dot(lhs, rhs):
    return jnp.dot(lhs, rhs, preferred_element_type=F32)


def unit_rms(vec, count):
    return vec * lax.rsqrt(jnp.sum(vec * vec, axis=-1, keepdims=True) / count + INNER_EPS)


def step_kernel(dims, res_in, norm_in, win_in, cw_in, cb_in, wx_in, wdt_in, dtb_in, al_in, dsk_in, wo_in, cs_in, ssm_in,
                res_out, conv_out, ssm_buf,
                res_ref, norm_ref, win_ref, cw_ref, cb_ref, wx_ref, wdt_ref, dtb_ref, al_ref, dsk_ref, wo_ref, cs_ref,
                w_buf, send_a, recv_a, send_b, recv_b, send_a2, recv_a2, send_b2, recv_b2, st_send, st_recv, st2_send, st2_recv, stat_t,
                p_send, p_recv, y_a, y_b, o_send, o_recv, sum_buf, res_buf, dt_buf, dx_buf, bc_buf, yv_buf, xc_buf,
                in_sems, *sem_refs):
    m_a, m_b, m_a2, m_b2, m_st, m_st2, m_p, m_ya, m_yb, m_ya2, m_yb2, m_o, m_s = [(sem_refs[2 * i], sem_refs[2 * i + 1]) for i in range(len(sem_refs) // 2)]
    n_z, n_y, n_ty, n_str, rows, layers, d_model, n_state, rank, order = dims
    tx, ty = lax.axis_index("tx"), lax.axis_index("ty")
    zi, yi = tx // n_y, tx % n_y
    chans = win_ref.shape[-1]
    half = chans // 2
    own_blocks = n_z * n_y // n_ty
    own_rows = own_blocks * rows
    group = n_y * rows
    pk = p_send.shape[1] - rows
    y1, z1, t1 = n_y - 1, n_z - 1, n_ty - 1
    scope = jax.named_scope

    def y_peer(off):
        return lax.rem(yi + off, n_y)

    def z_peer(off):
        return lax.rem(zi + off, n_z)

    def at_y(off):
        return {"tx": zi * n_y + y_peer(off), "ty": ty}

    def at_z(off):
        return {"tx": z_peer(off) * n_y + yi, "ty": ty}

    def at_ty(idx):
        return {"tx": tx, "ty": idx}

    def ty_peer(off):
        return at_ty(lax.rem(ty + off, n_ty))

    def send(src, dst, sems, slot, device):
        pltpu.make_async_remote_copy(src_ref=src, dst_ref=dst, send_sem=sems[0], recv_sem=sems[1].at[slot], device_id=device, device_id_type=MESH).start()

    def arrived(ref, sems, slot):
        pltpu.make_async_remote_copy(src_ref=ref, dst_ref=ref, send_sem=sems[0], recv_sem=sems[1].at[slot], device_id=ty_peer(1), device_id_type=MESH).wait_recv()

    def departed(ref, sems):
        pltpu.make_async_remote_copy(src_ref=ref, dst_ref=ref, send_sem=sems[0], recv_sem=sems[1].at[0], device_id=ty_peer(1), device_id_type=MESH).wait_send()

    def add_up(first, others):
        return functools.reduce(jnp.add, [o.astype(F32) for o in others], first.astype(F32))

    split = set()

    def split_weight(lyr, part):
        if (lyr, part) not in split:
            split.add((lyr, part))
            w_buf[lyr, part] = win_ref[lyr, :, part, :]

    def input_matmul(k, lyr, strm, source, part):
        split_weight(lyr, part)
        norm = norm_ref[lyr:lyr + 1, :]
        for zz in range(n_z):
            res = source[zz * n_y:(zz + 1) * n_y, strm].reshape(group, LANES)
            if part == 0:
                st_send[k, zz] = nt_dot(jnp.ones((8, LANES), F32), res * res, lax.Precision.HIGHEST)
            prod = nn_dot((res * norm).astype(BF16), w_buf[lyr, part]).astype(BF16)
            send_b[k, part, zz] = prod[:, half:]
            for yy in range(n_y):
                send_a[k, part, yy, zz * rows:(zz + 1) * rows, :] = prod[yy * rows:(yy + 1) * rows, :half]

    def phase_one(k, part):
        for off in range(1, n_z):
            if part == 0:
                send(st_send.at[k, z_peer(off)], st_recv.at[k, off - 1], m_st, k, at_z(off))
        for off in range(1, max(n_y, n_z)):
            if off < n_y:
                send(send_a.at[k, part, y_peer(off)], recv_a.at[k, part, off - 1], m_a, 2 * k + part, at_y(off))
            if off < n_z:
                send(send_b.at[k, part, z_peer(off)], recv_b.at[k, part, off - 1], m_b, 2 * k + part, at_z(off))

    def phase_two(k, part):
        if part == 0:
            arrived(st_recv.at[k], m_st, k)
            st2_send[k] = add_up(st_send[k, zi], [st_recv[k, off - 1] for off in range(1, n_z)])
            for off in range(1, n_y):
                send(st2_send.at[k], st2_recv.at[k, off - 1], m_st2, k, at_y(off))
        with scope(f"wait_a1_{part}"):
            arrived(recv_a.at[k, part], m_a, 2 * k + part)
        for zz in range(n_z):
            span = slice(zz * rows, (zz + 1) * rows)
            send_a2[k, part, zz] = add_up(send_a[k, part, yi, span, :], [recv_a[k, part, off - 1, span, :] for off in range(1, n_y)]).astype(BF16)
        for off in range(1, n_z):
            send(send_a2.at[k, part, z_peer(off)], recv_a2.at[k, part, off - 1], m_a2, 2 * k + part, at_z(off))
        with scope(f"wait_b1_{part}"):
            arrived(recv_b.at[k, part], m_b, 2 * k + part)
        for yy in range(n_y):
            span = slice(yy * rows, (yy + 1) * rows)
            send_b2[k, part, yy] = add_up(send_b[k, part, zi, span, :], [recv_b[k, part, off - 1, span, :] for off in range(1, n_z)]).astype(BF16)
        for off in range(1, n_y):
            send(send_b2.at[k, part, y_peer(off)], recv_b2.at[k, part, off - 1], m_b2, 2 * k + part, at_y(off))

    def finish_sum(k, part):
        with scope(f"wait_2_{part}"):
            arrived(recv_a2.at[k, part], m_a2, 2 * k + part)
            arrived(recv_b2.at[k, part], m_b2, 2 * k + part)
        tot_a = add_up(send_a2[k, part, zi], [recv_a2[k, part, off - 1] for off in range(1, n_z)])
        tot_b = add_up(send_b2[k, part, yi], [recv_b2[k, part, off - 1] for off in range(1, n_y)])
        return jnp.concatenate([tot_a, tot_b], axis=-1)

    def row_scale(k):
        arrived(st2_recv.at[k], m_st2, k)
        stat_t[k] = add_up(st2_send[k], [st2_recv[k, off - 1] for off in range(1, n_y)]).T
        mine = stat_t[k, pl.ds(pl.multiple_of(yi * rows, 8), rows), :][:, :1]
        return lax.rsqrt(mine / d_model + NORM_EPS)

    def conv_and_proj(k, lyr, mine, x_in):
        taps = [cs_ref[lyr, j, mine, :] for j in range(3)]
        conv_out[lyr, 0, mine, :] = taps[1]
        conv_out[lyr, 1, mine, :] = taps[2]
        conv_out[lyr, 2, mine, :] = x_in
        conv = x_in.astype(F32) * cw_ref[lyr, 3:4, :] + cb_ref[lyr:lyr + 1, :]
        for j in range(3):
            conv = conv + taps[j].astype(F32) * cw_ref[lyr, j:j + 1, :]
        x_conv = (conv * jax.nn.sigmoid(conv)).astype(BF16)
        xc_buf[k] = x_conv
        wx = wx_ref[lyr]
        bc_w = jnp.concatenate([wx[rank:], jnp.zeros((LANES - 2 * n_state, chans), BF16)], axis=0)
        bc_part = nt_dot(x_conv, bc_w)
        packed = bc_part[:pk]
        for q in range(1, rows // pk):
            packed = packed + pltpu.roll(bc_part[q * pk:(q + 1) * pk], q * 2 * n_state, 1)
        p_send[k, :rows] = nt_dot(x_conv, wx[:rank]).astype(BF16)
        p_send[k, rows:] = packed.astype(BF16)

    def step_sizes(k, lyr):
        proj = add_up(p_send[k], [p_recv[k, off - 1] for off in range(1, n_ty)])
        dt_low = unit_rms(proj[:rows], rank).astype(BF16)
        lane = lax.broadcasted_iota(jnp.int32, (pk, LANES), 1)
        for q in range(rows // pk):
            piece = proj[rows:]
            if q:
                piece = pltpu.roll(piece, LANES - q * 2 * n_state, 1)
            sq = piece * piece
            b_inv = lax.rsqrt(jnp.sum(jnp.where(lane < n_state, sq, 0.0), axis=-1, keepdims=True) / n_state + INNER_EPS)
            c_inv = lax.rsqrt(jnp.sum(jnp.where((lane >= n_state) & (lane < 2 * n_state), sq, 0.0), axis=-1, keepdims=True) / n_state + INNER_EPS)
            bc_buf[k, q * pk:(q + 1) * pk] = piece * jnp.where(lane < n_state, b_inv, c_inv)
        raw = nn_dot(dt_low, wdt_ref[lyr]) + dtb_ref[lyr:lyr + 1, :]
        delta = jnp.maximum(raw, 0.0) + jnp.log1p(jnp.exp(-jnp.abs(raw)))
        dt_buf[k] = delta
        dx_buf[k] = delta * xc_buf[k].astype(F32)

    def state_update(k, lyr, strm):
        neg_a = -jnp.exp(al_ref[lyr])

        def update(grp, carry):
            base = pl.multiple_of(grp * 8, 8)
            d_rows = dt_buf[k, pl.ds(base, 8), :]
            x_rows = dx_buf[k, pl.ds(base, 8), :]
            bc_t = bc_buf[k, pl.ds(base, 8), :].T
            outs = []
            for j in range(8):
                row = strm * rows + base + j
                decay = jnp.exp(d_rows[j:j + 1, :] * neg_a)
                state = decay * ssm_buf[lyr, row] + x_rows[j:j + 1, :] * bc_t[:n_state, j:j + 1]
                ssm_buf[lyr, row] = state
                outs.append(jnp.sum(state * bc_t[n_state:2 * n_state, j:j + 1], axis=0, keepdims=True))
            yv_buf[k, pl.ds(base, 8), :] = jnp.concatenate(outs, axis=0)
            return carry

        lax.fori_loop(0, rows // 8, update, 0)

    def push(buf, k, zz, yy, sems, slot, device):
        send(buf.at[k, zz, yy], buf.at[k, zz, yy], sems, slot, device)

    def main_thread(strm):
        mine = slice(strm * rows, (strm + 1) * rows)
        source = res_ref
        for lyr in range(layers):
            k = lyr * n_str + strm
            if lyr:
                source = gather_sums(k - n_str, lyr - 1, strm, source)
                with scope(f"matmul_{strm}"):
                    input_matmul(k, lyr, strm, source, 0)
            elif strm != order[0]:
                with scope(f"matmul_{strm}"):
                    input_matmul(k, lyr, strm, source, 0)
            sources[k] = source
            phase_one(k, 0)
            yield
            with scope(f"phase2_{strm}"):
                phase_two(k, 0)
            yield
            with scope(f"xconv_{strm}"):
                scale = row_scale(k)
                need(7)
                conv_and_proj(k, lyr, mine, (finish_sum(k, 0) * scale).astype(BF16))
            for off in range(1, n_ty):
                send(p_send.at[k], p_recv.at[k, off - 1], m_p, k, ty_peer(off))
            yield
            with scope(f"wait_p_{strm}"):
                arrived(p_recv.at[k], m_p, k)
            with scope(f"ssm_{strm}"):
                need(13 + lyr)
                step_sizes(k, lyr)
                state_update(k, lyr, strm)
            yield
            with scope(f"gate_{strm}"):
                z_in = (finish_sum(k, 1) * scale).astype(BF16).astype(F32)
                gated = ((yv_buf[k] + dsk_ref[lyr:lyr + 1, :] * xc_buf[k].astype(F32)) * (z_in * jax.nn.sigmoid(z_in))).astype(BF16)
                y_a[k, zi, yi] = gated[:, :half]
                y_b[k, zi, yi] = gated[:, half:]
            for off in range(1, n_y):
                push(y_a, k, zi, yi, m_ya, k * y1 + off - 1, at_y(off))
            for off in range(1, n_z):
                push(y_b, k, zi, yi, m_yb, k * z1 + off - 1, at_z(off))
            for out in range(1, n_z):
                push(y_a, k, zi, yi, m_ya2, k * z1 + out - 1, at_z(out))
            for out in range(1, n_y):
                push(y_b, k, zi, yi, m_yb2, k * n_z, at_y(out))
            yield
            with scope(f"fwd_{strm}"):
                for off in range(1, max(n_y, n_z)):
                    if off < n_y:
                        arrived(y_a.at[k, 0, 0], m_ya, k * y1 + off - 1)
                        for out in range(1, n_z):
                            push(y_a, k, zi, lax.rem(yi + n_y - off, n_y), m_ya2, k * z1 + out - 1, at_z(out))
                    if off < n_z:
                        arrived(y_b.at[k, 0, 0], m_yb, k * z1 + off - 1)
                        for out in range(1, n_y):
                            push(y_b, k, lax.rem(zi + n_z - off, n_z), yi, m_yb2, k * n_z + off, at_y(out))
            yield
            per_group = n_ty // n_z
            for off in range(n_z):
                with scope(f"outmm_{strm}_{off}"):
                    zz = lax.rem(zi + n_z - off, n_z)
                    if off:
                        arrived(y_a.at[k, 0], m_ya2, k * z1 + off - 1)
                    arrived(y_b.at[k, 0, :y1], m_yb2, k * n_z + off)
                    part = nn_dot(y_a[k, zz].reshape(group, half), wo_ref[lyr, :half]) + nn_dot(y_b[k, zz].reshape(group, half), wo_ref[lyr, half:])
                    for i in range(per_group):
                        o_send[k, zz * per_group + i] = part[i * own_rows:(i + 1) * own_rows].astype(BF16)
                    for i in range(per_group):
                        owner = zz * per_group + i
                        slot = lax.rem(owner - ty + n_ty - 1, n_ty)

                        @pl.when(owner != ty)
                        def _():
                            send(o_send.at[k, owner], o_recv.at[k, slot], m_o, k, at_ty(owner))

            yield
            with scope(f"wait_o_{strm}"):
                arrived(o_recv.at[k], m_o, k)
            sum_buf[k, ty] = add_up(o_send[k, ty], [o_recv[k, off - 1] for off in range(1, n_ty)]).astype(BF16)
            for off in range(1, n_ty):
                send(sum_buf.at[k, ty], sum_buf.at[k, ty], m_s, k, ty_peer(off))
            yield
        gather_sums(k, lyr, strm, source)

    def gather_sums(k, lyr, strm, source):
        with scope(f"wait_s_{strm}"):
            arrived(sum_buf.at[k, :t1], m_s, k)
        target = res_out if lyr == layers - 1 else res_buf
        for blk in range(n_ty):
            span = slice(blk * own_blocks, (blk + 1) * own_blocks)
            target[span, strm] = source[span, strm] + sum_buf[k, blk].astype(F32).reshape(own_blocks, rows, LANES)
        return target

    def gate_thread(strm):
        for lyr in range(layers):
            k = lyr * n_str + strm
            with scope(f"matmulz_{strm}"):
                input_matmul(k, lyr, strm, sources[k], 1)
            phase_one(k, 1)
            yield
            with scope(f"phase2z_{strm}"):
                phase_two(k, 1)
            yield

    sources = {}
    moves = [(res_in, res_ref), (norm_in, norm_ref), (win_in, win_ref), (cw_in, cw_ref), (cb_in, cb_ref), (cs_in, cs_ref), (wx_in, wx_ref),
             (wdt_in, wdt_ref), (dtb_in, dtb_ref), (al_in, al_ref), (dsk_in, dsk_ref), (wo_in, wo_ref)]
    moves += [(ssm_in.at[lyr], ssm_buf.at[lyr]) for lyr in range(layers)]
    loads = [pltpu.make_async_copy(src, dst, in_sems.at[i]) for i, (src, dst) in enumerate(moves)]
    for load in loads[:3]:
        load.start()

    barrier = pltpu.get_barrier_semaphore()
    for off in range(1, n_y):
        pl.semaphore_signal(barrier, inc=1, device_id=at_y(off), device_id_type=MESH)
    for off in range(1, n_z):
        pl.semaphore_signal(barrier, inc=1, device_id=at_z(off), device_id_type=MESH)
    for off in range(1, n_ty):
        pl.semaphore_signal(barrier, inc=1, device_id=ty_peer(off), device_id_type=MESH)

    def need(count):
        while len(moves) - len(loads) < count:
            loads.pop(0).wait()

    need(3)
    for load in loads:
        load.start()
    with scope("matmul_first"):
        input_matmul(order[0], 0, order[0], res_ref, 0)
    with scope("barrier"):
        pl.semaphore_wait(barrier, n_y + n_z + n_ty - 3)

    threads = {}
    for strm in range(n_str):
        threads[strm] = main_thread(strm)
        threads[GATE + strm] = gate_thread(strm)
    for name in order:
        next(threads[name], None)

    with scope("drain"):
        sent = [recv_a, recv_b, recv_a2, recv_b2, st_recv, st2_recv, p_recv, y_a.at[:, 0, :y1], y_b.at[:, 0, :z1],
                y_a.at[:, :z1], y_b.at[:, :, :y1], o_recv, sum_buf.at[:, :t1]]
        for ref, sems in zip(sent, [m_a, m_b, m_a2, m_b2, m_st, m_st2, m_p, m_ya, m_yb, m_ya2, m_yb2, m_o, m_s]):
            departed(ref, sems)


def store_kernel(res_ref, conv_ref, ssm_ref, res_out, conv_out, ssm_out, sems):
    copies = [pltpu.make_async_copy(src, dst, sems.at[i]) for i, (src, dst) in enumerate([(ssm_ref, ssm_out), (res_ref, res_out), (conv_ref, conv_out)])]
    for desc in copies:
        desc.start()
    for desc in copies:
        desc.wait()


def on_chip(shape, dtype):
    return pltpu.VMEM(shape, dtype)


def from_chip(array):
    return pltpu.with_memory_space_constraint(array, pltpu.VMEM)


def build(mesh, n_y, n_str, order):
    n_tx, n_ty = mesh.shape["tx"], mesh.shape["ty"]
    n_z = n_tx // n_y

    def local_step(residual, norm_w, w_in, conv_w, conv_b, w_x, w_dt, dt_bias, a_log, d_skip, w_out, conv_state, ssm_state):
        layers, batch, chans, n_state = ssm_state.shape
        rows = batch // n_str
        all_rows, d_local = residual.shape
        rank = w_dt.shape[1]
        half = chans // 2
        own = all_rows // n_ty // n_str
        pk = rows * 2 * n_state // LANES
        ks = layers * n_str
        dims = (n_z, n_y, n_ty, n_str, rows, layers, d_local * n_tx, n_state, rank, order)
        vmem = pl.BlockSpec(memory_space=pltpu.VMEM)
        anyspace = pl.BlockSpec(memory_space=pl.ANY)
        dma = pltpu.SemaphoreType.DMA
        res_shape = (n_tx, n_str, rows, d_local)
        conv_shape = (layers, 3, batch, chans)
        ssm_shape = (layers, batch, n_state, chans)
        operands = [
            residual.reshape(res_shape), norm_w, w_in, conv_w.transpose(0, 2, 1), conv_b, w_x.transpose(0, 2, 1), w_dt, dt_bias,
            a_log.transpose(0, 2, 1), d_skip, w_out, conv_state.transpose(0, 3, 1, 2), ssm_state.transpose(0, 1, 3, 2),
        ]
        scratch = [pltpu.VMEM(op.shape, op.dtype) for op in operands[:-1]]
        scratch += [
            pltpu.VMEM((layers, 2, d_local, chans), BF16),
            pltpu.VMEM((ks, 2, n_y, n_z * rows, half), BF16),
            pltpu.VMEM((ks, 2, n_y - 1, n_z * rows, half), BF16),
            pltpu.VMEM((ks, 2, n_z, n_y * rows, half), BF16),
            pltpu.VMEM((ks, 2, n_z - 1, n_y * rows, half), BF16),
            pltpu.VMEM((ks, 2, n_z, rows, half), BF16),
            pltpu.VMEM((ks, 2, n_z - 1, rows, half), BF16),
            pltpu.VMEM((ks, 2, n_y, rows, half), BF16),
            pltpu.VMEM((ks, 2, n_y - 1, rows, half), BF16),
            pltpu.VMEM((ks, n_z, 8, n_y * rows), F32),
            pltpu.VMEM((ks, n_z - 1, 8, n_y * rows), F32),
            pltpu.VMEM((ks, 8, n_y * rows), F32),
            pltpu.VMEM((ks, n_y - 1, 8, n_y * rows), F32),
            pltpu.VMEM((ks, n_y * rows, 8), F32),
            pltpu.VMEM((ks, rows + pk, LANES), BF16),
            pltpu.VMEM((ks, n_ty - 1, rows + pk, LANES), BF16),
            pltpu.VMEM((ks, n_z, n_y, rows, half), BF16),
            pltpu.VMEM((ks, n_z, n_y, rows, half), BF16),
            pltpu.VMEM((ks, n_ty, own, d_local), BF16),
            pltpu.VMEM((ks, n_ty - 1, own, d_local), BF16),
            pltpu.VMEM((ks, n_ty, own, d_local), BF16),
            pltpu.VMEM(res_shape, F32),
            pltpu.VMEM((ks, rows, chans), F32),
            pltpu.VMEM((ks, rows, chans), F32),
            pltpu.VMEM((ks, rows, LANES), F32),
            pltpu.VMEM((ks, rows, chans), F32),
            pltpu.VMEM((ks, rows, chans), BF16),
        ]
        y1, z1, t1 = n_y - 1, n_z - 1, n_ty - 1
        scratch += [dma((len(operands) - 1 + layers,))]
        for count in [2 * ks, 2 * ks, 2 * ks, 2 * ks, ks, ks, ks, ks * y1, ks * z1, ks * z1, ks * n_z, ks, ks]:
            scratch += [dma, dma((count,))]
        res, conv, ssm = pl.pallas_call(
            functools.partial(step_kernel, dims),
            out_shape=(on_chip(res_shape, F32), on_chip(conv_shape, BF16), on_chip(ssm_shape, F32)),
            in_specs=[pl.BlockSpec(memory_space=pltpu.HBM)] * len(operands),
            out_specs=(vmem, vmem, vmem),
            scratch_shapes=scratch,
            compiler_params=pltpu.CompilerParams(collective_id=0, has_side_effects=True, vmem_limit_bytes=VMEM_LIMIT),
        )(*operands)
        res, conv, ssm = pl.pallas_call(
            store_kernel,
            out_shape=(jax.ShapeDtypeStruct(res_shape, F32), jax.ShapeDtypeStruct(conv_shape, BF16), jax.ShapeDtypeStruct(ssm_shape, F32)),
            in_specs=[vmem] * 3,
            out_specs=(anyspace,) * 3,
            scratch_shapes=[dma((3,))],
            compiler_params=pltpu.CompilerParams(vmem_limit_bytes=16 * 1024 * 1024),
        )(*(from_chip(out) for out in (res, conv, ssm)))
        return res.reshape(all_rows, d_local), conv.transpose(0, 2, 3, 1), ssm.transpose(0, 1, 3, 2)

    cache_spec = P(None, ("dp", "tx"), "ty", None)
    in_specs = (P("dp", "tx"), P(None, "tx"), P(None, "tx", None, "ty"), P(None, "ty", None), P(None, "ty"), P(None, "ty", None), P(None, None, "ty"), P(None, "ty"), P(None, "ty", None), P(None, "ty"), P(None, "ty", "tx"), cache_spec, cache_spec)
    out_specs = (P("dp", "tx"), cache_spec, cache_spec)
    return jax.shard_map(local_step, mesh=mesh, in_specs=in_specs, out_specs=out_specs, check_vma=False)


def solution(mesh):
    return build(mesh, 4, STREAMS, ORDER)
```

```python
import functools

import jax
import jax.numpy as jnp
from jax import lax
from jax.experimental import pallas as pl
from jax.experimental.pallas import tpu as pltpu
from jax.sharding import PartitionSpec as P

NORM_EPS = 1e-5
INNER_EPS = 1e-6
MESH = pl.DeviceIdType.MESH
F32 = jnp.float32
BF16 = jnp.bfloat16
LANES = 128
GATE = 10
WEIGHT = 20
W_IN = 30
PIECES = 4
CUT = 2
STREAMS = 4
ORDER = (
    0, 1, 3, 0, 2, 1, 10, 11, 13, 1, 2, 0, 3, 12, 20, 13, 10, 30, 11, 2, 1, 30, 20, 0,
    3, 12, 20, 30, 2, 0, 20, 1, 3, 3, 2, 30, 30, 20, 0, 1, 3, 2, 30, 30, 0, 20, 1, 30,
    20, 3, 2, 0, 1, 3, 2, 0, 1, 3, 2, 0, 10, 11, 1, 13, 3, 2, 12, 20, 0, 0, 1, 1,
    3, 3, 2, 2, 0, 1, 3, 2, 0, 1, 3, 2, 1, 0, 3, 2,
)
VMEM_LIMIT = 52 * 1024 * 1024


def nt_dot(lhs, rhs, precision=None):
    return lax.dot_general(lhs, rhs, (((1,), (1,)), ((), ())), precision=precision, preferred_element_type=F32)


def nn_dot(lhs, rhs):
    return jnp.dot(lhs, rhs, preferred_element_type=F32)


def unit_rms(vec, count):
    return vec * lax.rsqrt(jnp.sum(vec * vec, axis=-1, keepdims=True) / count + INNER_EPS)


def step_kernel(dims, res_in, norm_in, win_in, cw_in, cb_in, wx_in, wdt_in, dtb_in, al_in, dsk_in, wo_in, cs_in, ssm_in,
                res_out, conv_out, ssm_buf,
                res_ref, norm_ref, win_ref, cw_ref, cb_ref, wx_ref, wdt_ref, dtb_ref, al_ref, dsk_ref, wo_ref, cs_ref,
                w_all, h_send, h_all, sth_send, sth_recv, stz_send, stz_recv, g_send, g_recv, send_a, recv_a, send_b, recv_b, send_a2, recv_a2, send_b2, recv_b2, st_send, st_recv, st2_send, st2_recv, stat_t,
                p_send, p_recv, y_buf, o_send, o_recv, sum_buf, res_buf, dt_buf, dx_buf, bc_buf, yv_buf, xc_buf,
                in_sems, *sem_refs):
    m_a, m_b, m_a2, m_b2, m_st, m_st2, m_p, m_y, m_o, m_s, m_w, m_h, m_sth, m_stz, m_g, m_i = [(sem_refs[2 * i], sem_refs[2 * i + 1]) for i in range(len(sem_refs) // 2)]
    n_z, n_y, n_ty, n_str, rows, layers, d_model, n_state, rank, order = dims
    tx, ty = lax.axis_index("tx"), lax.axis_index("ty")
    zi, yi = tx // n_y, tx % n_y
    chans = win_ref.shape[-1]
    cut = chans * CUT // 4
    group = n_y * rows
    own_rows = group // n_ty
    pk = p_send.shape[1] - rows
    y1, z1, t1 = n_y - 1, n_z - 1, n_ty - 1
    scope = jax.named_scope

    def y_peer(off):
        return lax.rem(yi + off, n_y)

    def z_peer(off):
        return lax.rem(zi + off, n_z)

    def at_y(off):
        return {"tx": zi * n_y + y_peer(off), "ty": ty}

    def at_z(off):
        return {"tx": z_peer(off) * n_y + yi, "ty": ty}

    def at_ty(idx):
        return {"tx": tx, "ty": idx}

    def ty_peer(off):
        return at_ty(lax.rem(ty + off, n_ty))

    def send(src, dst, sems, slot, device):
        pltpu.make_async_remote_copy(src_ref=src, dst_ref=dst, send_sem=sems[0], recv_sem=sems[1].at[slot], device_id=device, device_id_type=MESH).start()

    def arrived(ref, sems, slot):
        pltpu.make_async_remote_copy(src_ref=ref, dst_ref=ref, send_sem=sems[0], recv_sem=sems[1].at[slot], device_id=ty_peer(1), device_id_type=MESH).wait_recv()

    def departed(ref, sems):
        pltpu.make_async_remote_copy(src_ref=ref, dst_ref=ref, send_sem=sems[0], recv_sem=sems[1].at[0], device_id=ty_peer(1), device_id_type=MESH).wait_send()

    def add_up(first, others):
        return functools.reduce(jnp.add, [o.astype(F32) for o in others], first.astype(F32))

    split = set()

    def split_weight(lyr, part):
        if (lyr, part) not in split:
            split.add((lyr, part))
            need(("win", lyr))
            w_all[lyr, part, yi] = win_ref[lyr, :, part, :]

    def input_matmul(k, lyr, strm, source, part):
        split_weight(lyr, part)
        need(("res", strm))
        norm = norm_ref[lyr:lyr + 1, :]
        for zz in range(n_z):
            res = source[zz, :, strm].reshape(group, LANES)
            if part == 0:
                st_send[k, zz] = nt_dot(jnp.ones((8, LANES), F32), res * res, lax.Precision.HIGHEST)
            prod = nn_dot((res * norm).astype(BF16), w_all[lyr, part, yi]).astype(BF16)
            send_b[k, part, zz] = prod[:, cut:]
            for yy in range(n_y):
                send_a[k, part, yy, zz * rows:(zz + 1) * rows, :] = prod[yy * rows:(yy + 1) * rows, :cut]

    def phase_one(k, part):
        for off in range(1, n_z):
            if part == 0:
                send(st_send.at[k, z_peer(off)], st_recv.at[k, off - 1], m_st, k, at_z(off))
        for off in range(1, max(n_y, n_z)):
            if off < n_y:
                send(send_a.at[k, part, y_peer(off)], recv_a.at[k, part, off - 1], m_a, 2 * k + part, at_y(off))
            if off < n_z:
                send(send_b.at[k, part, z_peer(off)], recv_b.at[k, part, off - 1], m_b, 2 * k + part, at_z(off))

    def phase_two(k, part):
        if part == 0:
            arrived(st_recv.at[k], m_st, k)
            st2_send[k] = add_up(st_send[k, zi], [st_recv[k, off - 1] for off in range(1, n_z)])
            for off in range(1, n_y):
                send(st2_send.at[k], st2_recv.at[k, off - 1], m_st2, k, at_y(off))
        with scope(f"wait_a1_{part}"):
            arrived(recv_a.at[k, part], m_a, 2 * k + part)
        for zz in range(n_z):
            span = slice(zz * rows, (zz + 1) * rows)
            send_a2[k, part, zz] = add_up(send_a[k, part, yi, span, :], [recv_a[k, part, off - 1, span, :] for off in range(1, n_y)]).astype(BF16)
        for off in range(1, n_z):
            send(send_a2.at[k, part, z_peer(off)], recv_a2.at[k, part, off - 1], m_a2, 2 * k + part, at_z(off))
        with scope(f"wait_b1_{part}"):
            arrived(recv_b.at[k, part], m_b, 2 * k + part)
        for yy in range(n_y):
            span = slice(yy * rows, (yy + 1) * rows)
            send_b2[k, part, yy] = add_up(send_b[k, part, zi, span, :], [recv_b[k, part, off - 1, span, :] for off in range(1, n_z)]).astype(BF16)
        for off in range(1, n_y):
            send(send_b2.at[k, part, y_peer(off)], recv_b2.at[k, part, off - 1], m_b2, 2 * k + part, at_y(off))

    def finish_sum(k, part):
        if k >= n_str:
            kh = k - n_str
            with scope(f"wait_g_{part}"):
                arrived(g_recv.at[kh, part], m_g, 2 * kh + part)
            return add_up(g_send[kh, part, zi], [g_recv[kh, part, off - 1] for off in range(1, n_z)])
        with scope(f"wait_2_{part}"):
            arrived(recv_a2.at[k, part], m_a2, 2 * k + part)
            arrived(recv_b2.at[k, part], m_b2, 2 * k + part)
        tot_a = add_up(send_a2[k, part, zi], [recv_a2[k, part, off - 1] for off in range(1, n_z)])
        tot_b = add_up(send_b2[k, part, yi], [recv_b2[k, part, off - 1] for off in range(1, n_y)])
        return jnp.concatenate([tot_a, tot_b], axis=-1)

    def row_scale(k):
        if k >= n_str:
            kh = k - n_str
            arrived(stz_recv.at[kh], m_stz, kh)
            total, place = add_up(stz_send[kh], [stz_recv[kh, off - 1] for off in range(1, n_z)]), zi
        else:
            arrived(st2_recv.at[k], m_st2, k)
            total, place = add_up(st2_send[k], [st2_recv[k, off - 1] for off in range(1, n_y)]), yi
        stat_t[k] = total.T
        mine = stat_t[k, pl.ds(pl.multiple_of(place * rows, 8), rows), :][:, :1]
        return lax.rsqrt(mine / d_model + NORM_EPS)

    def spread_hidden(k, lyr, strm, source):
        kh = k - n_str
        norm = norm_ref[lyr:lyr + 1, :]
        for yy in range(n_y):
            res = source[:, yy, strm].reshape(n_z * rows, LANES)
            sth_send[kh, yy] = nt_dot(jnp.ones((8, LANES), F32), res * res, lax.Precision.HIGHEST)
            h_send[kh, yy] = (res * norm).astype(BF16)
        for off in range(1, n_y):
            send(h_send.at[kh, y_peer(off)], h_all.at[kh, yi], m_h, kh, at_y(off))
            send(sth_send.at[kh, y_peer(off)], sth_recv.at[kh, off - 1], m_sth, kh, at_y(off))
        h_all[kh, yi] = h_send[kh, yi]

    def slab_matmul(k, lyr, part):
        kh = k - n_str
        if part == 0:
            with scope(f"wait_h"):
                arrived(h_all.at[kh, :y1], m_h, kh)
                arrived(sth_recv.at[kh], m_sth, kh)
            stz_send[kh] = add_up(sth_send[kh, yi], [sth_recv[kh, off - 1] for off in range(1, n_y)])
            for off in range(1, n_z):
                send(stz_send.at[kh], stz_recv.at[kh, off - 1], m_stz, kh, at_z(off))
        if (lyr, part) not in gathered:
            gathered.add((lyr, part))
            with scope(f"wait_i"):
                arrived(w_all.at[lyr, part, :y1], m_i, 2 * (lyr - 1) + part)
        hidden = jnp.concatenate([h_all[kh, yy] for yy in range(n_y)], axis=1)
        prod = nn_dot(hidden, w_all[lyr, part].reshape(n_y * LANES, chans))
        g_send[kh, part] = prod.astype(BF16).reshape(n_z, rows, chans)
        for off in range(1, n_z):
            send(g_send.at[kh, part, z_peer(off)], g_recv.at[kh, part, off - 1], m_g, 2 * kh + part, at_z(off))

    def conv_and_proj(k, lyr, mine, x_in):
        taps = [cs_ref[lyr, j, mine, :] for j in range(3)]
        conv_out[lyr, 0, mine, :] = taps[1]
        conv_out[lyr, 1, mine, :] = taps[2]
        conv_out[lyr, 2, mine, :] = x_in
        conv = x_in.astype(F32) * cw_ref[lyr, 3:4, :] + cb_ref[lyr:lyr + 1, :]
        for j in range(3):
            conv = conv + taps[j].astype(F32) * cw_ref[lyr, j:j + 1, :]
        x_conv = (conv * jax.nn.sigmoid(conv)).astype(BF16)
        xc_buf[k] = x_conv
        wx = wx_ref[lyr]
        bc_w = jnp.concatenate([wx[rank:], jnp.zeros((LANES - 2 * n_state, chans), BF16)], axis=0)
        bc_part = nt_dot(x_conv, bc_w)
        packed = bc_part[:pk]
        for q in range(1, rows // pk):
            packed = packed + pltpu.roll(bc_part[q * pk:(q + 1) * pk], q * 2 * n_state, 1)
        p_send[k, :rows] = nt_dot(x_conv, wx[:rank]).astype(BF16)
        p_send[k, rows:] = packed.astype(BF16)

    def step_sizes(k, lyr):
        proj = add_up(p_send[k], [p_recv[k, off - 1] for off in range(1, n_ty)])
        dt_low = unit_rms(proj[:rows], rank).astype(BF16)
        lane = lax.broadcasted_iota(jnp.int32, (pk, LANES), 1)
        for q in range(rows // pk):
            piece = proj[rows:]
            if q:
                piece = pltpu.roll(piece, LANES - q * 2 * n_state, 1)
            sq = piece * piece
            b_inv = lax.rsqrt(jnp.sum(jnp.where(lane < n_state, sq, 0.0), axis=-1, keepdims=True) / n_state + INNER_EPS)
            c_inv = lax.rsqrt(jnp.sum(jnp.where((lane >= n_state) & (lane < 2 * n_state), sq, 0.0), axis=-1, keepdims=True) / n_state + INNER_EPS)
            bc_buf[k, q * pk:(q + 1) * pk] = piece * jnp.where(lane < n_state, b_inv, c_inv)
        raw = nn_dot(dt_low, wdt_ref[lyr]) + dtb_ref[lyr:lyr + 1, :]
        delta = jnp.maximum(raw, 0.0) + jnp.log1p(jnp.exp(-jnp.abs(raw)))
        dt_buf[k] = delta
        dx_buf[k] = delta * xc_buf[k].astype(F32)

    def state_update(k, lyr, strm):
        neg_a = -jnp.exp(al_ref[lyr])

        def update(grp, carry):
            base = pl.multiple_of(grp * 8, 8)
            d_rows = dt_buf[k, pl.ds(base, 8), :]
            x_rows = dx_buf[k, pl.ds(base, 8), :]
            bc_t = bc_buf[k, pl.ds(base, 8), :].T
            outs = []
            for j in range(8):
                row = strm * rows + base + j
                decay = jnp.exp(d_rows[j:j + 1, :] * neg_a)
                state = decay * ssm_buf[lyr, row] + x_rows[j:j + 1, :] * bc_t[:n_state, j:j + 1]
                ssm_buf[lyr, row] = state
                outs.append(jnp.sum(state * bc_t[n_state:2 * n_state, j:j + 1], axis=0, keepdims=True))
            yv_buf[k, pl.ds(base, 8), :] = jnp.concatenate(outs, axis=0)
            return carry

        lax.fori_loop(0, rows // 8, update, 0)

    def main_thread(strm):
        mine = slice(strm * rows, (strm + 1) * rows)
        source = res_ref
        for lyr in range(layers):
            k = lyr * n_str + strm
            if lyr:
                source = gather_sums(k - n_str, lyr - 1, strm, source)
                with scope(f"hidden_{strm}"):
                    spread_hidden(k, lyr, strm, source)
                yield
                with scope(f"slab_{strm}"):
                    slab_matmul(k, lyr, 0)
            else:
                if strm != lead:
                    with scope(f"matmul_{strm}"):
                        input_matmul(k, lyr, strm, source, 0)
                phase_one(k, 0)
                yield
                with scope(f"phase2_{strm}"):
                    phase_two(k, 0)
            yield
            with scope(f"xconv_{strm}"):
                scale = row_scale(k)
                need("cw", "cb", "cs", "wx")
                conv_and_proj(k, lyr, mine, (finish_sum(k, 0) * scale).astype(BF16))
            for off in range(1, n_ty):
                send(p_send.at[k], p_recv.at[k, off - 1], m_p, k, ty_peer(off))
            yield
            with scope(f"wait_p_{strm}"):
                arrived(p_recv.at[k], m_p, k)
            with scope(f"ssm_{strm}"):
                need("wdt", "dtb", "al", "dsk", ("ssm", lyr))
                step_sizes(k, lyr)
                state_update(k, lyr, strm)
            yield
            with scope(f"gate_{strm}"):
                z_in = (finish_sum(k, 1) * scale).astype(BF16).astype(F32)
                gated = ((yv_buf[k] + dsk_ref[lyr:lyr + 1, :] * xc_buf[k].astype(F32)) * (z_in * jax.nn.sigmoid(z_in))).astype(BF16)
                y_buf[k, yi] = gated
            for off in range(1, n_y):
                send(y_buf.at[k, yi], y_buf.at[k, yi], m_y, k, at_y(off))
            yield
            with scope(f"wait_y_{strm}"):
                arrived(y_buf.at[k, :y1], m_y, k)
            with scope(f"outmm_{strm}"):
                if lyr not in gathered:
                    gathered.add(lyr)
                    arrived(wo_ref.at[lyr, :z1], m_w, lyr)
                everyone = y_buf[k].reshape(group, chans)
                for off in range(n_z):
                    zz = z_peer(off)
                    o_send[k, zz] = nn_dot(everyone, wo_ref[lyr, zz]).reshape(n_ty, own_rows, LANES).astype(BF16)
                    for step in range(n_ty):
                        owner = lax.rem(ty + step, n_ty)
                        if off or step:
                            send(o_send.at[k, zz, owner], o_recv.at[k, zi * n_ty + ty], m_o, k, {"tx": zz * n_y + yi, "ty": owner})
                o_recv[k, zi * n_ty + ty] = o_send[k, zi, ty]
            yield
            with scope(f"wait_o_{strm}"):
                arrived(o_recv.at[k, :n_z * n_ty - 1], m_o, k)
            parts = o_recv[k].astype(F32).reshape(n_z, n_ty, own_rows, LANES)
            sum_buf[k, ty] = functools.reduce(jnp.add, [parts[:, i] for i in range(n_ty)]).astype(BF16)
            for off in range(1, n_ty):
                send(sum_buf.at[k, ty], sum_buf.at[k, ty], m_s, k, ty_peer(off))
            yield
        gather_sums(k, lyr, strm, source)

    def gather_sums(k, lyr, strm, source):
        with scope(f"wait_s_{strm}"):
            arrived(sum_buf.at[k, :t1], m_s, k)
        target = res_out if lyr == layers - 1 else res_buf
        for owner in range(n_ty):
            blk, low = owner * own_rows // rows, owner * own_rows % rows
            span = slice(low, low + own_rows)
            target[:, blk, strm, span, :] = source[:, blk, strm, span, :] + sum_buf[k, owner].astype(F32)
        return target

    def gate_thread(strm):
        for lyr in range(layers):
            k = lyr * n_str + strm
            if lyr:
                with scope(f"slabz_{strm}"):
                    slab_matmul(k, lyr, 1)
                yield
                continue
            with scope(f"matmulz_{strm}"):
                input_matmul(k, lyr, strm, res_ref, 1)
            phase_one(k, 1)
            yield
            with scope(f"phase2z_{strm}"):
                phase_two(k, 1)
            yield

    def weight_thread():
        for lyr in range(layers):
            for piece in range(PIECES):
                if piece == 0:
                    need(("wo", lyr))
                span = pl.ds(piece * width, width)
                for off in range(1, n_z):
                    send(wo_ref.at[lyr, zi, span], wo_ref.at[lyr, zi, span], m_w, lyr, at_z(off))
                yield

    def w_in_thread():
        for lyr in range(1, layers):
            for part in range(2):
                split_weight(lyr, part)
                for piece in range(PIECES):
                    span = pl.ds(piece * LANES // PIECES, LANES // PIECES)
                    for off in range(1, n_y):
                        send(w_all.at[lyr, part, yi, span], w_all.at[lyr, part, yi, span], m_i, 2 * (lyr - 1) + part, at_y(off))
                    yield

    gathered = set()
    width = chans // PIECES
    lead = next(name for name in order if name < GATE)
    moves = {("res", lead): (res_in.at[:, :, lead], res_ref.at[:, :, lead]), "norm": (norm_in, norm_ref), ("win", 0): (win_in.at[0], win_ref.at[0])}
    first = len(moves)
    moves.update({("res", strm): (res_in.at[:, :, strm], res_ref.at[:, :, strm]) for strm in range(n_str) if strm != lead})
    moves.update({"cw": (cw_in, cw_ref), "cb": (cb_in, cb_ref), "cs": (cs_in, cs_ref), "wx": (wx_in, wx_ref), "wdt": (wdt_in, wdt_ref)})
    moves.update({"dtb": (dtb_in, dtb_ref), "al": (al_in, al_ref), "dsk": (dsk_in, dsk_ref)})
    second = len(moves)
    moves.update({("wo", lyr): (wo_in.at[lyr], wo_ref.at[lyr, zi]) for lyr in range(layers)})
    moves.update({("win", lyr): (win_in.at[lyr], win_ref.at[lyr]) for lyr in range(1, layers)})
    moves.update({("ssm", lyr): (ssm_in.at[lyr], ssm_buf.at[lyr]) for lyr in range(layers)})
    loads = {name: pltpu.make_async_copy(src, dst, in_sems.at[i]) for i, (name, (src, dst)) in enumerate(moves.items())}
    for name in list(loads)[:first]:
        loads[name].start()
    rest, late = list(loads)[first:second], list(loads)[second:]

    def need(*names):
        for name in names:
            if name in loads:
                loads.pop(name).wait()

    barrier = pltpu.get_barrier_semaphore()
    peers = [at_y(off) for off in range(1, n_y)] + [at_z(off) for off in range(1, n_z)] + [ty_peer(off) for off in range(1, n_ty)]
    for peer in peers:
        pl.semaphore_signal(barrier, inc=1, device_id=peer, device_id_type=MESH)
    need(("res", lead), "norm", ("win", 0))
    for name in rest:
        loads[name].start()
    with scope("matmul_first"):
        input_matmul(lead, 0, lead, res_ref, 0)
    with scope("barrier"):
        pl.semaphore_wait(barrier, len(peers))

    threads = {}
    for strm in range(n_str):
        threads[strm] = main_thread(strm)
        threads[GATE + strm] = gate_thread(strm)
    threads[WEIGHT] = weight_thread()
    threads[W_IN] = w_in_thread()
    for turn, name in enumerate(order):
        if turn == n_str:
            for load in late:
                loads[load].start()
        next(threads[name], None)

    with scope("drain"):
        sent = [recv_a, recv_b, recv_a2, recv_b2, st_recv, st2_recv, p_recv, y_buf.at[:, :y1], o_recv.at[:, :n_z * n_ty - 1], sum_buf.at[:, :t1], wo_ref.at[:, :z1],
                h_all.at[:, :y1], sth_recv, stz_recv, g_recv, w_all.at[1:, :, :y1]]
        for ref, sems in zip(sent, [m_a, m_b, m_a2, m_b2, m_st, m_st2, m_p, m_y, m_o, m_s, m_w, m_h, m_sth, m_stz, m_g, m_i]):
            departed(ref, sems)


def store_kernel(res_ref, conv_ref, ssm_ref, res_out, conv_out, ssm_out, sems):
    copies = [pltpu.make_async_copy(src, dst, sems.at[i]) for i, (src, dst) in enumerate([(ssm_ref, ssm_out), (res_ref, res_out), (conv_ref, conv_out)])]
    for desc in copies:
        desc.start()
    for desc in copies:
        desc.wait()


def on_chip(shape, dtype):
    return pltpu.VMEM(shape, dtype)


def from_chip(array):
    return pltpu.with_memory_space_constraint(array, pltpu.VMEM)


def build(mesh, n_y, n_str, order):
    n_tx, n_ty = mesh.shape["tx"], mesh.shape["ty"]
    n_z = n_tx // n_y

    def local_step(residual, norm_w, w_in, conv_w, conv_b, w_x, w_dt, dt_bias, a_log, d_skip, w_out, conv_state, ssm_state):
        layers, batch, chans, n_state = ssm_state.shape
        rows = batch // n_str
        all_rows, d_local = residual.shape
        rank = w_dt.shape[1]
        cut = chans * CUT // 4
        own = n_y * rows // n_ty
        pk = rows * 2 * n_state // LANES
        ks = layers * n_str
        kh = ks - n_str
        dims = (n_z, n_y, n_ty, n_str, rows, layers, d_local * n_tx, n_state, rank, order)
        vmem = pl.BlockSpec(memory_space=pltpu.VMEM)
        anyspace = pl.BlockSpec(memory_space=pl.ANY)
        dma = pltpu.SemaphoreType.DMA
        res_shape = (n_z, n_y, n_str, rows, d_local)
        conv_shape = (layers, 3, batch, chans)
        ssm_shape = (layers, batch, n_state, chans)
        operands = [
            residual.reshape(res_shape), norm_w, w_in, conv_w.transpose(0, 2, 1), conv_b, w_x.transpose(0, 2, 1), w_dt, dt_bias,
            a_log.transpose(0, 2, 1), d_skip, w_out, conv_state.transpose(0, 3, 1, 2), ssm_state.transpose(0, 1, 3, 2),
        ]
        shapes = [op.shape for op in operands[:-1]]
        shapes[10] = (layers, n_z, chans, d_local)
        scratch = [pltpu.VMEM(shape, op.dtype) for shape, op in zip(shapes, operands)]
        scratch += [
            pltpu.VMEM((layers, 2, n_y, d_local, chans), BF16),
            pltpu.VMEM((kh, n_y, n_z * rows, d_local), BF16),
            pltpu.VMEM((kh, n_y, n_z * rows, d_local), BF16),
            pltpu.VMEM((kh, n_y, 8, n_z * rows), F32),
            pltpu.VMEM((kh, n_y - 1, 8, n_z * rows), F32),
            pltpu.VMEM((kh, 8, n_z * rows), F32),
            pltpu.VMEM((kh, n_z - 1, 8, n_z * rows), F32),
            pltpu.VMEM((kh, 2, n_z, rows, chans), BF16),
            pltpu.VMEM((kh, 2, n_z - 1, rows, chans), BF16),
            pltpu.VMEM((n_str, 2, n_y, n_z * rows, cut), BF16),
            pltpu.VMEM((n_str, 2, n_y - 1, n_z * rows, cut), BF16),
            pltpu.VMEM((n_str, 2, n_z, n_y * rows, chans - cut), BF16),
            pltpu.VMEM((n_str, 2, n_z - 1, n_y * rows, chans - cut), BF16),
            pltpu.VMEM((n_str, 2, n_z, rows, cut), BF16),
            pltpu.VMEM((n_str, 2, n_z - 1, rows, cut), BF16),
            pltpu.VMEM((n_str, 2, n_y, rows, chans - cut), BF16),
            pltpu.VMEM((n_str, 2, n_y - 1, rows, chans - cut), BF16),
            pltpu.VMEM((n_str, n_z, 8, n_y * rows), F32),
            pltpu.VMEM((n_str, n_z - 1, 8, n_y * rows), F32),
            pltpu.VMEM((n_str, 8, n_y * rows), F32),
            pltpu.VMEM((n_str, n_y - 1, 8, n_y * rows), F32),
            pltpu.VMEM((ks, n_y * rows, 8), F32),
            pltpu.VMEM((ks, rows + pk, LANES), BF16),
            pltpu.VMEM((ks, n_ty - 1, rows + pk, LANES), BF16),
            pltpu.VMEM((ks, n_y, rows, chans), BF16),
            pltpu.VMEM((ks, n_z, n_ty, own, d_local), BF16),
            pltpu.VMEM((ks, n_z * n_ty, own, d_local), BF16),
            pltpu.VMEM((ks, n_ty, n_z, own, d_local), BF16),
            pltpu.VMEM(res_shape, F32),
            pltpu.VMEM((ks, rows, chans), F32),
            pltpu.VMEM((ks, rows, chans), F32),
            pltpu.VMEM((ks, rows, LANES), F32),
            pltpu.VMEM((ks, rows, chans), F32),
            pltpu.VMEM((ks, rows, chans), BF16),
        ]
        scratch += [dma((len(operands) + n_str + 3 * layers,))]
        for count in [2 * n_str, 2 * n_str, 2 * n_str, 2 * n_str, n_str, n_str, ks, ks, ks, ks, layers, kh, kh, kh, 2 * kh, 2 * (layers - 1)]:
            scratch += [dma, dma((count,))]
        res, conv, ssm = pl.pallas_call(
            functools.partial(step_kernel, dims),
            out_shape=(on_chip(res_shape, F32), on_chip(conv_shape, BF16), on_chip(ssm_shape, F32)),
            in_specs=[pl.BlockSpec(memory_space=pltpu.HBM)] * len(operands),
            out_specs=(vmem, vmem, vmem),
            scratch_shapes=scratch,
            compiler_params=pltpu.CompilerParams(collective_id=0, has_side_effects=True, vmem_limit_bytes=VMEM_LIMIT),
        )(*operands)
        res, conv, ssm = pl.pallas_call(
            store_kernel,
            out_shape=(jax.ShapeDtypeStruct(res_shape, F32), jax.ShapeDtypeStruct(conv_shape, BF16), jax.ShapeDtypeStruct(ssm_shape, F32)),
            in_specs=[vmem] * 3,
            out_specs=(anyspace,) * 3,
            scratch_shapes=[dma((3,))],
            compiler_params=pltpu.CompilerParams(vmem_limit_bytes=16 * 1024 * 1024),
        )(*(from_chip(out) for out in (res, conv, ssm)))
        return res.reshape(all_rows, d_local), conv.transpose(0, 2, 3, 1), ssm.transpose(0, 1, 3, 2)

    cache_spec = P(None, ("dp", "tx"), "ty", None)
    in_specs = (P("dp", "tx"), P(None, "tx"), P(None, "tx", None, "ty"), P(None, "ty", None), P(None, "ty"), P(None, "ty", None), P(None, None, "ty"), P(None, "ty"), P(None, "ty", None), P(None, "ty"), P(None, "ty", "tx"), cache_spec, cache_spec)
    out_specs = (P("dp", "tx"), cache_spec, cache_spec)
    return jax.shard_map(local_step, mesh=mesh, in_specs=in_specs, out_specs=out_specs, check_vma=False)


def solution(mesh):
    return build(mesh, 4, STREAMS, ORDER)
```

```python
import functools

import jax
import jax.numpy as jnp
from jax import lax
from jax.experimental import pallas as pl
from jax.experimental.pallas import tpu as pltpu
from jax.sharding import PartitionSpec as P

NORM_EPS = 1e-5
INNER_EPS = 1e-6
MESH = pl.DeviceIdType.MESH
F32 = jnp.float32
BF16 = jnp.bfloat16
LANES = 128
GATE = 10
WEIGHT = 20
W_IN = 30
PIECES = 4
CUT = 2
STREAMS = 4
ORDER = (
    1, 2, 11, 3, 1, 0, 20, 30, 2, 1, 3, 11, 13, 20, 0, 10, 3, 12, 1, 30, 13, 30, 2, 20,
    0, 20, 10, 3, 1, 12, 20, 2, 3, 0, 0, 20, 2, 1, 30, 3, 30, 30, 0, 2, 1, 20, 20, 3,
    0, 2, 30, 30, 1, 3, 0, 2, 1, 3, 13, 0, 11, 2, 10, 12, 1, 3, 3, 1, 0, 0, 2, 2,
    3, 1, 0, 2, 3, 1, 0, 2, 1, 0, 3, 2,
)
STORES = 1
VMEM_LIMIT = 52 * 1024 * 1024


def nt_dot(lhs, rhs, precision=None):
    return lax.dot_general(lhs, rhs, (((1,), (1,)), ((), ())), precision=precision, preferred_element_type=F32)


def nn_dot(lhs, rhs):
    return jnp.dot(lhs, rhs, preferred_element_type=F32)


def unit_rms(vec, count):
    return vec * lax.rsqrt(jnp.sum(vec * vec, axis=-1, keepdims=True) / count + INNER_EPS)


def step_kernel(dims, res_in, norm_in, win_in, cw_in, cb_in, wx_in, wdt_in, dtb_in, al_in, dsk_in, wo_in, cs_in, ssm_in,
                res_out, conv_out, ssm_buf,
                res_ref, norm_ref, win_ref, cw_ref, cb_ref, wx_ref, wdt_ref, dtb_ref, al_ref, dsk_ref, wo_ref, cs_ref,
                w_all, h_send, h_all, sth_send, sth_all, stz_send, stz_recv, g_send, g_recv, send_a, recv_a, send_b, recv_b, send_a2, recv_a2, send_b2, recv_b2, st_send, st_recv, st2_send, st2_recv, stat_t,
                p_send, p_recv, y_buf, o_send, o_recv, sum_buf, tot_buf, dt_buf, dx_buf, bc_buf, yv_buf, xc_buf,
                in_sems, *sem_refs):
    m_a, m_b, m_a2, m_b2, m_st, m_st2, m_p, m_y, m_o, m_s, m_w, m_h, m_sth, m_stz, m_g, m_i = [(sem_refs[2 * i], sem_refs[2 * i + 1]) for i in range(len(sem_refs) // 2)]
    n_z, n_y, n_ty, n_str, rows, layers, d_model, n_state, rank, order = dims
    tx, ty = lax.axis_index("tx"), lax.axis_index("ty")
    zi, yi = tx // n_y, tx % n_y
    chans = win_ref.shape[-1]
    cut = chans * CUT // 4
    group = n_y * rows
    own_rows = group // n_ty
    per = n_ty // n_y
    cy, cc = lax.rem(ty // per + yi, n_y), ty % per

    def chunk_of(owner):
        return lax.rem(owner // per + yi, n_y) * per + owner % per

    pk = p_send.shape[1] - rows
    y1, z1, t1 = n_y - 1, n_z - 1, n_ty - 1
    scope = jax.named_scope

    def y_peer(off):
        return lax.rem(yi + off, n_y)

    def z_peer(off):
        return lax.rem(zi + off, n_z)

    def at_y(off):
        return {"tx": zi * n_y + y_peer(off), "ty": ty}

    def at_z(off):
        return {"tx": z_peer(off) * n_y + yi, "ty": ty}

    def at_ty(idx):
        return {"tx": tx, "ty": idx}

    def ty_peer(off):
        return at_ty(lax.rem(ty + off, n_ty))

    def send(src, dst, sems, slot, device):
        pltpu.make_async_remote_copy(src_ref=src, dst_ref=dst, send_sem=sems[0], recv_sem=sems[1].at[slot], device_id=device, device_id_type=MESH).start()

    def arrived(ref, sems, slot):
        pltpu.make_async_remote_copy(src_ref=ref, dst_ref=ref, send_sem=sems[0], recv_sem=sems[1].at[slot], device_id=ty_peer(1), device_id_type=MESH).wait_recv()

    def departed(ref, sems):
        pltpu.make_async_remote_copy(src_ref=ref, dst_ref=ref, send_sem=sems[0], recv_sem=sems[1].at[0], device_id=ty_peer(1), device_id_type=MESH).wait_send()

    def add_up(first, others):
        return functools.reduce(jnp.add, [o.astype(F32) for o in others], first.astype(F32))

    split = set()

    def split_weight(lyr, part):
        if (lyr, part) not in split:
            split.add((lyr, part))
            need(("win", lyr))
            w_all[lyr, part, yi] = win_ref[lyr, :, part, :]

    def input_matmul(k, lyr, strm, source, part):
        split_weight(lyr, part)
        need(("res", strm))
        norm = norm_ref[lyr:lyr + 1, :]
        for zz in range(n_z):
            res = source[zz, :, strm].reshape(group, LANES)
            if part == 0:
                st_send[k, zz] = nt_dot(jnp.ones((8, LANES), F32), res * res, lax.Precision.HIGHEST)
            prod = nn_dot((res * norm).astype(BF16), w_all[lyr, part, yi]).astype(BF16)
            send_b[k, part, zz] = prod[:, cut:]
            for yy in range(n_y):
                send_a[k, part, yy, zz * rows:(zz + 1) * rows, :] = prod[yy * rows:(yy + 1) * rows, :cut]

    def phase_one(k, part):
        for off in range(1, n_z):
            if part == 0:
                send(st_send.at[k, z_peer(off)], st_recv.at[k, off - 1], m_st, k, at_z(off))
        for off in range(1, max(n_y, n_z)):
            if off < n_y:
                send(send_a.at[k, part, y_peer(off)], recv_a.at[k, part, off - 1], m_a, 2 * k + part, at_y(off))
            if off < n_z:
                send(send_b.at[k, part, z_peer(off)], recv_b.at[k, part, off - 1], m_b, 2 * k + part, at_z(off))

    def phase_two(k, part):
        if part == 0:
            arrived(st_recv.at[k], m_st, k)
            st2_send[k] = add_up(st_send[k, zi], [st_recv[k, off - 1] for off in range(1, n_z)])
            for off in range(1, n_y):
                send(st2_send.at[k], st2_recv.at[k, off - 1], m_st2, k, at_y(off))
        with scope(f"wait_a1_{part}"):
            arrived(recv_a.at[k, part], m_a, 2 * k + part)
        for zz in range(n_z):
            span = slice(zz * rows, (zz + 1) * rows)
            send_a2[k, part, zz] = add_up(send_a[k, part, yi, span, :], [recv_a[k, part, off - 1, span, :] for off in range(1, n_y)]).astype(BF16)
        for off in range(1, n_z):
            send(send_a2.at[k, part, z_peer(off)], recv_a2.at[k, part, off - 1], m_a2, 2 * k + part, at_z(off))
        with scope(f"wait_b1_{part}"):
            arrived(recv_b.at[k, part], m_b, 2 * k + part)
        for yy in range(n_y):
            span = slice(yy * rows, (yy + 1) * rows)
            send_b2[k, part, yy] = add_up(send_b[k, part, zi, span, :], [recv_b[k, part, off - 1, span, :] for off in range(1, n_z)]).astype(BF16)
        for off in range(1, n_y):
            send(send_b2.at[k, part, y_peer(off)], recv_b2.at[k, part, off - 1], m_b2, 2 * k + part, at_y(off))

    def finish_sum(k, part):
        if k >= n_str:
            kh = k - n_str
            with scope(f"wait_g_{part}"):
                arrived(g_recv.at[kh, part], m_g, 2 * kh + part)
            return add_up(g_send[kh, part, zi], [g_recv[kh, part, off - 1] for off in range(1, n_z)])
        with scope(f"wait_2_{part}"):
            arrived(recv_a2.at[k, part], m_a2, 2 * k + part)
            arrived(recv_b2.at[k, part], m_b2, 2 * k + part)
        tot_a = add_up(send_a2[k, part, zi], [recv_a2[k, part, off - 1] for off in range(1, n_z)])
        tot_b = add_up(send_b2[k, part, yi], [recv_b2[k, part, off - 1] for off in range(1, n_y)])
        return jnp.concatenate([tot_a, tot_b], axis=-1)

    def row_scale(k):
        if k >= n_str:
            kh = k - n_str
            arrived(stz_recv.at[kh], m_stz, kh)
            total = add_up(stz_send[kh], [stz_recv[kh, off - 1] for off in range(1, n_z)])
            mine = []
            for c in range(per):
                stat_t[k, c * n_z * own_rows:(c + 1) * n_z * own_rows, :] = total[c].T
                mine.append(stat_t[k, pl.ds(pl.multiple_of((c * n_z + zi) * own_rows, own_rows), own_rows), :][:, :1])
            mine = jnp.concatenate(mine, axis=0)
        else:
            arrived(st2_recv.at[k], m_st2, k)
            stat_t[k, :group] = add_up(st2_send[k], [st2_recv[k, off - 1] for off in range(1, n_y)]).T
            mine = stat_t[k, pl.ds(pl.multiple_of(yi * rows, 8), rows), :][:, :1]
        return lax.rsqrt(mine / d_model + NORM_EPS)

    def spread_hidden(k, strm, total):
        tot_buf[strm] = total
        res = res_ref[:, cy, strm, pl.ds(pl.multiple_of(cc * own_rows, own_rows), own_rows), :] + total
        norm = norm_ref[k // n_str + 1:k // n_str + 2, :].reshape(1, 1, LANES)
        sth_send[k] = nt_dot(jnp.ones((8, LANES), F32), (res * res).reshape(n_z * own_rows, LANES), lax.Precision.HIGHEST)
        h_send[k] = (res * norm).astype(BF16)
        slot = yi * per + cc
        for step in range(n_ty):
            device = {"tx": zi * n_y + cy, "ty": lax.rem(ty + step, n_ty)}

            def deliver():
                send(h_send.at[k], h_all.at[k, slot], m_h, k, device)
                send(sth_send.at[k], sth_all.at[k, slot], m_sth, k, device)

            if step:
                deliver()
            else:
                pl.when(cy != yi)(deliver)

        @pl.when(cy == yi)
        def _():
            h_all[k, slot] = h_send[k]
            sth_all[k, slot] = sth_send[k]

    def slab_matmul(k, lyr, part):
        kh = k - n_str
        if part == 0:
            with scope(f"wait_h"):
                @pl.when(cy != yi)
                def _():
                    arrived(h_all.at[kh], m_h, kh)
                    arrived(sth_all.at[kh], m_sth, kh)

                @pl.when(cy == yi)
                def _():
                    arrived(h_all.at[kh, :n_ty - 1], m_h, kh)
                    arrived(sth_all.at[kh, :n_ty - 1], m_sth, kh)

            for c in range(per):
                stz_send[kh, c] = functools.reduce(jnp.add, [sth_all[kh, yy * per + c] for yy in range(n_y)])
            for off in range(1, n_z):
                send(stz_send.at[kh], stz_recv.at[kh, off - 1], m_stz, kh, at_z(off))
        if (lyr, part) not in gathered:
            gathered.add((lyr, part))
            with scope(f"wait_i"):
                arrived(w_all.at[lyr, part, :y1], m_i, 2 * (lyr - 1) + part)
        hidden = jnp.concatenate([h_all[kh, yy * per:(yy + 1) * per].reshape(n_z * rows, LANES) for yy in range(n_y)], axis=1)
        prod = nn_dot(hidden, w_all[lyr, part].reshape(n_y * LANES, chans)).reshape(per, n_z, own_rows, chans)
        for zz in range(n_z):
            g_send[kh, part, zz] = prod[:, zz].reshape(rows, chans).astype(BF16)
        for off in range(1, n_z):
            send(g_send.at[kh, part, z_peer(off)], g_recv.at[kh, part, off - 1], m_g, 2 * kh + part, at_z(off))

    def conv_and_proj(k, lyr, mine, x_in):
        taps = [cs_ref[lyr, j, mine, :] for j in range(3)]
        conv_out[lyr, 0, mine, :] = taps[1]
        conv_out[lyr, 1, mine, :] = taps[2]
        conv_out[lyr, 2, mine, :] = x_in
        conv = x_in.astype(F32) * cw_ref[lyr, 3:4, :] + cb_ref[lyr:lyr + 1, :]
        for j in range(3):
            conv = conv + taps[j].astype(F32) * cw_ref[lyr, j:j + 1, :]
        x_conv = (conv * jax.nn.sigmoid(conv)).astype(BF16)
        xc_buf[k] = x_conv
        wx = wx_ref[lyr]
        bc_w = jnp.concatenate([wx[rank:], jnp.zeros((LANES - 2 * n_state, chans), BF16)], axis=0)
        bc_part = nt_dot(x_conv, bc_w)
        packed = bc_part[:pk]
        for q in range(1, rows // pk):
            packed = packed + pltpu.roll(bc_part[q * pk:(q + 1) * pk], q * 2 * n_state, 1)
        p_send[k, :rows] = nt_dot(x_conv, wx[:rank]).astype(BF16)
        p_send[k, rows:] = packed.astype(BF16)

    def step_sizes(k, lyr):
        proj = add_up(p_send[k], [p_recv[k, off - 1] for off in range(1, n_ty)])
        dt_low = unit_rms(proj[:rows], rank).astype(BF16)
        lane = lax.broadcasted_iota(jnp.int32, (pk, LANES), 1)
        for q in range(rows // pk):
            piece = proj[rows:]
            if q:
                piece = pltpu.roll(piece, LANES - q * 2 * n_state, 1)
            sq = piece * piece
            b_inv = lax.rsqrt(jnp.sum(jnp.where(lane < n_state, sq, 0.0), axis=-1, keepdims=True) / n_state + INNER_EPS)
            c_inv = lax.rsqrt(jnp.sum(jnp.where((lane >= n_state) & (lane < 2 * n_state), sq, 0.0), axis=-1, keepdims=True) / n_state + INNER_EPS)
            bc_buf[k, q * pk:(q + 1) * pk] = piece * jnp.where(lane < n_state, b_inv, c_inv)
        raw = nn_dot(dt_low, wdt_ref[lyr]) + dtb_ref[lyr:lyr + 1, :]
        delta = jnp.maximum(raw, 0.0) + jnp.log1p(jnp.exp(-jnp.abs(raw)))
        dt_buf[k] = delta
        dx_buf[k] = delta * xc_buf[k].astype(F32)

    def state_update(k, lyr, strm):
        neg_a = -jnp.exp(al_ref[lyr])

        def update(grp, carry):
            base = pl.multiple_of(grp * 8, 8)
            d_rows = dt_buf[k, pl.ds(base, 8), :]
            x_rows = dx_buf[k, pl.ds(base, 8), :]
            bc_t = bc_buf[k, pl.ds(base, 8), :].T
            outs = []
            for j in range(8):
                row = strm * rows + base + j
                decay = jnp.exp(d_rows[j:j + 1, :] * neg_a)
                state = decay * ssm_buf[lyr, row] + x_rows[j:j + 1, :] * bc_t[:n_state, j:j + 1]
                ssm_buf[lyr, row] = state
                outs.append(jnp.sum(state * bc_t[n_state:2 * n_state, j:j + 1], axis=0, keepdims=True))
            yv_buf[k, pl.ds(base, 8), :] = jnp.concatenate(outs, axis=0)
            return carry

        lax.fori_loop(0, rows // 8, update, 0)

    def main_thread(strm):
        mine = slice(strm * rows, (strm + 1) * rows)
        for lyr in range(layers):
            k = lyr * n_str + strm
            if lyr:
                with scope(f"slab_{strm}"):
                    slab_matmul(k, lyr, 0)
            else:
                if strm != lead:
                    with scope(f"matmul_{strm}"):
                        input_matmul(k, lyr, strm, res_ref, 0)
                phase_one(k, 0)
                yield
                with scope(f"phase2_{strm}"):
                    phase_two(k, 0)
            yield
            with scope(f"xconv_{strm}"):
                scale = row_scale(k)
                need("cw", "cb", "cs", "wx")
                conv_and_proj(k, lyr, mine, (finish_sum(k, 0) * scale).astype(BF16))
            for off in range(1, n_ty):
                send(p_send.at[k], p_recv.at[k, off - 1], m_p, k, ty_peer(off))
            yield
            with scope(f"wait_p_{strm}"):
                arrived(p_recv.at[k], m_p, k)
            with scope(f"ssm_{strm}"):
                need("wdt", "dtb", "al", "dsk", ("ssm", lyr))
                step_sizes(k, lyr)
                state_update(k, lyr, strm)
            yield
            with scope(f"gate_{strm}"):
                z_in = (finish_sum(k, 1) * scale).astype(BF16).astype(F32)
                gated = ((yv_buf[k] + dsk_ref[lyr:lyr + 1, :] * xc_buf[k].astype(F32)) * (z_in * jax.nn.sigmoid(z_in))).astype(BF16)
                y_buf[k, yi] = gated
            for off in range(1, n_y):
                send(y_buf.at[k, yi], y_buf.at[k, yi], m_y, k, at_y(off))
            yield
            with scope(f"wait_y_{strm}"):
                arrived(y_buf.at[k, :y1], m_y, k)
            with scope(f"outmm_{strm}"):
                if lyr not in gathered:
                    gathered.add(lyr)
                    arrived(wo_ref.at[lyr, :z1 - 1], m_w, lyr)
                everyone = y_buf[k].reshape(group, chans)
                for off in range(n_z):
                    zz = z_peer(off)
                    o_send[k, zz] = nn_dot(everyone, wo_ref[lyr, zz]).reshape(n_ty, own_rows, LANES).astype(BF16)
                    for step in range(n_ty):
                        owner = lax.rem(ty + step, n_ty)
                        if off or step:
                            send(o_send.at[k, zz, chunk_of(owner)], o_recv.at[k, zi * n_ty + ty], m_o, k, {"tx": zz * n_y + yi, "ty": owner})
                o_recv[k, zi * n_ty + ty] = o_send[k, zi, chunk_of(ty)]
            yield
            with scope(f"wait_o_{strm}"):
                arrived(o_recv.at[k, :n_z * n_ty - 1], m_o, k)
            parts = o_recv[k].astype(F32).reshape(n_z, n_ty, own_rows, LANES)
            total = functools.reduce(jnp.add, [parts[:, i] for i in range(n_ty)])
            if lyr:
                total = total + tot_buf[strm]
            if lyr < layers - 1:
                with scope(f"hidden_{strm}"):
                    spread_hidden(k, strm, total)
                yield
                continue
            sum_buf[strm, ty] = total.astype(BF16)
            for off in range(1, n_ty):
                send(sum_buf.at[strm, ty], sum_buf.at[strm, ty], m_s, strm, ty_peer(off))
            yield
        with scope(f"wait_s_{strm}"):
            arrived(sum_buf.at[strm, :t1], m_s, strm)
        for owner in range(n_ty):
            blk, low = lax.rem(owner // per + yi, n_y), owner % per * own_rows
            span = slice(low, low + own_rows)
            res_out[:, blk, strm, span, :] = res_ref[:, blk, strm, span, :] + sum_buf[strm, owner].astype(F32)

    def gate_thread(strm):
        for lyr in range(layers):
            k = lyr * n_str + strm
            if lyr:
                with scope(f"slabz_{strm}"):
                    slab_matmul(k, lyr, 1)
                yield
                continue
            with scope(f"matmulz_{strm}"):
                input_matmul(k, lyr, strm, res_ref, 1)
            phase_one(k, 1)
            yield
            with scope(f"phase2z_{strm}"):
                phase_two(k, 1)
            yield

    def weight_thread():
        width = chans // 2

        def hand_out(lyr, piece, back, ahead):
            block = wo_ref.at[lyr, z_peer(n_z - back), pl.ds(piece * width, width)]
            slot = layers + 2 * lyr + piece if back == 0 and ahead == (1, n_z - 1)[piece] else lyr
            send(block, block, m_w, slot, at_z(ahead))

        for lyr in range(layers):
            for piece in range(2):
                if piece == 0:
                    need(("wo", lyr))
                hand_out(lyr, piece, 0, 1)
                if n_z > 2:
                    hand_out(lyr, piece, 0, n_z - 1)
                yield
            for piece in range(2):
                if n_z > 2:
                    arrived(wo_ref.at[lyr, 0, pl.ds(piece * width, width)], m_w, layers + 2 * lyr + piece)
                    ahead = (1, n_z - 1)[piece]
                    hand_out(lyr, piece, ahead, ahead)
                yield

    def w_in_thread():
        for lyr in range(1, layers):
            for part in range(2):
                split_weight(lyr, part)
                for piece in range(PIECES):
                    span = pl.ds(piece * LANES // PIECES, LANES // PIECES)
                    for off in range(1, n_y):
                        send(w_all.at[lyr, part, yi, span], w_all.at[lyr, part, yi, span], m_i, 2 * (lyr - 1) + part, at_y(off))
                    yield

    gathered = set()
    lead = next(name for name in order if name < GATE)
    moves = {("res", lead): (res_in.at[:, :, lead], res_ref.at[:, :, lead]), "norm": (norm_in, norm_ref), ("win", 0): (win_in.at[0], win_ref.at[0])}
    first = len(moves)
    moves.update({("res", strm): (res_in.at[:, :, strm], res_ref.at[:, :, strm]) for strm in range(n_str) if strm != lead})
    moves.update({"cw": (cw_in, cw_ref), "cb": (cb_in, cb_ref), "cs": (cs_in, cs_ref), "wx": (wx_in, wx_ref), "wdt": (wdt_in, wdt_ref)})
    moves.update({"dtb": (dtb_in, dtb_ref), "al": (al_in, al_ref), "dsk": (dsk_in, dsk_ref)})
    second = len(moves)
    moves.update({("wo", lyr): (wo_in.at[lyr], wo_ref.at[lyr, zi]) for lyr in range(layers)})
    moves.update({("win", lyr): (win_in.at[lyr], win_ref.at[lyr]) for lyr in range(1, layers)})
    moves.update({("ssm", lyr): (ssm_in.at[lyr], ssm_buf.at[lyr]) for lyr in range(layers)})
    loads = {name: pltpu.make_async_copy(src, dst, in_sems.at[i]) for i, (name, (src, dst)) in enumerate(moves.items())}
    for name in list(loads)[:first]:
        loads[name].start()
    rest, late = list(loads)[first:second], list(loads)[second:]

    def need(*names):
        for name in names:
            if name in loads:
                loads.pop(name).wait()

    barrier = pltpu.get_barrier_semaphore()
    peers = [at_y(off) for off in range(1, n_y)] + [at_z(off) for off in range(1, n_z)] + [ty_peer(off) for off in range(1, n_ty)]
    for peer in peers:
        pl.semaphore_signal(barrier, inc=1, device_id=peer, device_id_type=MESH)
    need(("res", lead), "norm", ("win", 0))
    for name in rest:
        loads[name].start()
    with scope("matmul_first"):
        input_matmul(lead, 0, lead, res_ref, 0)
    with scope("barrier"):
        pl.semaphore_wait(barrier, len(peers))

    threads = {}
    for strm in range(n_str):
        threads[strm] = main_thread(strm)
        threads[GATE + strm] = gate_thread(strm)
    threads[WEIGHT] = weight_thread()
    threads[W_IN] = w_in_thread()
    for turn, name in enumerate(order):
        if turn == n_str:
            for load in late:
                loads[load].start()
        next(threads[name], None)

    with scope("drain"):
        sent = [recv_a, recv_b, recv_a2, recv_b2, st_recv, st2_recv, p_recv, y_buf.at[:, :y1], o_recv.at[:, :n_z * n_ty - 1], sum_buf.at[:, :t1], wo_ref.at[:, :z1],
                stz_recv, g_recv, w_all.at[1:, :, :y1]]
        for ref, sems in zip(sent, [m_a, m_b, m_a2, m_b2, m_st, m_st2, m_p, m_y, m_o, m_s, m_w, m_stz, m_g, m_i]):
            departed(ref, sems)

        @pl.when(cy != yi)
        def _():
            departed(h_all, m_h)
            departed(sth_all, m_sth)

        @pl.when(cy == yi)
        def _():
            departed(h_all.at[:, :n_ty - 1], m_h)
            departed(sth_all.at[:, :n_ty - 1], m_sth)


def store_kernel(res_ref, conv_ref, ssm_ref, res_out, conv_out, ssm_out, sems):
    pairs = []
    step = ssm_ref.shape[1] // STORES
    for lyr in range(ssm_ref.shape[0]):
        for i in range(STORES):
            pairs.append((ssm_ref.at[lyr, i * step:(i + 1) * step], ssm_out.at[lyr, i * step:(i + 1) * step]))
    pairs += [(res_ref, res_out), (conv_ref, conv_out)]
    copies = [pltpu.make_async_copy(src, dst, sems.at[i]) for i, (src, dst) in enumerate(pairs)]
    for desc in copies:
        desc.start()
    for desc in copies:
        desc.wait()


def on_chip(shape, dtype):
    return pltpu.VMEM(shape, dtype)


def from_chip(array):
    return pltpu.with_memory_space_constraint(array, pltpu.VMEM)


def build(mesh, n_y, n_str, order):
    n_tx, n_ty = mesh.shape["tx"], mesh.shape["ty"]
    n_z = n_tx // n_y

    def local_step(residual, norm_w, w_in, conv_w, conv_b, w_x, w_dt, dt_bias, a_log, d_skip, w_out, conv_state, ssm_state):
        layers, batch, chans, n_state = ssm_state.shape
        rows = batch // n_str
        all_rows, d_local = residual.shape
        rank = w_dt.shape[1]
        cut = chans * CUT // 4
        own = n_y * rows // n_ty
        pk = rows * 2 * n_state // LANES
        ks = layers * n_str
        kh = ks - n_str
        dims = (n_z, n_y, n_ty, n_str, rows, layers, d_local * n_tx, n_state, rank, order)
        vmem = pl.BlockSpec(memory_space=pltpu.VMEM)
        anyspace = pl.BlockSpec(memory_space=pl.ANY)
        dma = pltpu.SemaphoreType.DMA
        res_shape = (n_z, n_y, n_str, rows, d_local)
        conv_shape = (layers, 3, batch, chans)
        ssm_shape = (layers, batch, n_state, chans)
        operands = [
            residual.reshape(res_shape), norm_w, w_in, conv_w.transpose(0, 2, 1), conv_b, w_x.transpose(0, 2, 1), w_dt, dt_bias,
            a_log.transpose(0, 2, 1), d_skip, w_out, conv_state.transpose(0, 3, 1, 2), ssm_state.transpose(0, 1, 3, 2),
        ]
        shapes = [op.shape for op in operands[:-1]]
        shapes[10] = (layers, n_z, chans, d_local)
        scratch = [pltpu.VMEM(shape, op.dtype) for shape, op in zip(shapes, operands)]
        scratch += [
            pltpu.VMEM((layers, 2, n_y, d_local, chans), BF16),
            pltpu.VMEM((kh, n_z, own, d_local), BF16),
            pltpu.VMEM((kh, n_ty, n_z, own, d_local), BF16),
            pltpu.VMEM((kh, 8, n_z * own), F32),
            pltpu.VMEM((kh, n_ty, 8, n_z * own), F32),
            pltpu.VMEM((kh, n_ty // n_y, 8, n_z * own), F32),
            pltpu.VMEM((kh, n_z - 1, n_ty // n_y, 8, n_z * own), F32),
            pltpu.VMEM((kh, 2, n_z, rows, chans), BF16),
            pltpu.VMEM((kh, 2, n_z - 1, rows, chans), BF16),
            pltpu.VMEM((n_str, 2, n_y, n_z * rows, cut), BF16),
            pltpu.VMEM((n_str, 2, n_y - 1, n_z * rows, cut), BF16),
            pltpu.VMEM((n_str, 2, n_z, n_y * rows, chans - cut), BF16),
            pltpu.VMEM((n_str, 2, n_z - 1, n_y * rows, chans - cut), BF16),
            pltpu.VMEM((n_str, 2, n_z, rows, cut), BF16),
            pltpu.VMEM((n_str, 2, n_z - 1, rows, cut), BF16),
            pltpu.VMEM((n_str, 2, n_y, rows, chans - cut), BF16),
            pltpu.VMEM((n_str, 2, n_y - 1, rows, chans - cut), BF16),
            pltpu.VMEM((n_str, n_z, 8, n_y * rows), F32),
            pltpu.VMEM((n_str, n_z - 1, 8, n_y * rows), F32),
            pltpu.VMEM((n_str, 8, n_y * rows), F32),
            pltpu.VMEM((n_str, n_y - 1, 8, n_y * rows), F32),
            pltpu.VMEM((ks, max(n_y, n_z) * rows, 8), F32),
            pltpu.VMEM((ks, rows + pk, LANES), BF16),
            pltpu.VMEM((ks, n_ty - 1, rows + pk, LANES), BF16),
            pltpu.VMEM((ks, n_y, rows, chans), BF16),
            pltpu.VMEM((ks, n_z, n_ty, own, d_local), BF16),
            pltpu.VMEM((ks, n_z * n_ty, own, d_local), BF16),
            pltpu.VMEM((n_str, n_ty, n_z, own, d_local), BF16),
            pltpu.VMEM((n_str, n_z, own, d_local), F32),
            pltpu.VMEM((ks, rows, chans), F32),
            pltpu.VMEM((ks, rows, chans), F32),
            pltpu.VMEM((ks, rows, LANES), F32),
            pltpu.VMEM((ks, rows, chans), F32),
            pltpu.VMEM((ks, rows, chans), BF16),
        ]
        scratch += [dma((len(operands) + n_str + 3 * layers,))]
        for count in [2 * n_str, 2 * n_str, 2 * n_str, 2 * n_str, n_str, n_str, ks, ks, ks, n_str, 3 * layers, kh, kh, kh, 2 * kh, 2 * (layers - 1)]:
            scratch += [dma, dma((count,))]
        res, conv, ssm = pl.pallas_call(
            functools.partial(step_kernel, dims),
            out_shape=(on_chip(res_shape, F32), on_chip(conv_shape, BF16), on_chip(ssm_shape, F32)),
            in_specs=[pl.BlockSpec(memory_space=pltpu.HBM)] * len(operands),
            out_specs=(vmem, vmem, vmem),
            scratch_shapes=scratch,
            compiler_params=pltpu.CompilerParams(collective_id=0, has_side_effects=True, vmem_limit_bytes=VMEM_LIMIT),
        )(*operands)
        res, conv, ssm = pl.pallas_call(
            store_kernel,
            out_shape=(jax.ShapeDtypeStruct(res_shape, F32), jax.ShapeDtypeStruct(conv_shape, BF16), jax.ShapeDtypeStruct(ssm_shape, F32)),
            in_specs=[vmem] * 3,
            out_specs=(anyspace,) * 3,
            scratch_shapes=[dma((layers * STORES + 2,))],
            compiler_params=pltpu.CompilerParams(vmem_limit_bytes=16 * 1024 * 1024),
        )(*(from_chip(out) for out in (res, conv, ssm)))
        return res.reshape(all_rows, d_local), conv.transpose(0, 2, 3, 1), ssm.transpose(0, 1, 3, 2)

    cache_spec = P(None, ("dp", "tx"), "ty", None)
    in_specs = (P("dp", "tx"), P(None, "tx"), P(None, "tx", None, "ty"), P(None, "ty", None), P(None, "ty"), P(None, "ty", None), P(None, None, "ty"), P(None, "ty"), P(None, "ty", None), P(None, "ty"), P(None, "ty", "tx"), cache_spec, cache_spec)
    out_specs = (P("dp", "tx"), cache_spec, cache_spec)
    return jax.shard_map(local_step, mesh=mesh, in_specs=in_specs, out_specs=out_specs, check_vma=False)


def solution(mesh):
    return build(mesh, 4, STREAMS, ORDER)
```

```python
import functools

import jax
import jax.numpy as jnp
from jax import lax
from jax.experimental import pallas as pl
from jax.experimental.pallas import tpu as pltpu
from jax.sharding import PartitionSpec as P

NORM_EPS = 1e-5
INNER_EPS = 1e-6
MESH = pl.DeviceIdType.MESH
F32 = jnp.float32
BF16 = jnp.bfloat16
LANES = 128
GATE = 10
WEIGHT = 20
W_IN = 30
PIECES = 4
CUT = 2
STREAMS = 4
ORDER = (
    0, 2, 3, 1, 0, 2, 10, 30, 3, 20, 1, 2, 20, 11, 0, 12, 3, 10, 13, 30, 1, 0, 11, 30,
    20, 20, 12, 0, 1, 13, 2, 20, 1, 2, 3, 3, 30, 0, 1, 2, 30, 30, 3, 0, 1, 20, 2, 3,
    30, 30, 0, 1, 2, 3, 0, 20, 1, 20, 10, 2, 11, 3, 12, 13, 0, 1, 0, 1, 2, 2, 3, 3,
    0, 1, 2, 3, 0, 1, 2, 3, 2, 0, 1, 3,
)
STORES = 1
VMEM_LIMIT = 52 * 1024 * 1024


def far(count):
    return sorted(range(1, count), key=lambda off: -min(off, count - off))


def nt_dot(lhs, rhs, precision=None):
    return lax.dot_general(lhs, rhs, (((1,), (1,)), ((), ())), precision=precision, preferred_element_type=F32)


def nn_dot(lhs, rhs):
    return jnp.dot(lhs, rhs, preferred_element_type=F32)


def unit_rms(vec, count):
    return vec * lax.rsqrt(jnp.sum(vec * vec, axis=-1, keepdims=True) / count + INNER_EPS)


def step_kernel(dims, res_in, norm_in, win_in, cw_in, cb_in, wx_in, wdt_in, dtb_in, al_in, dsk_in, wo_in, cs_in, ssm_in,
                res_out, conv_out, ssm_buf,
                res_ref, norm_ref, win_ref, cw_ref, cb_ref, wx_ref, wdt_ref, dtb_ref, al_ref, dsk_ref, wo_ref, cs_ref,
                w_all, h_send, h_all, sth_send, sth_all, stz_send, stz_recv, g_send, g_recv, send_a, recv_a, send_b, recv_b, send_a2, recv_a2, send_b2, recv_b2, st_send, st_recv, st2_send, st2_recv, stat_t,
                p_send, p_recv, y_buf, o_send, o_recv, sum_buf, tot_buf, dt_buf, dx_buf, bc_buf, yv_buf, xc_buf,
                in_sems, *sem_refs):
    m_a, m_b, m_a2, m_b2, m_st, m_st2, m_p, m_y, m_o, m_s, m_w, m_h, m_sth, m_stz, m_g, m_i = [(sem_refs[2 * i], sem_refs[2 * i + 1]) for i in range(len(sem_refs) // 2)]
    n_z, n_y, n_ty, n_str, rows, layers, d_model, n_state, rank, order = dims
    tx, ty = lax.axis_index("tx"), lax.axis_index("ty")
    zi, yi = tx // n_y, tx % n_y
    chans = win_ref.shape[-1]
    cut = chans * CUT // 4
    group = n_y * rows
    own_rows = group // n_ty
    per = n_ty // n_y
    cy, cc = lax.rem(ty // per + yi, n_y), ty % per

    def chunk_of(owner):
        return lax.rem(owner // per + yi, n_y) * per + owner % per

    pk = p_send.shape[1] - rows
    y1, z1, t1 = n_y - 1, n_z - 1, n_ty - 1
    scope = jax.named_scope

    def y_peer(off):
        return lax.rem(yi + off, n_y)

    def z_peer(off):
        return lax.rem(zi + off, n_z)

    def at_y(off):
        return {"tx": zi * n_y + y_peer(off), "ty": ty}

    def at_z(off):
        return {"tx": z_peer(off) * n_y + yi, "ty": ty}

    def at_ty(idx):
        return {"tx": tx, "ty": idx}

    def ty_peer(off):
        return at_ty(lax.rem(ty + off, n_ty))

    def send(src, dst, sems, slot, device):
        pltpu.make_async_remote_copy(src_ref=src, dst_ref=dst, send_sem=sems[0], recv_sem=sems[1].at[slot], device_id=device, device_id_type=MESH).start()

    def arrived(ref, sems, slot):
        pltpu.make_async_remote_copy(src_ref=ref, dst_ref=ref, send_sem=sems[0], recv_sem=sems[1].at[slot], device_id=ty_peer(1), device_id_type=MESH).wait_recv()

    def departed(ref, sems):
        pltpu.make_async_remote_copy(src_ref=ref, dst_ref=ref, send_sem=sems[0], recv_sem=sems[1].at[0], device_id=ty_peer(1), device_id_type=MESH).wait_send()

    def add_up(first, others):
        return functools.reduce(jnp.add, [o.astype(F32) for o in others], first.astype(F32))

    split = set()

    def split_weight(lyr, part):
        if (lyr, part) not in split:
            split.add((lyr, part))
            need(("win", lyr))
            w_all[lyr, part, yi] = win_ref[lyr, :, part, :]

    def input_matmul(k, lyr, strm, source, part):
        split_weight(lyr, part)
        need(("res", strm))
        norm = norm_ref[lyr:lyr + 1, :]
        for zz in range(n_z):
            res = source[zz, :, strm].reshape(group, LANES)
            if part == 0:
                st_send[k, zz] = nt_dot(jnp.ones((8, LANES), F32), res * res, lax.Precision.HIGHEST)
            prod = nn_dot((res * norm).astype(BF16), w_all[lyr, part, yi]).astype(BF16)
            send_b[k, part, zz] = prod[:, cut:]
            for yy in range(n_y):
                send_a[k, part, yy, zz * rows:(zz + 1) * rows, :] = prod[yy * rows:(yy + 1) * rows, :cut]

    def phase_one(k, part):
        for off in far(n_z):
            if part == 0:
                send(st_send.at[k, z_peer(off)], st_recv.at[k, off - 1], m_st, k, at_z(off))
        for off in far(max(n_y, n_z)):
            if off < n_y:
                send(send_a.at[k, part, y_peer(off)], recv_a.at[k, part, off - 1], m_a, 2 * k + part, at_y(off))
            if off < n_z:
                send(send_b.at[k, part, z_peer(off)], recv_b.at[k, part, off - 1], m_b, 2 * k + part, at_z(off))

    def phase_two(k, part):
        if part == 0:
            arrived(st_recv.at[k], m_st, k)
            st2_send[k] = add_up(st_send[k, zi], [st_recv[k, off - 1] for off in range(1, n_z)])
            for off in far(n_y):
                send(st2_send.at[k], st2_recv.at[k, off - 1], m_st2, k, at_y(off))
        with scope(f"wait_a1_{part}"):
            arrived(recv_a.at[k, part], m_a, 2 * k + part)
        for zz in range(n_z):
            span = slice(zz * rows, (zz + 1) * rows)
            send_a2[k, part, zz] = add_up(send_a[k, part, yi, span, :], [recv_a[k, part, off - 1, span, :] for off in range(1, n_y)]).astype(BF16)
        for off in far(n_z):
            send(send_a2.at[k, part, z_peer(off)], recv_a2.at[k, part, off - 1], m_a2, 2 * k + part, at_z(off))
        with scope(f"wait_b1_{part}"):
            arrived(recv_b.at[k, part], m_b, 2 * k + part)
        for yy in range(n_y):
            span = slice(yy * rows, (yy + 1) * rows)
            send_b2[k, part, yy] = add_up(send_b[k, part, zi, span, :], [recv_b[k, part, off - 1, span, :] for off in range(1, n_z)]).astype(BF16)
        for off in far(n_y):
            send(send_b2.at[k, part, y_peer(off)], recv_b2.at[k, part, off - 1], m_b2, 2 * k + part, at_y(off))

    def finish_sum(k, part):
        if k >= n_str:
            kh = k - n_str
            with scope(f"wait_g_{part}"):
                arrived(g_recv.at[kh, part], m_g, 2 * kh + part)
            return add_up(g_send[kh, part, zi], [g_recv[kh, part, off - 1] for off in range(1, n_z)])
        with scope(f"wait_2_{part}"):
            arrived(recv_a2.at[k, part], m_a2, 2 * k + part)
            arrived(recv_b2.at[k, part], m_b2, 2 * k + part)
        tot_a = add_up(send_a2[k, part, zi], [recv_a2[k, part, off - 1] for off in range(1, n_z)])
        tot_b = add_up(send_b2[k, part, yi], [recv_b2[k, part, off - 1] for off in range(1, n_y)])
        return jnp.concatenate([tot_a, tot_b], axis=-1)

    def row_scale(k):
        if k >= n_str:
            kh = k - n_str
            arrived(stz_recv.at[kh], m_stz, kh)
            total = add_up(stz_send[kh], [stz_recv[kh, off - 1] for off in range(1, n_z)])
            mine = []
            for c in range(per):
                stat_t[k, c * n_z * own_rows:(c + 1) * n_z * own_rows, :] = total[c].T
                mine.append(stat_t[k, pl.ds(pl.multiple_of((c * n_z + zi) * own_rows, own_rows), own_rows), :][:, :1])
            mine = jnp.concatenate(mine, axis=0)
        else:
            arrived(st2_recv.at[k], m_st2, k)
            stat_t[k, :group] = add_up(st2_send[k], [st2_recv[k, off - 1] for off in range(1, n_y)]).T
            mine = stat_t[k, pl.ds(pl.multiple_of(yi * rows, 8), rows), :][:, :1]
        return lax.rsqrt(mine / d_model + NORM_EPS)

    def spread_hidden(k, strm, total):
        tot_buf[strm] = total
        res = res_ref[:, cy, strm, pl.ds(pl.multiple_of(cc * own_rows, own_rows), own_rows), :] + total
        norm = norm_ref[k // n_str + 1:k // n_str + 2, :].reshape(1, 1, LANES)
        sth_send[k] = nt_dot(jnp.ones((8, LANES), F32), (res * res).reshape(n_z * own_rows, LANES), lax.Precision.HIGHEST)
        h_send[k] = (res * norm).astype(BF16)
        slot = yi * per + cc
        for step in far(n_ty) + [0]:
            device = {"tx": zi * n_y + cy, "ty": lax.rem(ty + step, n_ty)}

            def deliver():
                send(h_send.at[k], h_all.at[k, slot], m_h, k, device)
                send(sth_send.at[k], sth_all.at[k, slot], m_sth, k, device)

            if step:
                deliver()
            else:
                pl.when(cy != yi)(deliver)

        @pl.when(cy == yi)
        def _():
            h_all[k, slot] = h_send[k]
            sth_all[k, slot] = sth_send[k]

    def slab_matmul(k, lyr, part):
        kh = k - n_str
        if part == 0:
            with scope(f"wait_h"):
                @pl.when(cy != yi)
                def _():
                    arrived(h_all.at[kh], m_h, kh)
                    arrived(sth_all.at[kh], m_sth, kh)

                @pl.when(cy == yi)
                def _():
                    arrived(h_all.at[kh, :n_ty - 1], m_h, kh)
                    arrived(sth_all.at[kh, :n_ty - 1], m_sth, kh)

            for c in range(per):
                stz_send[kh, c] = functools.reduce(jnp.add, [sth_all[kh, yy * per + c] for yy in range(n_y)])
            for off in far(n_z):
                send(stz_send.at[kh], stz_recv.at[kh, off - 1], m_stz, kh, at_z(off))
        if (lyr, part) not in gathered:
            gathered.add((lyr, part))
            with scope(f"wait_i"):
                arrived(w_all.at[lyr, part, :y1], m_i, 2 * (lyr - 1) + part)
        hidden = jnp.concatenate([h_all[kh, yy * per:(yy + 1) * per].reshape(n_z * rows, LANES) for yy in range(n_y)], axis=1)
        prod = nn_dot(hidden, w_all[lyr, part].reshape(n_y * LANES, chans)).reshape(per, n_z, own_rows, chans)
        for zz in range(n_z):
            g_send[kh, part, zz] = prod[:, zz].reshape(rows, chans).astype(BF16)
        for off in far(n_z):
            send(g_send.at[kh, part, z_peer(off)], g_recv.at[kh, part, off - 1], m_g, 2 * kh + part, at_z(off))

    def conv_and_proj(k, lyr, mine, x_in):
        taps = [cs_ref[lyr, j, mine, :] for j in range(3)]
        conv_out[lyr, 0, mine, :] = taps[1]
        conv_out[lyr, 1, mine, :] = taps[2]
        conv_out[lyr, 2, mine, :] = x_in
        conv = x_in.astype(F32) * cw_ref[lyr, 3:4, :] + cb_ref[lyr:lyr + 1, :]
        for j in range(3):
            conv = conv + taps[j].astype(F32) * cw_ref[lyr, j:j + 1, :]
        x_conv = (conv * jax.nn.sigmoid(conv)).astype(BF16)
        xc_buf[k] = x_conv
        wx = wx_ref[lyr]
        bc_w = jnp.concatenate([wx[rank:], jnp.zeros((LANES - 2 * n_state, chans), BF16)], axis=0)
        bc_part = nt_dot(x_conv, bc_w)
        packed = bc_part[:pk]
        for q in range(1, rows // pk):
            packed = packed + pltpu.roll(bc_part[q * pk:(q + 1) * pk], q * 2 * n_state, 1)
        p_send[k, :rows] = nt_dot(x_conv, wx[:rank]).astype(BF16)
        p_send[k, rows:] = packed.astype(BF16)

    def step_sizes(k, lyr):
        proj = add_up(p_send[k], [p_recv[k, off - 1] for off in range(1, n_ty)])
        dt_low = unit_rms(proj[:rows], rank).astype(BF16)
        lane = lax.broadcasted_iota(jnp.int32, (pk, LANES), 1)
        for q in range(rows // pk):
            piece = proj[rows:]
            if q:
                piece = pltpu.roll(piece, LANES - q * 2 * n_state, 1)
            sq = piece * piece
            b_inv = lax.rsqrt(jnp.sum(jnp.where(lane < n_state, sq, 0.0), axis=-1, keepdims=True) / n_state + INNER_EPS)
            c_inv = lax.rsqrt(jnp.sum(jnp.where((lane >= n_state) & (lane < 2 * n_state), sq, 0.0), axis=-1, keepdims=True) / n_state + INNER_EPS)
            bc_buf[k, q * pk:(q + 1) * pk] = piece * jnp.where(lane < n_state, b_inv, c_inv)
        raw = nn_dot(dt_low, wdt_ref[lyr]) + dtb_ref[lyr:lyr + 1, :]
        delta = jnp.maximum(raw, 0.0) + jnp.log1p(jnp.exp(-jnp.abs(raw)))
        dt_buf[k] = delta
        dx_buf[k] = delta * xc_buf[k].astype(F32)

    def state_update(k, lyr, strm):
        neg_a = -jnp.exp(al_ref[lyr])

        def update(grp, carry):
            base = pl.multiple_of(grp * 8, 8)
            d_rows = dt_buf[k, pl.ds(base, 8), :]
            x_rows = dx_buf[k, pl.ds(base, 8), :]
            bc_t = bc_buf[k, pl.ds(base, 8), :].T
            outs = []
            for j in range(8):
                row = strm * rows + base + j
                decay = jnp.exp(d_rows[j:j + 1, :] * neg_a)
                state = decay * ssm_buf[lyr, row] + x_rows[j:j + 1, :] * bc_t[:n_state, j:j + 1]
                ssm_buf[lyr, row] = state
                outs.append(jnp.sum(state * bc_t[n_state:2 * n_state, j:j + 1], axis=0, keepdims=True))
            yv_buf[k, pl.ds(base, 8), :] = jnp.concatenate(outs, axis=0)
            return carry

        lax.fori_loop(0, rows // 8, update, 0)

    def main_thread(strm):
        mine = slice(strm * rows, (strm + 1) * rows)
        for lyr in range(layers):
            k = lyr * n_str + strm
            if lyr:
                with scope(f"slab_{strm}"):
                    slab_matmul(k, lyr, 0)
            else:
                if strm != lead:
                    with scope(f"matmul_{strm}"):
                        input_matmul(k, lyr, strm, res_ref, 0)
                phase_one(k, 0)
                yield
                with scope(f"phase2_{strm}"):
                    phase_two(k, 0)
            yield
            with scope(f"xconv_{strm}"):
                scale = row_scale(k)
                need("cw", "cb", "cs", "wx")
                conv_and_proj(k, lyr, mine, (finish_sum(k, 0) * scale).astype(BF16))
            for off in far(n_ty):
                send(p_send.at[k], p_recv.at[k, off - 1], m_p, k, ty_peer(off))
            yield
            with scope(f"wait_p_{strm}"):
                arrived(p_recv.at[k], m_p, k)
            with scope(f"ssm_{strm}"):
                need("wdt", "dtb", "al", "dsk", ("ssm", lyr))
                step_sizes(k, lyr)
                state_update(k, lyr, strm)
            yield
            with scope(f"gate_{strm}"):
                z_in = (finish_sum(k, 1) * scale).astype(BF16).astype(F32)
                gated = ((yv_buf[k] + dsk_ref[lyr:lyr + 1, :] * xc_buf[k].astype(F32)) * (z_in * jax.nn.sigmoid(z_in))).astype(BF16)
                y_buf[k, yi] = gated
            for off in far(n_y):
                send(y_buf.at[k, yi], y_buf.at[k, yi], m_y, k, at_y(off))
            yield
            with scope(f"wait_y_{strm}"):
                arrived(y_buf.at[k, :y1], m_y, k)
            with scope(f"outmm_{strm}"):
                if lyr not in gathered:
                    gathered.add(lyr)
                    arrived(wo_ref.at[lyr, :z1 - 1], m_w, lyr)
                everyone = y_buf[k].reshape(group, chans)
                for off in far(n_z) + [0]:
                    zz = z_peer(off)
                    o_send[k, zz] = nn_dot(everyone, wo_ref[lyr, zz]).reshape(n_ty, own_rows, LANES).astype(BF16)
                    for step in far(n_ty) + [0]:
                        owner = lax.rem(ty + step, n_ty)
                        if off or step:
                            send(o_send.at[k, zz, chunk_of(owner)], o_recv.at[k, zi * n_ty + ty], m_o, k, {"tx": zz * n_y + yi, "ty": owner})
                o_recv[k, zi * n_ty + ty] = o_send[k, zi, chunk_of(ty)]
            yield
            with scope(f"wait_o_{strm}"):
                arrived(o_recv.at[k, :n_z * n_ty - 1], m_o, k)
            parts = o_recv[k].astype(F32).reshape(n_z, n_ty, own_rows, LANES)
            total = functools.reduce(jnp.add, [parts[:, i] for i in range(n_ty)])
            if lyr:
                total = total + tot_buf[strm]
            if lyr < layers - 1:
                with scope(f"hidden_{strm}"):
                    spread_hidden(k, strm, total)
                yield
                continue
            sum_buf[strm, ty] = total.astype(BF16)
            for off in far(n_ty):
                send(sum_buf.at[strm, ty], sum_buf.at[strm, ty], m_s, strm, ty_peer(off))
            yield
        with scope(f"wait_s_{strm}"):
            arrived(sum_buf.at[strm, :t1], m_s, strm)
        for owner in range(n_ty):
            blk, low = lax.rem(owner // per + yi, n_y), owner % per * own_rows
            span = slice(low, low + own_rows)
            res_out[:, blk, strm, span, :] = res_ref[:, blk, strm, span, :] + sum_buf[strm, owner].astype(F32)

    def gate_thread(strm):
        for lyr in range(layers):
            k = lyr * n_str + strm
            if lyr:
                with scope(f"slabz_{strm}"):
                    slab_matmul(k, lyr, 1)
                yield
                continue
            with scope(f"matmulz_{strm}"):
                input_matmul(k, lyr, strm, res_ref, 1)
            phase_one(k, 1)
            yield
            with scope(f"phase2z_{strm}"):
                phase_two(k, 1)
            yield

    def weight_thread():
        width = chans // 2

        def hand_out(lyr, piece, back, ahead):
            block = wo_ref.at[lyr, z_peer(n_z - back), pl.ds(piece * width, width)]
            slot = layers + 2 * lyr + piece if back == 0 and ahead == (1, n_z - 1)[piece] else lyr
            send(block, block, m_w, slot, at_z(ahead))

        for lyr in range(layers):
            for piece in range(2):
                if piece == 0:
                    need(("wo", lyr))
                hand_out(lyr, piece, 0, 1)
                if n_z > 2:
                    hand_out(lyr, piece, 0, n_z - 1)
                yield
            for piece in range(2):
                if n_z > 2:
                    arrived(wo_ref.at[lyr, 0, pl.ds(piece * width, width)], m_w, layers + 2 * lyr + piece)
                    ahead = (1, n_z - 1)[piece]
                    hand_out(lyr, piece, ahead, ahead)
                yield

    def w_in_thread():
        for lyr in range(1, layers):
            for part in range(2):
                split_weight(lyr, part)
                for piece in range(PIECES):
                    span = pl.ds(piece * LANES // PIECES, LANES // PIECES)
                    for off in far(n_y):
                        send(w_all.at[lyr, part, yi, span], w_all.at[lyr, part, yi, span], m_i, 2 * (lyr - 1) + part, at_y(off))
                    yield

    gathered = set()
    lead = next(name for name in order if name < GATE)
    moves = {("res", lead): (res_in.at[:, :, lead], res_ref.at[:, :, lead]), "norm": (norm_in, norm_ref), ("win", 0): (win_in.at[0], win_ref.at[0])}
    first = len(moves)
    moves.update({("res", strm): (res_in.at[:, :, strm], res_ref.at[:, :, strm]) for strm in range(n_str) if strm != lead})
    moves.update({"cw": (cw_in, cw_ref), "cb": (cb_in, cb_ref), "cs": (cs_in, cs_ref), "wx": (wx_in, wx_ref), "wdt": (wdt_in, wdt_ref)})
    moves.update({"dtb": (dtb_in, dtb_ref), "al": (al_in, al_ref), "dsk": (dsk_in, dsk_ref)})
    second = len(moves)
    moves.update({("wo", lyr): (wo_in.at[lyr], wo_ref.at[lyr, zi]) for lyr in range(layers)})
    moves.update({("win", lyr): (win_in.at[lyr], win_ref.at[lyr]) for lyr in range(1, layers)})
    moves.update({("ssm", lyr): (ssm_in.at[lyr], ssm_buf.at[lyr]) for lyr in range(layers)})
    loads = {name: pltpu.make_async_copy(src, dst, in_sems.at[i]) for i, (name, (src, dst)) in enumerate(moves.items())}
    for name in list(loads)[:first]:
        loads[name].start()
    rest, late = list(loads)[first:second], list(loads)[second:]

    def need(*names):
        for name in names:
            if name in loads:
                loads.pop(name).wait()

    barrier = pltpu.get_barrier_semaphore()
    peers = [at_y(off) for off in range(1, n_y)] + [at_z(off) for off in range(1, n_z)] + [ty_peer(off) for off in range(1, n_ty)]
    for peer in peers:
        pl.semaphore_signal(barrier, inc=1, device_id=peer, device_id_type=MESH)
    need(("res", lead), "norm", ("win", 0))
    for name in rest:
        loads[name].start()
    with scope("matmul_first"):
        input_matmul(lead, 0, lead, res_ref, 0)
    with scope("barrier"):
        pl.semaphore_wait(barrier, len(peers))

    threads = {}
    for strm in range(n_str):
        threads[strm] = main_thread(strm)
        threads[GATE + strm] = gate_thread(strm)
    threads[WEIGHT] = weight_thread()
    threads[W_IN] = w_in_thread()
    for turn, name in enumerate(order):
        if turn == n_str:
            for load in late:
                loads[load].start()
        next(threads[name], None)

    with scope("drain"):
        sent = [recv_a, recv_b, recv_a2, recv_b2, st_recv, st2_recv, p_recv, y_buf.at[:, :y1], o_recv.at[:, :n_z * n_ty - 1], sum_buf.at[:, :t1], wo_ref.at[:, :z1],
                stz_recv, g_recv, w_all.at[1:, :, :y1]]
        for ref, sems in zip(sent, [m_a, m_b, m_a2, m_b2, m_st, m_st2, m_p, m_y, m_o, m_s, m_w, m_stz, m_g, m_i]):
            departed(ref, sems)

        @pl.when(cy != yi)
        def _():
            departed(h_all, m_h)
            departed(sth_all, m_sth)

        @pl.when(cy == yi)
        def _():
            departed(h_all.at[:, :n_ty - 1], m_h)
            departed(sth_all.at[:, :n_ty - 1], m_sth)


def store_kernel(res_ref, conv_ref, ssm_ref, res_out, conv_out, ssm_out, sems):
    pairs = []
    step = ssm_ref.shape[1] // STORES
    for lyr in range(ssm_ref.shape[0]):
        for i in range(STORES):
            pairs.append((ssm_ref.at[lyr, i * step:(i + 1) * step], ssm_out.at[lyr, i * step:(i + 1) * step]))
    pairs += [(res_ref, res_out), (conv_ref, conv_out)]
    copies = [pltpu.make_async_copy(src, dst, sems.at[i]) for i, (src, dst) in enumerate(pairs)]
    for desc in copies:
        desc.start()
    for desc in copies:
        desc.wait()


def on_chip(shape, dtype):
    return pltpu.VMEM(shape, dtype)


def from_chip(array):
    return pltpu.with_memory_space_constraint(array, pltpu.VMEM)


def build(mesh, n_y, n_str, order):
    n_tx, n_ty = mesh.shape["tx"], mesh.shape["ty"]
    n_z = n_tx // n_y

    def local_step(residual, norm_w, w_in, conv_w, conv_b, w_x, w_dt, dt_bias, a_log, d_skip, w_out, conv_state, ssm_state):
        layers, batch, chans, n_state = ssm_state.shape
        rows = batch // n_str
        all_rows, d_local = residual.shape
        rank = w_dt.shape[1]
        cut = chans * CUT // 4
        own = n_y * rows // n_ty
        pk = rows * 2 * n_state // LANES
        ks = layers * n_str
        kh = ks - n_str
        dims = (n_z, n_y, n_ty, n_str, rows, layers, d_local * n_tx, n_state, rank, order)
        vmem = pl.BlockSpec(memory_space=pltpu.VMEM)
        anyspace = pl.BlockSpec(memory_space=pl.ANY)
        dma = pltpu.SemaphoreType.DMA
        res_shape = (n_z, n_y, n_str, rows, d_local)
        conv_shape = (layers, 3, batch, chans)
        ssm_shape = (layers, batch, n_state, chans)
        operands = [
            residual.reshape(res_shape), norm_w, w_in, conv_w.transpose(0, 2, 1), conv_b, w_x.transpose(0, 2, 1), w_dt, dt_bias,
            a_log.transpose(0, 2, 1), d_skip, w_out, conv_state.transpose(0, 3, 1, 2), ssm_state.transpose(0, 1, 3, 2),
        ]
        shapes = [op.shape for op in operands[:-1]]
        shapes[10] = (layers, n_z, chans, d_local)
        scratch = [pltpu.VMEM(shape, op.dtype) for shape, op in zip(shapes, operands)]
        scratch += [
            pltpu.VMEM((layers, 2, n_y, d_local, chans), BF16),
            pltpu.VMEM((kh, n_z, own, d_local), BF16),
            pltpu.VMEM((kh, n_ty, n_z, own, d_local), BF16),
            pltpu.VMEM((kh, 8, n_z * own), F32),
            pltpu.VMEM((kh, n_ty, 8, n_z * own), F32),
            pltpu.VMEM((kh, n_ty // n_y, 8, n_z * own), F32),
            pltpu.VMEM((kh, n_z - 1, n_ty // n_y, 8, n_z * own), F32),
            pltpu.VMEM((kh, 2, n_z, rows, chans), BF16),
            pltpu.VMEM((kh, 2, n_z - 1, rows, chans), BF16),
            pltpu.VMEM((n_str, 2, n_y, n_z * rows, cut), BF16),
            pltpu.VMEM((n_str, 2, n_y - 1, n_z * rows, cut), BF16),
            pltpu.VMEM((n_str, 2, n_z, n_y * rows, chans - cut), BF16),
            pltpu.VMEM((n_str, 2, n_z - 1, n_y * rows, chans - cut), BF16),
            pltpu.VMEM((n_str, 2, n_z, rows, cut), BF16),
            pltpu.VMEM((n_str, 2, n_z - 1, rows, cut), BF16),
            pltpu.VMEM((n_str, 2, n_y, rows, chans - cut), BF16),
            pltpu.VMEM((n_str, 2, n_y - 1, rows, chans - cut), BF16),
            pltpu.VMEM((n_str, n_z, 8, n_y * rows), F32),
            pltpu.VMEM((n_str, n_z - 1, 8, n_y * rows), F32),
            pltpu.VMEM((n_str, 8, n_y * rows), F32),
            pltpu.VMEM((n_str, n_y - 1, 8, n_y * rows), F32),
            pltpu.VMEM((ks, max(n_y, n_z) * rows, 8), F32),
            pltpu.VMEM((ks, rows + pk, LANES), BF16),
            pltpu.VMEM((ks, n_ty - 1, rows + pk, LANES), BF16),
            pltpu.VMEM((ks, n_y, rows, chans), BF16),
            pltpu.VMEM((ks, n_z, n_ty, own, d_local), BF16),
            pltpu.VMEM((ks, n_z * n_ty, own, d_local), BF16),
            pltpu.VMEM((n_str, n_ty, n_z, own, d_local), BF16),
            pltpu.VMEM((n_str, n_z, own, d_local), F32),
            pltpu.VMEM((ks, rows, chans), F32),
            pltpu.VMEM((ks, rows, chans), F32),
            pltpu.VMEM((ks, rows, LANES), F32),
            pltpu.VMEM((ks, rows, chans), F32),
            pltpu.VMEM((ks, rows, chans), BF16),
        ]
        scratch += [dma((len(operands) + n_str + 3 * layers,))]
        for count in [2 * n_str, 2 * n_str, 2 * n_str, 2 * n_str, n_str, n_str, ks, ks, ks, n_str, 3 * layers, kh, kh, kh, 2 * kh, 2 * (layers - 1)]:
            scratch += [dma, dma((count,))]
        res, conv, ssm = pl.pallas_call(
            functools.partial(step_kernel, dims),
            out_shape=(on_chip(res_shape, F32), on_chip(conv_shape, BF16), on_chip(ssm_shape, F32)),
            in_specs=[pl.BlockSpec(memory_space=pltpu.HBM)] * len(operands),
            out_specs=(vmem, vmem, vmem),
            scratch_shapes=scratch,
            compiler_params=pltpu.CompilerParams(collective_id=0, has_side_effects=True, vmem_limit_bytes=VMEM_LIMIT),
        )(*operands)
        res, conv, ssm = pl.pallas_call(
            store_kernel,
            out_shape=(jax.ShapeDtypeStruct(res_shape, F32), jax.ShapeDtypeStruct(conv_shape, BF16), jax.ShapeDtypeStruct(ssm_shape, F32)),
            in_specs=[vmem] * 3,
            out_specs=(anyspace,) * 3,
            scratch_shapes=[dma((layers * STORES + 2,))],
            compiler_params=pltpu.CompilerParams(vmem_limit_bytes=16 * 1024 * 1024),
        )(*(from_chip(out) for out in (res, conv, ssm)))
        return res.reshape(all_rows, d_local), conv.transpose(0, 2, 3, 1), ssm.transpose(0, 1, 3, 2)

    cache_spec = P(None, ("dp", "tx"), "ty", None)
    in_specs = (P("dp", "tx"), P(None, "tx"), P(None, "tx", None, "ty"), P(None, "ty", None), P(None, "ty"), P(None, "ty", None), P(None, None, "ty"), P(None, "ty"), P(None, "ty", None), P(None, "ty"), P(None, "ty", "tx"), cache_spec, cache_spec)
    out_specs = (P("dp", "tx"), cache_spec, cache_spec)
    return jax.shard_map(local_step, mesh=mesh, in_specs=in_specs, out_specs=out_specs, check_vma=False)


def solution(mesh):
    return build(mesh, 4, STREAMS, ORDER)
```

```python
import functools

import jax
import jax.numpy as jnp
from jax import lax
from jax.experimental import pallas as pl
from jax.experimental.pallas import tpu as pltpu
from jax.sharding import PartitionSpec as P

NORM_EPS = 1e-5
INNER_EPS = 1e-6
MESH = pl.DeviceIdType.MESH
F32 = jnp.float32
BF16 = jnp.bfloat16
LANES = 128
GATE = 10
WEIGHT = 20
W_IN = 30
PIECES = 4
CUT = 2
STREAMS = 4
ORDER = (
    0, 3, 2, 1, 0, 3, 30, 20, 11, 10, 1, 20, 2, 13, 12, 3, 0, 10, 1, 30, 3, 20, 11, 30,
    2, 0, 20, 13, 12, 0, 20, 1, 20, 1, 3, 2, 2, 30, 30, 0, 30, 30, 1, 3, 2, 20, 0, 1,
    3, 2, 30, 0, 1, 3, 2, 0, 20, 10, 1, 11, 3, 13, 2, 12, 0, 0, 1, 1, 3, 3, 2, 2,
    0, 1, 3, 2, 0, 1, 3, 2, 1, 0, 3, 2,
)
STORES = 1
VMEM_LIMIT = 52 * 1024 * 1024


def far(count):
    return sorted(range(1, count), key=lambda off: -min(off, count - off))


def nt_dot(lhs, rhs, precision=None):
    return lax.dot_general(lhs, rhs, (((1,), (1,)), ((), ())), precision=precision, preferred_element_type=F32)


def nn_dot(lhs, rhs):
    return jnp.dot(lhs, rhs, preferred_element_type=F32)


def unit_rms(vec, count):
    return vec * lax.rsqrt(jnp.sum(vec * vec, axis=-1, keepdims=True) / count + INNER_EPS)


def step_kernel(dims, res_in, norm_in, win_in, cw_in, cb_in, wx_in, wdt_in, dtb_in, al_in, dsk_in, wo_in, cs_in, ssm_in,
                res_out, conv_out, ssm_buf,
                res_ref, norm_ref, win_ref, cw_ref, cb_ref, wx_ref, wdt_ref, dtb_ref, al_ref, dsk_ref, wo_ref, cs_ref,
                w_all, h_send, h_all, sth_send, sth_all, stz_send, stz_recv, g_send, g_recv, send_a, recv_a, send_b, recv_b, send_a2, recv_a2, send_b2, recv_b2, st_send, st_recv, st2_send, st2_recv, stat_t,
                p_send, p_recv, y_buf, o_send, o_recv, sum_buf, tot_buf, neg_buf, dt_buf, dx_buf, bc_buf, yv_buf, xc_buf,
                in_sems, *sem_refs):
    m_a, m_b, m_a2, m_b2, m_st, m_st2, m_p, m_y, m_o, m_s, m_w, m_h, m_sth, m_stz, m_g, m_i = [(sem_refs[2 * i], sem_refs[2 * i + 1]) for i in range(len(sem_refs) // 2)]
    n_z, n_y, n_ty, n_str, rows, layers, d_model, n_state, rank, order = dims
    tx, ty = lax.axis_index("tx"), lax.axis_index("ty")
    zi, yi = tx // n_y, tx % n_y
    chans = win_ref.shape[-1]
    cut = chans * CUT // 4
    group = n_y * rows
    own_rows = group // n_ty
    per = n_ty // n_y
    cy, cc = lax.rem(ty // per + yi, n_y), ty % per

    def chunk_of(owner):
        return lax.rem(owner // per + yi, n_y) * per + owner % per

    pk = p_send.shape[1] - rows
    y1, z1, t1 = n_y - 1, n_z - 1, n_ty - 1
    scope = jax.named_scope

    def y_peer(off):
        return lax.rem(yi + off, n_y)

    def z_peer(off):
        return lax.rem(zi + off, n_z)

    def at_y(off):
        return {"tx": zi * n_y + y_peer(off), "ty": ty}

    def at_z(off):
        return {"tx": z_peer(off) * n_y + yi, "ty": ty}

    def at_ty(idx):
        return {"tx": tx, "ty": idx}

    def ty_peer(off):
        return at_ty(lax.rem(ty + off, n_ty))

    def send(src, dst, sems, slot, device):
        pltpu.make_async_remote_copy(src_ref=src, dst_ref=dst, send_sem=sems[0], recv_sem=sems[1].at[slot], device_id=device, device_id_type=MESH).start()

    def arrived(ref, sems, slot):
        pltpu.make_async_remote_copy(src_ref=ref, dst_ref=ref, send_sem=sems[0], recv_sem=sems[1].at[slot], device_id=ty_peer(1), device_id_type=MESH).wait_recv()

    def departed(ref, sems):
        pltpu.make_async_remote_copy(src_ref=ref, dst_ref=ref, send_sem=sems[0], recv_sem=sems[1].at[0], device_id=ty_peer(1), device_id_type=MESH).wait_send()

    def add_up(first, others):
        return functools.reduce(jnp.add, [o.astype(F32) for o in others], first.astype(F32))

    split = set()

    def split_weight(lyr, part):
        if (lyr, part) not in split:
            split.add((lyr, part))
            need(("win", lyr))
            w_all[lyr, part, yi] = win_ref[lyr, :, part, :]

    def input_matmul(k, lyr, strm, source, part):
        split_weight(lyr, part)
        need(("res", strm))
        norm = norm_ref[lyr:lyr + 1, :]
        for zz in range(n_z):
            res = source[zz, :, strm].reshape(group, LANES)
            if part == 0:
                st_send[k, zz] = nt_dot(jnp.ones((8, LANES), F32), res * res, lax.Precision.HIGHEST)
            prod = nn_dot((res * norm).astype(BF16), w_all[lyr, part, yi]).astype(BF16)
            send_b[k, part, zz] = prod[:, cut:]
            for yy in range(n_y):
                send_a[k, part, yy, zz * rows:(zz + 1) * rows, :] = prod[yy * rows:(yy + 1) * rows, :cut]

    def phase_one(k, part):
        for off in far(n_z):
            if part == 0:
                send(st_send.at[k, z_peer(off)], st_recv.at[k, off - 1], m_st, k, at_z(off))
        for off in far(max(n_y, n_z)):
            if off < n_y:
                send(send_a.at[k, part, y_peer(off)], recv_a.at[k, part, off - 1], m_a, 2 * k + part, at_y(off))
            if off < n_z:
                send(send_b.at[k, part, z_peer(off)], recv_b.at[k, part, off - 1], m_b, 2 * k + part, at_z(off))

    def phase_two(k, part):
        if part == 0:
            arrived(st_recv.at[k], m_st, k)
            st2_send[k] = add_up(st_send[k, zi], [st_recv[k, off - 1] for off in range(1, n_z)])
            for off in far(n_y):
                send(st2_send.at[k], st2_recv.at[k, off - 1], m_st2, k, at_y(off))
        with scope(f"wait_a1_{part}"):
            arrived(recv_a.at[k, part], m_a, 2 * k + part)
        for zz in range(n_z):
            span = slice(zz * rows, (zz + 1) * rows)
            send_a2[k, part, zz] = add_up(send_a[k, part, yi, span, :], [recv_a[k, part, off - 1, span, :] for off in range(1, n_y)]).astype(BF16)
        for off in far(n_z):
            send(send_a2.at[k, part, z_peer(off)], recv_a2.at[k, part, off - 1], m_a2, 2 * k + part, at_z(off))
        with scope(f"wait_b1_{part}"):
            arrived(recv_b.at[k, part], m_b, 2 * k + part)
        for yy in range(n_y):
            span = slice(yy * rows, (yy + 1) * rows)
            send_b2[k, part, yy] = add_up(send_b[k, part, zi, span, :], [recv_b[k, part, off - 1, span, :] for off in range(1, n_z)]).astype(BF16)
        for off in far(n_y):
            send(send_b2.at[k, part, y_peer(off)], recv_b2.at[k, part, off - 1], m_b2, 2 * k + part, at_y(off))

    def finish_sum(k, part):
        if k >= n_str:
            kh = k - n_str
            with scope(f"wait_g_{part}"):
                arrived(g_recv.at[kh, part], m_g, 2 * kh + part)
            return add_up(g_send[kh, part, zi], [g_recv[kh, part, off - 1] for off in range(1, n_z)])
        with scope(f"wait_2_{part}"):
            arrived(recv_a2.at[k, part], m_a2, 2 * k + part)
            arrived(recv_b2.at[k, part], m_b2, 2 * k + part)
        tot_a = add_up(send_a2[k, part, zi], [recv_a2[k, part, off - 1] for off in range(1, n_z)])
        tot_b = add_up(send_b2[k, part, yi], [recv_b2[k, part, off - 1] for off in range(1, n_y)])
        return jnp.concatenate([tot_a, tot_b], axis=-1)

    def row_scale(k):
        if k >= n_str:
            kh = k - n_str
            arrived(stz_recv.at[kh], m_stz, kh)
            total = add_up(stz_send[kh], [stz_recv[kh, off - 1] for off in range(1, n_z)])
            mine = []
            for c in range(per):
                stat_t[k, c * n_z * own_rows:(c + 1) * n_z * own_rows, :] = total[c].T
                mine.append(stat_t[k, pl.ds(pl.multiple_of((c * n_z + zi) * own_rows, own_rows), own_rows), :][:, :1])
            mine = jnp.concatenate(mine, axis=0)
        else:
            arrived(st2_recv.at[k], m_st2, k)
            stat_t[k, :group] = add_up(st2_send[k], [st2_recv[k, off - 1] for off in range(1, n_y)]).T
            mine = stat_t[k, pl.ds(pl.multiple_of(yi * rows, 8), rows), :][:, :1]
        return lax.rsqrt(mine / d_model + NORM_EPS)

    def spread_hidden(k, strm, total):
        tot_buf[strm] = total
        res = res_ref[:, cy, strm, pl.ds(pl.multiple_of(cc * own_rows, own_rows), own_rows), :] + total
        norm = norm_ref[k // n_str + 1:k // n_str + 2, :].reshape(1, 1, LANES)
        h_send[k] = (res * norm).astype(BF16)
        slot = yi * per + cc

        def deliver(src, dst, sems):
            for step in far(n_ty):
                send(src.at[k], dst.at[k, slot], sems, k, {"tx": zi * n_y + cy, "ty": lax.rem(ty + step, n_ty)})

            @pl.when(cy != yi)
            def _():
                send(src.at[k], dst.at[k, slot], sems, k, {"tx": zi * n_y + cy, "ty": ty})

        deliver(h_send, h_all, m_h)
        sth_send[k] = nt_dot(jnp.ones((8, LANES), F32), (res * res).reshape(n_z * own_rows, LANES), lax.Precision.HIGHEST)
        deliver(sth_send, sth_all, m_sth)

        @pl.when(cy == yi)
        def _():
            h_all[k, slot] = h_send[k]
            sth_all[k, slot] = sth_send[k]

    def slab_matmul(k, lyr, part):
        kh = k - n_str
        if part == 0:
            with scope(f"wait_h"):
                @pl.when(cy != yi)
                def _():
                    arrived(h_all.at[kh], m_h, kh)
                    arrived(sth_all.at[kh], m_sth, kh)

                @pl.when(cy == yi)
                def _():
                    arrived(h_all.at[kh, :n_ty - 1], m_h, kh)
                    arrived(sth_all.at[kh, :n_ty - 1], m_sth, kh)

            for c in range(per):
                stz_send[kh, c] = functools.reduce(jnp.add, [sth_all[kh, yy * per + c] for yy in range(n_y)])
            for off in far(n_z):
                send(stz_send.at[kh], stz_recv.at[kh, off - 1], m_stz, kh, at_z(off))
        if (lyr, part) not in gathered:
            gathered.add((lyr, part))
            with scope(f"wait_i"):
                arrived(w_all.at[lyr, part, :y1], m_i, 2 * (lyr - 1) + part)
        hidden = jnp.concatenate([h_all[kh, yy * per:(yy + 1) * per].reshape(n_z * rows, LANES) for yy in range(n_y)], axis=1)
        prod = nn_dot(hidden, w_all[lyr, part].reshape(n_y * LANES, chans)).reshape(per, n_z, own_rows, chans)
        for zz in range(n_z):
            g_send[kh, part, zz] = prod[:, zz].reshape(rows, chans).astype(BF16)
        for off in far(n_z):
            send(g_send.at[kh, part, z_peer(off)], g_recv.at[kh, part, off - 1], m_g, 2 * kh + part, at_z(off))

    def conv_and_proj(k, lyr, mine, x_in):
        taps = [cs_ref[lyr, j, mine, :] for j in range(3)]
        conv_out[lyr, 0, mine, :] = taps[1]
        conv_out[lyr, 1, mine, :] = taps[2]
        conv_out[lyr, 2, mine, :] = x_in
        conv = x_in.astype(F32) * cw_ref[lyr, 3:4, :] + cb_ref[lyr:lyr + 1, :]
        for j in range(3):
            conv = conv + taps[j].astype(F32) * cw_ref[lyr, j:j + 1, :]
        x_conv = (conv * jax.nn.sigmoid(conv)).astype(BF16)
        xc_buf[k] = x_conv
        wx = wx_ref[lyr]
        bc_w = jnp.concatenate([wx[rank:], jnp.zeros((LANES - 2 * n_state, chans), BF16)], axis=0)
        bc_part = nt_dot(x_conv, bc_w)
        packed = bc_part[:pk]
        for q in range(1, rows // pk):
            packed = packed + pltpu.roll(bc_part[q * pk:(q + 1) * pk], q * 2 * n_state, 1)
        p_send[k, :rows] = nt_dot(x_conv, wx[:rank]).astype(BF16)
        p_send[k, rows:] = packed.astype(BF16)

    def step_sizes(k, lyr):
        proj = add_up(p_send[k], [p_recv[k, off - 1] for off in range(1, n_ty)])
        dt_low = unit_rms(proj[:rows], rank).astype(BF16)
        lane = lax.broadcasted_iota(jnp.int32, (pk, LANES), 1)
        for q in range(rows // pk):
            piece = proj[rows:]
            if q:
                piece = pltpu.roll(piece, LANES - q * 2 * n_state, 1)
            sq = piece * piece
            b_inv = lax.rsqrt(jnp.sum(jnp.where(lane < n_state, sq, 0.0), axis=-1, keepdims=True) / n_state + INNER_EPS)
            c_inv = lax.rsqrt(jnp.sum(jnp.where((lane >= n_state) & (lane < 2 * n_state), sq, 0.0), axis=-1, keepdims=True) / n_state + INNER_EPS)
            bc_buf[k, q * pk:(q + 1) * pk] = piece * jnp.where(lane < n_state, b_inv, c_inv)
        raw = nn_dot(dt_low, wdt_ref[lyr]) + dtb_ref[lyr:lyr + 1, :]
        delta = jnp.maximum(raw, 0.0) + jnp.log1p(jnp.exp(-jnp.abs(raw)))
        dt_buf[k] = delta
        dx_buf[k] = delta * xc_buf[k].astype(F32)

    def state_update(k, lyr, strm):
        neg_a = neg_buf[lyr]

        def update(grp, carry):
            base = pl.multiple_of(grp * 8, 8)
            d_rows = dt_buf[k, pl.ds(base, 8), :]
            x_rows = dx_buf[k, pl.ds(base, 8), :]
            bc_t = bc_buf[k, pl.ds(base, 8), :].T
            outs = []
            for j in range(8):
                row = strm * rows + base + j
                decay = jnp.exp(d_rows[j:j + 1, :] * neg_a)
                state = decay * ssm_buf[lyr, row] + x_rows[j:j + 1, :] * bc_t[:n_state, j:j + 1]
                ssm_buf[lyr, row] = state
                outs.append(jnp.sum(state * bc_t[n_state:2 * n_state, j:j + 1], axis=0, keepdims=True))
            yv_buf[k, pl.ds(base, 8), :] = jnp.concatenate(outs, axis=0)
            return carry

        lax.fori_loop(0, rows // 8, update, 0)

    def main_thread(strm):
        mine = slice(strm * rows, (strm + 1) * rows)
        for lyr in range(layers):
            k = lyr * n_str + strm
            if lyr:
                with scope(f"slab_{strm}"):
                    slab_matmul(k, lyr, 0)
            else:
                if strm != lead:
                    with scope(f"matmul_{strm}"):
                        input_matmul(k, lyr, strm, res_ref, 0)
                phase_one(k, 0)
                yield
                with scope(f"phase2_{strm}"):
                    phase_two(k, 0)
            yield
            with scope(f"xconv_{strm}"):
                scale = row_scale(k)
                need("cw", "cb", "cs", "wx")
                conv_and_proj(k, lyr, mine, (finish_sum(k, 0) * scale).astype(BF16))
            for off in far(n_ty):
                send(p_send.at[k], p_recv.at[k, off - 1], m_p, k, ty_peer(off))
            yield
            if ("neg", lyr) not in split:
                split.add(("neg", lyr))
                need("al")
                neg_buf[lyr] = -jnp.exp(al_ref[lyr])
            with scope(f"wait_p_{strm}"):
                arrived(p_recv.at[k], m_p, k)
            with scope(f"ssm_{strm}"):
                need("wdt", "dtb", "al", "dsk", ("ssm", lyr))
                step_sizes(k, lyr)
                state_update(k, lyr, strm)
            yield
            with scope(f"gate_{strm}"):
                z_in = (finish_sum(k, 1) * scale).astype(BF16).astype(F32)
                gated = ((yv_buf[k] + dsk_ref[lyr:lyr + 1, :] * xc_buf[k].astype(F32)) * (z_in * jax.nn.sigmoid(z_in))).astype(BF16)
                y_buf[k, yi] = gated
            for off in far(n_y):
                send(y_buf.at[k, yi], y_buf.at[k, yi], m_y, k, at_y(off))
            yield
            with scope(f"wait_y_{strm}"):
                arrived(y_buf.at[k, :y1], m_y, k)
            with scope(f"outmm_{strm}"):
                if lyr not in gathered:
                    gathered.add(lyr)
                    arrived(wo_ref.at[lyr, :z1 - 1], m_w, lyr)
                everyone = y_buf[k].reshape(group, chans)
                for off in far(n_z) + [0]:
                    zz = z_peer(off)
                    o_send[k, zz] = nn_dot(everyone, wo_ref[lyr, zz]).reshape(n_ty, own_rows, LANES).astype(BF16)
                    for step in far(n_ty) + [0]:
                        owner = lax.rem(ty + step, n_ty)
                        if off or step:
                            send(o_send.at[k, zz, chunk_of(owner)], o_recv.at[k, zi * n_ty + ty], m_o, k, {"tx": zz * n_y + yi, "ty": owner})
                o_recv[k, zi * n_ty + ty] = o_send[k, zi, chunk_of(ty)]
            yield
            with scope(f"wait_o_{strm}"):
                arrived(o_recv.at[k, :n_z * n_ty - 1], m_o, k)
            parts = o_recv[k].astype(F32).reshape(n_z, n_ty, own_rows, LANES)
            total = functools.reduce(jnp.add, [parts[:, i] for i in range(n_ty)])
            if lyr:
                total = total + tot_buf[strm]
            if lyr < layers - 1:
                with scope(f"hidden_{strm}"):
                    spread_hidden(k, strm, total)
                yield
                continue
            sum_buf[strm, ty] = total.astype(BF16)
            for off in far(n_ty):
                send(sum_buf.at[strm, ty], sum_buf.at[strm, ty], m_s, strm, ty_peer(off))
            yield
        with scope(f"wait_s_{strm}"):
            arrived(sum_buf.at[strm, :t1], m_s, strm)
        for owner in range(n_ty):
            blk, low = lax.rem(owner // per + yi, n_y), owner % per * own_rows
            span = slice(low, low + own_rows)
            res_out[:, blk, strm, span, :] = res_ref[:, blk, strm, span, :] + sum_buf[strm, owner].astype(F32)

    def gate_thread(strm):
        for lyr in range(layers):
            k = lyr * n_str + strm
            if lyr:
                with scope(f"slabz_{strm}"):
                    slab_matmul(k, lyr, 1)
                yield
                continue
            with scope(f"matmulz_{strm}"):
                input_matmul(k, lyr, strm, res_ref, 1)
            phase_one(k, 1)
            yield
            with scope(f"phase2z_{strm}"):
                phase_two(k, 1)
            yield

    def weight_thread():
        width = chans // 2

        def hand_out(lyr, piece, back, ahead):
            block = wo_ref.at[lyr, z_peer(n_z - back), pl.ds(piece * width, width)]
            slot = layers + 2 * lyr + piece if back == 0 and ahead == (1, n_z - 1)[piece] else lyr
            send(block, block, m_w, slot, at_z(ahead))

        for lyr in range(layers):
            for piece in range(2):
                if piece == 0:
                    need(("wo", lyr))
                hand_out(lyr, piece, 0, 1)
                if n_z > 2:
                    hand_out(lyr, piece, 0, n_z - 1)
                yield
            for piece in range(2):
                if n_z > 2:
                    arrived(wo_ref.at[lyr, 0, pl.ds(piece * width, width)], m_w, layers + 2 * lyr + piece)
                    ahead = (1, n_z - 1)[piece]
                    hand_out(lyr, piece, ahead, ahead)
                yield

    def w_in_thread():
        for lyr in range(1, layers):
            for part in range(2):
                split_weight(lyr, part)
                for piece in range(PIECES):
                    span = pl.ds(piece * LANES // PIECES, LANES // PIECES)
                    for off in far(n_y):
                        send(w_all.at[lyr, part, yi, span], w_all.at[lyr, part, yi, span], m_i, 2 * (lyr - 1) + part, at_y(off))
                    yield

    gathered = set()
    lead = next(name for name in order if name < GATE)
    moves = {("res", lead): (res_in.at[:, :, lead], res_ref.at[:, :, lead]), "norm": (norm_in, norm_ref), ("win", 0): (win_in.at[0], win_ref.at[0])}
    first = len(moves)
    moves.update({("res", strm): (res_in.at[:, :, strm], res_ref.at[:, :, strm]) for strm in range(n_str) if strm != lead})
    moves.update({"cw": (cw_in, cw_ref), "cb": (cb_in, cb_ref), "cs": (cs_in, cs_ref), "wx": (wx_in, wx_ref), "wdt": (wdt_in, wdt_ref)})
    moves.update({"dtb": (dtb_in, dtb_ref), "al": (al_in, al_ref), "dsk": (dsk_in, dsk_ref)})
    second = len(moves)
    moves.update({("wo", lyr): (wo_in.at[lyr], wo_ref.at[lyr, zi]) for lyr in range(layers)})
    moves.update({("win", lyr): (win_in.at[lyr], win_ref.at[lyr]) for lyr in range(1, layers)})
    moves.update({("ssm", lyr): (ssm_in.at[lyr], ssm_buf.at[lyr]) for lyr in range(layers)})
    loads = {name: pltpu.make_async_copy(src, dst, in_sems.at[i]) for i, (name, (src, dst)) in enumerate(moves.items())}
    for name in list(loads)[:first]:
        loads[name].start()
    rest, late = list(loads)[first:second], list(loads)[second:]

    def need(*names):
        for name in names:
            if name in loads:
                loads.pop(name).wait()

    barrier = pltpu.get_barrier_semaphore()
    peers = [at_y(off) for off in range(1, n_y)] + [at_z(off) for off in range(1, n_z)] + [ty_peer(off) for off in range(1, n_ty)]
    for peer in peers:
        pl.semaphore_signal(barrier, inc=1, device_id=peer, device_id_type=MESH)
    need(("res", lead), "norm", ("win", 0))
    for name in rest:
        loads[name].start()
    with scope("matmul_first"):
        input_matmul(lead, 0, lead, res_ref, 0)
    with scope("barrier"):
        pl.semaphore_wait(barrier, len(peers))

    threads = {}
    for strm in range(n_str):
        threads[strm] = main_thread(strm)
        threads[GATE + strm] = gate_thread(strm)
    threads[WEIGHT] = weight_thread()
    threads[W_IN] = w_in_thread()
    for turn, name in enumerate(order):
        if turn == n_str:
            for load in late:
                loads[load].start()
        next(threads[name], None)

    with scope("drain"):
        sent = [recv_a, recv_b, recv_a2, recv_b2, st_recv, st2_recv, p_recv, y_buf.at[:, :y1], o_recv.at[:, :n_z * n_ty - 1], sum_buf.at[:, :t1], wo_ref.at[:, :z1],
                stz_recv, g_recv, w_all.at[1:, :, :y1]]
        for ref, sems in zip(sent, [m_a, m_b, m_a2, m_b2, m_st, m_st2, m_p, m_y, m_o, m_s, m_w, m_stz, m_g, m_i]):
            departed(ref, sems)

        @pl.when(cy != yi)
        def _():
            departed(h_all, m_h)
            departed(sth_all, m_sth)

        @pl.when(cy == yi)
        def _():
            departed(h_all.at[:, :n_ty - 1], m_h)
            departed(sth_all.at[:, :n_ty - 1], m_sth)


def store_kernel(res_ref, conv_ref, ssm_ref, res_out, conv_out, ssm_out, sems):
    pairs = []
    step = ssm_ref.shape[1] // STORES
    for lyr in range(ssm_ref.shape[0]):
        for i in range(STORES):
            pairs.append((ssm_ref.at[lyr, i * step:(i + 1) * step], ssm_out.at[lyr, i * step:(i + 1) * step]))
    pairs += [(res_ref, res_out), (conv_ref, conv_out)]
    copies = [pltpu.make_async_copy(src, dst, sems.at[i]) for i, (src, dst) in enumerate(pairs)]
    for desc in copies:
        desc.start()
    for desc in copies:
        desc.wait()


def on_chip(shape, dtype):
    return pltpu.VMEM(shape, dtype)


def from_chip(array):
    return pltpu.with_memory_space_constraint(array, pltpu.VMEM)


def build(mesh, n_y, n_str, order):
    n_tx, n_ty = mesh.shape["tx"], mesh.shape["ty"]
    n_z = n_tx // n_y

    def local_step(residual, norm_w, w_in, conv_w, conv_b, w_x, w_dt, dt_bias, a_log, d_skip, w_out, conv_state, ssm_state):
        layers, batch, chans, n_state = ssm_state.shape
        rows = batch // n_str
        all_rows, d_local = residual.shape
        rank = w_dt.shape[1]
        cut = chans * CUT // 4
        own = n_y * rows // n_ty
        pk = rows * 2 * n_state // LANES
        ks = layers * n_str
        kh = ks - n_str
        dims = (n_z, n_y, n_ty, n_str, rows, layers, d_local * n_tx, n_state, rank, order)
        vmem = pl.BlockSpec(memory_space=pltpu.VMEM)
        anyspace = pl.BlockSpec(memory_space=pl.ANY)
        dma = pltpu.SemaphoreType.DMA
        res_shape = (n_z, n_y, n_str, rows, d_local)
        conv_shape = (layers, 3, batch, chans)
        ssm_shape = (layers, batch, n_state, chans)
        operands = [
            residual.reshape(res_shape), norm_w, w_in, conv_w.transpose(0, 2, 1), conv_b, w_x.transpose(0, 2, 1), w_dt, dt_bias,
            a_log.transpose(0, 2, 1), d_skip, w_out, conv_state.transpose(0, 3, 1, 2), ssm_state.transpose(0, 1, 3, 2),
        ]
        shapes = [op.shape for op in operands[:-1]]
        shapes[10] = (layers, n_z, chans, d_local)
        scratch = [pltpu.VMEM(shape, op.dtype) for shape, op in zip(shapes, operands)]
        scratch += [
            pltpu.VMEM((layers, 2, n_y, d_local, chans), BF16),
            pltpu.VMEM((kh, n_z, own, d_local), BF16),
            pltpu.VMEM((kh, n_ty, n_z, own, d_local), BF16),
            pltpu.VMEM((kh, 8, n_z * own), F32),
            pltpu.VMEM((kh, n_ty, 8, n_z * own), F32),
            pltpu.VMEM((kh, n_ty // n_y, 8, n_z * own), F32),
            pltpu.VMEM((kh, n_z - 1, n_ty // n_y, 8, n_z * own), F32),
            pltpu.VMEM((kh, 2, n_z, rows, chans), BF16),
            pltpu.VMEM((kh, 2, n_z - 1, rows, chans), BF16),
            pltpu.VMEM((n_str, 2, n_y, n_z * rows, cut), BF16),
            pltpu.VMEM((n_str, 2, n_y - 1, n_z * rows, cut), BF16),
            pltpu.VMEM((n_str, 2, n_z, n_y * rows, chans - cut), BF16),
            pltpu.VMEM((n_str, 2, n_z - 1, n_y * rows, chans - cut), BF16),
            pltpu.VMEM((n_str, 2, n_z, rows, cut), BF16),
            pltpu.VMEM((n_str, 2, n_z - 1, rows, cut), BF16),
            pltpu.VMEM((n_str, 2, n_y, rows, chans - cut), BF16),
            pltpu.VMEM((n_str, 2, n_y - 1, rows, chans - cut), BF16),
            pltpu.VMEM((n_str, n_z, 8, n_y * rows), F32),
            pltpu.VMEM((n_str, n_z - 1, 8, n_y * rows), F32),
            pltpu.VMEM((n_str, 8, n_y * rows), F32),
            pltpu.VMEM((n_str, n_y - 1, 8, n_y * rows), F32),
            pltpu.VMEM((ks, max(n_y, n_z) * rows, 8), F32),
            pltpu.VMEM((ks, rows + pk, LANES), BF16),
            pltpu.VMEM((ks, n_ty - 1, rows + pk, LANES), BF16),
            pltpu.VMEM((ks, n_y, rows, chans), BF16),
            pltpu.VMEM((ks, n_z, n_ty, own, d_local), BF16),
            pltpu.VMEM((ks, n_z * n_ty, own, d_local), BF16),
            pltpu.VMEM((n_str, n_ty, n_z, own, d_local), BF16),
            pltpu.VMEM((n_str, n_z, own, d_local), F32),
            pltpu.VMEM((layers, n_state, chans), F32),
            pltpu.VMEM((ks, rows, chans), F32),
            pltpu.VMEM((ks, rows, chans), F32),
            pltpu.VMEM((ks, rows, LANES), F32),
            pltpu.VMEM((ks, rows, chans), F32),
            pltpu.VMEM((ks, rows, chans), BF16),
        ]
        scratch += [dma((len(operands) + n_str + 3 * layers,))]
        for count in [2 * n_str, 2 * n_str, 2 * n_str, 2 * n_str, n_str, n_str, ks, ks, ks, n_str, 3 * layers, kh, kh, kh, 2 * kh, 2 * (layers - 1)]:
            scratch += [dma, dma((count,))]
        res, conv, ssm = pl.pallas_call(
            functools.partial(step_kernel, dims),
            out_shape=(on_chip(res_shape, F32), on_chip(conv_shape, BF16), on_chip(ssm_shape, F32)),
            in_specs=[pl.BlockSpec(memory_space=pltpu.HBM)] * len(operands),
            out_specs=(vmem, vmem, vmem),
            scratch_shapes=scratch,
            compiler_params=pltpu.CompilerParams(collective_id=0, has_side_effects=True, vmem_limit_bytes=VMEM_LIMIT),
        )(*operands)
        res, conv, ssm = pl.pallas_call(
            store_kernel,
            out_shape=(jax.ShapeDtypeStruct(res_shape, F32), jax.ShapeDtypeStruct(conv_shape, BF16), jax.ShapeDtypeStruct(ssm_shape, F32)),
            in_specs=[vmem] * 3,
            out_specs=(anyspace,) * 3,
            scratch_shapes=[dma((layers * STORES + 2,))],
            compiler_params=pltpu.CompilerParams(vmem_limit_bytes=16 * 1024 * 1024),
        )(*(from_chip(out) for out in (res, conv, ssm)))
        return res.reshape(all_rows, d_local), conv.transpose(0, 2, 3, 1), ssm.transpose(0, 1, 3, 2)

    cache_spec = P(None, ("dp", "tx"), "ty", None)
    in_specs = (P("dp", "tx"), P(None, "tx"), P(None, "tx", None, "ty"), P(None, "ty", None), P(None, "ty"), P(None, "ty", None), P(None, None, "ty"), P(None, "ty"), P(None, "ty", None), P(None, "ty"), P(None, "ty", "tx"), cache_spec, cache_spec)
    out_specs = (P("dp", "tx"), cache_spec, cache_spec)
    return jax.shard_map(local_step, mesh=mesh, in_specs=in_specs, out_specs=out_specs, check_vma=False)


def solution(mesh):
    return build(mesh, 4, STREAMS, ORDER)
```
